128 devices in a mesh: lon: 8 (over y, x_lo), lat: 16 (over x_hi, z, core).
Axes of the slice: x: 4 (x_hi: 2, x_lo: 2; x = x_hi * 2 + x_lo), y: 4, z: 4, core: 2. Of those that a mesh axis runs over, the one named last changes fastest.
Arguments:
- tracers: float32 [4, 16, 2048, 1024], P(None, None, 'lat', 'lon'), may hold values from -6 to 6
- fill_fraction: float32 [16, 2048, 1024], P(None, 'lat', 'lon'), may hold values from 0.3 to 1
- ocean_mask: int32 [16, 2048, 1024], P(None, 'lat', 'lon'), may hold values 0 or 1
- east_speed: float32 [16, 2048, 1024], P(None, 'lat', 'lon'), may hold values from -3 to 3
- north_speed: float32 [16, 2048, 1024], P(None, 'lat', 'lon'), may hold values from -3 to 3
- diffusivity: float32 [16], replicated, may hold values from 0.1 to 1
- cell_area: float32 [2048, 1024], P('lat', 'lon'), may hold values from 0.25 to 1
- owner_map: int32 [16384, 1], P(('lon', 'lat')), may hold values from 0 to 127; in each aligned block of 128 rows (0 to 127, 128 to 255, ...) at most 2 rows name the same one
Outputs:
- updated: float32 [4, 16, 2048, 1024], P(None, None, 'lat', 'lon')
- received_two: float32 [128, 256, 2048], P(('lon', 'lat'))
- received_four: float32 [128, 256, 512], P(('lon', 'lat'))
The draws below stay inside these ranges and needn't reach their ends.
Inputs may be any that keep to these rules, and one draw needn't show every extreme that they name: `owner_map`: owner device numbers in lon-major order. Of the 128 rows of one device, at most 2 name the same owner, and in some device exactly 2 do.
All inputs are finite; a program needn't handle non-finite values. No bound on the sum of `ocean_mask` on one device may be relied on, other than what follows from the above.
Results may differ from the reference program's by a relative error of at most 0.00007.
Values sent between devices are 32-bit elements; how exact they have to be, the bound alone decides.
No kernel may reach another device: no remote copies, remote signals or barrier semaphores. Data moves between devices by JAX's collectives and lax.ppermute only.
A program may use at most 128 MiB of HBM per device.

```python
import math
import jax
import jax.numpy as jnp
import numpy as np

TRACERS = 4
LEVELS = 16
BAND_ROWS = 16
NLON = 1024
NLAT = 2048
UNITS = 128
CAP = 2
N_LON = 8
N_LAT = 16
DEVICES = 128


def with_ends(result, key, smallest, high):
    index_at = [jax.random.randint(jax.random.fold_in(key, axis), (), 0, length) for axis, length in enumerate(result.shape)]
    longest = result.shape.index(max(result.shape))
    next_to = index_at[:longest] + [(index_at[longest] + 1) % result.shape[longest]] + index_at[longest + 1:]
    return result.at[tuple(index_at)].set(smallest).at[tuple(next_to)].set(high)


def steps_of(own_key, shape, shards, least, largest):
    gain, own = 1.0, jax.random.fold_in(own_key, 6)
    for dim, shards_of in shards:
        steps = jnp.exp(jax.random.uniform(jax.random.fold_in(own, dim), (shards_of,), jnp.float32, least / len(shards), largest / len(shards)))
        gain = gain * jnp.repeat(steps, shape[dim] // shards_of).reshape([-1 if axis == dim else 1 for axis in range(len(shape))])
    return gain


def shared_out(key, own, number, rows, amount, top, bound, slope):
    ranking = jax.random.permutation(key, amount)
    crowded, common = portions_of(amount, rows * top, bound, slope, True), portions_of(amount, rows * top, bound, slope, False)
    places = jnp.arange(amount)

    def named(lengths, rotation):
        used = int((lengths > 0).sum())
        fixed = max(1, used // 4)
        shifted = fixed + (places - fixed + rotation * (used - fixed)) % max(1, amount - fixed)
        return jnp.zeros((amount,), jnp.int32).at[ranking[jnp.where(places < fixed, places, shifted)]].set(jnp.asarray(lengths, jnp.int32))

    lengths = jnp.where(number % 4 == 0, named(crowded, number // 4), named(common, number - number // 4 - 1))
    mixed = jax.random.permutation(jax.random.fold_in(own, 3), amount)
    source_of, taker = mixed[0:amount // 2 * 2:2], mixed[1:amount // 2 * 2:2]
    margin = jnp.minimum(lengths[source_of] - 1, bound - lengths[taker]) // 2
    margin = jnp.where((source_of == ranking[0]) | (taker == ranking[0]) | (lengths[taker] == 0), 0, jnp.maximum(margin, 0))
    shifted = jax.random.randint(jax.random.fold_in(own, 4), (amount // 2,), 0, 1 << 20) % (margin + 1)
    lengths = lengths.at[source_of].add(-shifted).at[taker].add(shifted)
    items = jnp.searchsorted(jnp.cumsum(lengths), jnp.arange(rows * top), side="right").astype(jnp.int32)
    listing = items.reshape(top, rows).T
    listing = listing[jax.random.permutation(jax.random.fold_in(own, 1), rows)]
    rotation = jax.random.randint(jax.random.fold_in(own, 2), (rows, 1), 0, top)
    return jnp.take_along_axis(listing, (jnp.arange(top)[None, :] + rotation) % top, axis=1)


def portions_of(count, total, bound, lean, full):
    weights = [(1 << 20) // math.isqrt(standing ** lean) + 1 for standing in range(1, count + 1)]
    largest = bound if full else min(bound, max(-(-total // count), total * weights[0] // sum(weights)))
    least = 1 if total - largest >= count - 1 else 0
    given, spare = [largest] + [least] * (count - 1), total - largest - least * (count - 1)
    while spare > 0:
        free = [i for i in range(1, count) if given[i] < largest] or [i for i in range(1, count) if given[i] < bound]
        mass, budget = sum([weights[i] for i in free]), spare
        for i in free:
            addition = min(bound - given[i], max(1, budget * weights[i] // mass), spare)
            given[i] = given[i] + addition
            spare = spare - addition
    return np.array(given)


def bell_draw(key, shape, deviation, reach, cuts=(), held_as=jnp.bfloat16):
    gain = steps_of(key, shape, cuts, -0.22, 0.18) if cuts else 1.0
    result = jax.random.normal(key, shape, jnp.float32) * deviation * gain
    return jnp.minimum(jnp.maximum(result, -reach), reach).astype(held_as)


def setup_inputs(seed: int = 0) -> dict:
    splits = jax.random.split(jax.random.key(seed), 9)
    tracers = bell_draw(splits[0], (TRACERS, LEVELS, NLAT, NLON), 1.0, 6.0, ((2, 16), (3, 8)), jnp.float32)
    fill_fraction = jnp.clip(jnp.exp(math.log(1.0) - 1.2039728 * jax.random.uniform(splits[1], (LEVELS, NLAT, NLON), jnp.float32) ** steps_of(splits[1], (LEVELS, NLAT, NLON), ((1, 16), (2, 8)), -0.2, 0.2)), 0.3, 1.0)
    ocean_mask = with_ends((jax.random.randint(splits[2], (LEVELS, NLAT, NLON), 0, 2) < 1).astype(jnp.int32), jax.random.fold_in(splits[2], 1), 0, 1)
    east_speed = bell_draw(splits[3], (LEVELS, NLAT, NLON), 0.5, 3.0, ((1, 16), (2, 8)), jnp.float32)
    north_speed = bell_draw(splits[4], (LEVELS, NLAT, NLON), 0.5, 3.0, ((1, 16), (2, 8)), jnp.float32)
    diffusivity = jnp.clip(jnp.exp(jax.random.uniform(splits[5], (LEVELS,), jnp.float32, math.log(0.1), math.log(1.0))), 0.1, 1.0)
    cell_area = jnp.clip(jnp.exp(math.log(1.0) - 1.3862944 * jax.random.uniform(splits[6], (NLAT, NLON), jnp.float32) ** steps_of(splits[6], (NLAT, NLON), ((0, 16), (1, 8)), -0.2, 0.2)), 0.25, 1.0)
    owner_map_keys = jax.random.split(jax.random.fold_in(splits[7], 1), (DEVICES * UNITS) // UNITS)
    owner_map_turns = jax.random.permutation(jax.random.fold_in(splits[7], 3), (DEVICES * UNITS) // UNITS)
    owner_map = jax.vmap(lambda own, number: shared_out(jax.random.fold_in(splits[7], 2), own, number, UNITS, DEVICES, 1, CAP, 2))(owner_map_keys, owner_map_turns).reshape((DEVICES * UNITS, 1))
    return dict(tracers=tracers, fill_fraction=fill_fraction, ocean_mask=ocean_mask, east_speed=east_speed, north_speed=north_speed, diffusivity=diffusivity, cell_area=cell_area, owner_map=owner_map)


time_step = 0.05
depth_floor = 0.25
weight_floor = 0.25


def face_flux(lower_val, upper_val, lower_h, upper_h, lower_speed, upper_speed, mixing):
    open_depth = jnp.minimum(lower_h, upper_h)
    face_speed = 0.5 * (lower_speed + upper_speed)
    return open_depth * (0.5 * face_speed * (lower_val + upper_val) - 0.5 * jnp.abs(face_speed) * (upper_val - lower_val) - mixing * (upper_val - lower_val))


def pool_pairs(field):
    old_shape = field.shape
    return field.reshape(old_shape[:-2] + (old_shape[-2] // 2, 2, old_shape[-1] // 2, 2)).sum(axis=(-3, -1))


def coarsen(updated, weight):
    weighted = pool_pairs(updated * weight[None])
    weight_two = pool_pairs(weight)
    weighted_four = pool_pairs(weighted)
    weight_four = pool_pairs(weight_two)
    coarse_two = weighted / jnp.maximum(weight_two, weight_floor)[None]
    coarse_four = weighted_four / jnp.maximum(weight_four, weight_floor)[None]
    return coarse_two, coarse_four


def device_blocks(field, band):
    shape_of = field.shape
    bands = shape_of[2] // N_LAT // band
    width = shape_of[3] // N_LON
    split = field.reshape(shape_of[0], shape_of[1], N_LAT, bands, band, N_LON, width)
    moved = split.transpose(5, 2, 1, 3, 0, 4, 6)
    return moved.reshape(N_LON * N_LAT, shape_of[1] * bands, shape_of[0] * band * width)


def deliver(blocks, owners):
    devices = N_LON * N_LAT
    onehot = (owners[:, :, None] == jnp.arange(devices, dtype=jnp.int32)[None, None, :]).astype(jnp.int32)
    rank_in = jnp.sum((jnp.cumsum(onehot, axis=1) - onehot) * onehot, axis=2)
    slot_index = (owners * CAP + rank_in).astype(jnp.int32)
    source_ids = jnp.broadcast_to(jnp.arange(devices, dtype=jnp.int32)[:, None], slot_index.shape)
    width = blocks.shape[-1]
    buffers = jnp.zeros((devices, devices * CAP, width), jnp.float32).at[source_ids, slot_index].set(blocks)
    return buffers.reshape(devices, devices, CAP, width).transpose(1, 0, 2, 3).reshape(devices, devices * CAP, width)


def reference(tracers, fill_fraction, ocean_mask, east_speed, north_speed, diffusivity, cell_area, owner_map):
    wet_depth = fill_fraction * ocean_mask.astype(jnp.float32)
    mixing = diffusivity[:, None, None]
    h_east = jnp.roll(wet_depth, -1, axis=-1)
    u_east = jnp.roll(east_speed, -1, axis=-1)
    h_north = jnp.concatenate([wet_depth[:, 1:], jnp.flip(wet_depth[:, -1:], -1)], axis=1)
    v_north = jnp.concatenate([north_speed[:, 1:], -jnp.flip(north_speed[:, -1:], -1)], axis=1)
    volume = cell_area[None] * jnp.maximum(wet_depth, depth_floor)
    results = []
    for tracer_index in range(TRACERS):
        tracer = tracers[tracer_index]
        east_flux = face_flux(tracer, jnp.roll(tracer, -1, axis=-1), wet_depth, h_east, east_speed, u_east, mixing)
        west_flux = jnp.roll(east_flux, 1, axis=-1)
        north_val = jnp.concatenate([tracer[:, 1:], jnp.flip(tracer[:, -1:], -1)], axis=1)
        north_flux = face_flux(tracer, north_val, wet_depth, h_north, north_speed, v_north, mixing)
        south_flux = jnp.concatenate([jnp.zeros_like(north_flux[:, :1]), north_flux[:, :-1]], axis=1)
        results.append(tracer + time_step * ((west_flux - east_flux) + (south_flux - north_flux)) / volume)
    updated = jnp.stack(results, axis=0)
    coarse_two, coarse_four = coarsen(updated, cell_area[None] * wet_depth)
    owners = owner_map.reshape(N_LON * N_LAT, -1)
    received_two = deliver(device_blocks(coarse_two, BAND_ROWS // 2), owners)
    received_four = deliver(device_blocks(coarse_four, BAND_ROWS // 4), owners)
    return updated, received_two, received_four
```

```python
import jax
import jax.numpy as jnp
from jax import lax
from jax.experimental import pallas as pl
from jax.experimental.pallas import tpu as pltpu
from jax.sharding import PartitionSpec as P

time_step = 0.05
depth_floor = 0.25
weight_floor = 0.25

TR, LV = 4, 16
ROWS, LANES = 128, 128
GROUPS = 8
DEV, CAP = 128, 2
CHUNKS = 20
F32, BF16 = jnp.float32, jnp.bfloat16
MIB = 1 << 20


def lane_iota(shape=(8, 128)):
    return lax.broadcasted_iota(jnp.int32, shape, len(shape) - 1)


def sub_iota(shape=(8, 128)):
    return lax.broadcasted_iota(jnp.int32, shape, len(shape) - 2)


def face(lower_h, upper_h, lower_speed, upper_speed, mixing):
    open_depth = jnp.minimum(lower_h, upper_h)
    speed = 0.5 * (lower_speed + upper_speed)
    ahead = jnp.maximum(speed, 0.0)
    back = ahead - speed
    return open_depth * (ahead + mixing), open_depth * (back + mixing)


def split_dot(left, right, split_left=True):
    values = left if split_left else right
    high = values.astype(BF16)
    low = (values - high.astype(F32)).astype(BF16)
    if split_left:
        return jnp.dot(high, right, preferred_element_type=F32) + jnp.dot(
            low, right, preferred_element_type=F32
        )
    return jnp.dot(left, high, preferred_element_type=F32) + jnp.dot(
        left, low, preferred_element_type=F32
    )


def input_copies(hbm, vmem, sems):
    per = LV // GROUPS

    def copies(group):
        levels = pl.ds(group * per, per)
        out = [pltpu.make_async_copy(hbm[0].at[:, levels], vmem[0].at[:, levels], sems.at[0, group])]
        for n in range(1, 5):
            out.append(
                pltpu.make_async_copy(hbm[n].at[levels], vmem[n].at[levels], sems.at[n, group])
            )
        return out

    return copies


def strided(ref, *lead, i):
    return ref[(*lead, pl.ds(i, 8, stride=16), slice(None))]


def level_coefficients(k, mixing, refs, area_ref, coef, visit):
    fill, mask, east, north = refs
    lane, sub = lane_iota(), sub_iota()

    def depth(i):
        return strided(fill, k, i=i) * strided(mask, k, i=i).astype(F32)

    h_first, v_first = depth(0), strided(north, k, i=0)
    h, v = h_first, v_first
    for i in range(16):
        if i < 15:
            h_next, v_next = depth(i + 1), strided(north, k, i=i + 1)
        else:
            h_next, v_next = pltpu.roll(h_first, 7, 0), pltpu.roll(v_first, 7, 0)
        u = strided(east, k, i=i)
        p_e, q_e = face(h, pltpu.roll(h, 127, 1), u, pltpu.roll(u, 127, 1), mixing)
        coef[0, i] = jnp.where(lane < 127, p_e, 0.0)
        coef[1, i] = jnp.where(lane < 127, q_e, 0.0)
        p_n, q_n = face(h, h_next, v, v_next, mixing)
        if i == 15:
            p_n, q_n = jnp.where(sub < 7, p_n, 0.0), jnp.where(sub < 7, q_n, 0.0)
        coef[2, i] = p_n
        coef[3, i] = q_n
        visit(i, h, u, v, strided(area_ref, i=i))
        h, v = h_next, v_next


def interior(k, tracers, coef, visit):
    p15, q15 = coef[2, 15], coef[3, 15]
    cells, south, last = [], [], []
    for t in range(TR):
        first = strided(tracers, t, k, i=0)
        top = strided(tracers, t, k, i=15)
        flux = p15 * top - q15 * pltpu.roll(first, 7, 0)
        cells.append(first)
        last.append(flux)
        south.append(pltpu.roll(flux, 1, 0))
    for i in range(16):
        p_e, q_e = coef[0, i], coef[1, i]
        if i < 15:
            p_n, q_n = coef[2, i], coef[3, i]
        divs, after = [], []
        for t in range(TR):
            cell = cells[t]
            if i < 15:
                nxt = strided(tracers, t, k, i=i + 1)
                north = p_n * cell - q_n * nxt
                after.append(nxt)
            else:
                north = last[t]
            east = p_e * cell - q_e * pltpu.roll(cell, 127, 1)
            divs.append((pltpu.roll(east, 1, 1) - east) + (south[t] - north))
            south[t] = north
        visit(i, cells, divs)
        cells = after


def kernel_first(
    tr, fill, mask, east, north, diff, area, owner,
    sums, weights, ew, ns, placing,
    tr_s, fill_s, mask_s, east_s, north_s, area_s, coef, sems, area_sem,
):
    hbm, vmem = (tr, fill, mask, east, north), (tr_s, fill_s, mask_s, east_s, north_s)
    copies = input_copies(hbm, vmem, sems)
    area_copy = pltpu.make_async_copy(area, area_s, area_sem)
    for group in range(GROUPS):
        for copy in copies(group):
            copy.start()
        if group == 0:
            area_copy.start()
    flip = jnp.where(lax.axis_index("lon") < lax.axis_size("lon") // 2, 0, 1)

    across = lane_iota((DEV, DEV))
    down = sub_iota((DEV, DEV))
    who_row = owner[...]
    who = jnp.sum(jnp.where(down == across, who_row, 0), axis=1, keepdims=True)
    same = jnp.where((who == who_row) & (down < across), 1, 0)
    rank = jnp.sum(same, axis=0, keepdims=True)
    row_of = who_row * CAP + rank
    for part in range(CAP):
        here = jnp.where(down + part * DEV == row_of, 1.0, 0.0).astype(BF16)
        placing[pl.ds(part * DEV, DEV), 0:DEV] = here
        placing[pl.ds(part * DEV, DEV), DEV : 2 * DEV] = here

    area_copy.wait()
    lane = lane_iota()
    per = LV // GROUPS

    def level(k):
        mixing = diff[k]
        rows = pl.ds(pl.multiple_of(k * 8, 8), 8)
        pending = {}

        def seen(i, h, u, v, cell_area):
            w = cell_area * h
            coef[4, i] = w
            coef[5, i] = (time_step * h) / jnp.maximum(h, depth_floor)
            base = 64 * (i % 2)
            packed = ew[16 + i // 2]
            packed = jnp.where(
                (lane >> 1) == k + base // 2, pltpu.roll(h, 2 * k + 1 + base, 1), packed
            )
            packed = jnp.where(
                (lane >> 1) == k + 16 + base // 2, pltpu.roll(u, 2 * k + 33 + base, 1), packed
            )
            ew[16 + i // 2] = packed
            if i == 0:
                ns[1 - flip, pl.ds(64 + k, 1), :] = h[0:1]
                ns[1 - flip, pl.ds(80 + k, 1), :] = v[0:1]
            if i == 15:
                ns[flip, pl.ds(64 + k, 1), :] = h[7:8]
                ns[flip, pl.ds(80 + k, 1), :] = v[7:8]
            if i % 2 == 0:
                pending["w"] = w
            else:
                weights[i // 2, rows, :] = pending["w"] + w

        level_coefficients(k, mixing, (fill_s, mask_s, east_s, north_s), area_s, coef, seen)
        where_t = [(lane >> 1) == t * 16 + k for t in range(TR)]

        def done(i, cells, divs):
            w, g = coef[4, i], coef[5, i]
            packed = ew[i]
            for t in range(TR):
                cell = cells[t]
                packed = jnp.where(where_t[t], pltpu.roll(cell, 2 * k + 32 * t + 1, 1), packed)
                value = w * cell + g * divs[t]
                if i == 0:
                    ns[1 - flip, pl.ds(t * 16 + k, 1), :] = cell[0:1]
                if i == 15:
                    ns[flip, pl.ds(t * 16 + k, 1), :] = cell[7:8]
                if i % 2 == 0:
                    pending[t] = value
                else:
                    sums[t, i // 2, rows, :] = pending[t] + value
            ew[i] = packed

        interior(k, tr_s, coef, done)

    def group_body(group, carry):
        for copy in copies(group):
            copy.wait()
        for n in range(per):
            level(group * per + n)
        return carry

    lax.fori_loop(0, GROUPS, group_body, 0)


def kernel_first_call(tracers, fill, mask, east, north, diff, area, owner):
    any_spec = pl.BlockSpec(memory_space=pltpu.HBM)
    vmem = pl.BlockSpec(memory_space=pltpu.VMEM)
    return pl.pallas_call(
        kernel_first,
        name="first",
        out_shape=(
            jax.ShapeDtypeStruct((TR, 8, 128, 128), F32),
            jax.ShapeDtypeStruct((8, 128, 128), F32),
            jax.ShapeDtypeStruct((24, 8, 128), F32),
            jax.ShapeDtypeStruct((2, 96, 128), F32),
            jax.ShapeDtypeStruct((CAP * DEV, 2 * DEV), BF16),
        ),
        in_specs=[any_spec] * 5
        + [pl.BlockSpec(memory_space=pltpu.SMEM), any_spec, vmem],
        out_specs=(vmem,) * 5,
        scratch_shapes=[
            pltpu.VMEM((TR, LV, ROWS, LANES), F32),
            pltpu.VMEM((LV, ROWS, LANES), F32),
            pltpu.VMEM((LV, ROWS, LANES), jnp.int32),
            pltpu.VMEM((LV, ROWS, LANES), F32),
            pltpu.VMEM((LV, ROWS, LANES), F32),
            pltpu.VMEM((ROWS, LANES), F32),
            pltpu.VMEM((6, 16, 8, 128), F32),
            pltpu.SemaphoreType.DMA((5, GROUPS)),
            pltpu.SemaphoreType.DMA,
        ],
        compiler_params=pltpu.CompilerParams(vmem_limit_bytes=24 * MIB),
        cost_estimate=pl.CostEstimate(flops=60_000_000, bytes_accessed=11 * MIB, transcendentals=0),
    )(tracers, fill, mask, east, north, diff, area, owner)


def spread(values, offset):
    index = (lane_iota() & 31) + offset
    return jnp.take_along_axis(values, index, axis=1)


def kernel_second(
    sums, weights, ew, from_east, from_west, ns, got_fwd, got_bwd, diff, placing,
    send, d_ew, d_ns,
    work, acc, chunks,
):
    lane, sub = lane_iota(), sub_iota()
    flip = jnp.where(lax.axis_index("lon") < lax.axis_size("lon") // 2, 0, 1)
    at_fold = lax.axis_index("lat") == lax.axis_size("lat") - 1
    is_east = (lane & 1) == 0
    level_of = (lane >> 1) & 15
    mixing = jnp.zeros((8, 128), F32)
    for k in range(LV):
        mixing = jnp.where(level_of == k, diff[k], mixing)

    def neighbour(n):
        return jnp.where(
            is_east, pltpu.roll(from_east[n], 127, 1), pltpu.roll(from_west[n], 1, 1)
        )

    pending = None
    for i in range(16):
        own_hu, near_hu = ew[16 + i // 2], neighbour(16 + i // 2)
        base = 64 * (i % 2)
        h = spread(own_hu, base)
        p, q = face(
            h, spread(near_hu, base), spread(own_hu, base + 32), spread(near_hu, base + 32), mixing
        )
        div = jnp.where(is_east, q, p) * neighbour(i) - jnp.where(is_east, p, q) * ew[i]
        d_ew[i] = div
        value = (time_step * h) / jnp.maximum(h, depth_floor) * div
        if i % 2 == 0:
            pending = value
        else:
            work[i // 2] = pending + value

    ends = (lane == 0) | (lane == 127)

    def add_ends(k, carry):
        rows = pl.ds(pl.multiple_of(k * 8, 8), 8)
        for t in range(TR):
            for pair in range(8):
                at = (t, pair, rows, slice(None))
                moved = pltpu.roll(work[pair], 127 - 2 * k + (128 - 32 * t), 1)
                acc[at] = sums[at] + jnp.where(ends, moved, 0.0)
        return carry

    lax.fori_loop(0, LV, add_ends, 0)

    back = 127 - lane
    for half in range(2):
        rows = pl.ds(8 * half, 8)
        levels = sub + 8 * half
        mix = jnp.zeros((8, 128), F32)
        for k in range(8):
            mix = jnp.where(sub == k, diff[8 * half + k], mix)

        def far(ref, n, sign=None):
            value = ref[pl.ds(n * 16 + 8 * half, 8), :]
            turned = jnp.take_along_axis(value, back, axis=1)
            if sign is not None:
                turned = -turned
            return jnp.where(at_fold, turned, value)

        for side in range(2):
            own = lambda n: ns[flip if side == 0 else 1 - flip, pl.ds(n * 16 + 8 * half, 8), :]
            if side == 0:
                near = lambda n, sign=None: jnp.where(
                    flip == 1, far(got_fwd, n, sign), far(got_bwd, n, sign)
                )
            else:
                near = lambda n, sign=None: jnp.where(
                    flip == 1,
                    got_bwd[pl.ds(n * 16 + 8 * half, 8), :],
                    got_fwd[pl.ds(n * 16 + 8 * half, 8), :],
                )
            h = own(4)
            p, q = face(h, near(4), own(5), near(5, -1), mix)
            gain = (time_step * h) / jnp.maximum(h, depth_floor)
            for t in range(TR):
                if side == 0:
                    div = q * near(t) - p * own(t)
                    at = (t, 7, pl.ds(64 * half + 7, 8, stride=8), slice(None))
                else:
                    div = p * near(t) - q * own(t)
                    at = (t, 0, pl.ds(64 * half, 8, stride=8), slice(None))
                d_ns[side, pl.ds(t * 16 + 8 * half, 8), :] = div
                acc[at] = acc[at] + gain * div

    source = sub_iota((256, 128))
    target = lane_iota((256, 128))
    pool = jnp.where(target == (source >> 7) * 64 + ((source & 127) >> 1), 1.0, 0.0).astype(BF16)
    source = sub_iota((128, 128))
    target = lane_iota((128, 128))
    quarter = [
        jnp.where(target == j * 32 + ((source & 63) >> 1), 1.0, 0.0).astype(BF16) for j in range(4)
    ]

    def both_rows(ref, *lead, j):
        return jnp.concatenate([ref[(*lead, 2 * j)], ref[(*lead, 2 * j + 1)]], axis=1)

    def keep(n, values):
        high = values.astype(BF16)
        chunks[0:128, pl.ds(n * 128, 128)] = high
        chunks[128:256, pl.ds(n * 128, 128)] = (values - high.astype(F32)).astype(BF16)

    gains = []
    den4 = jnp.zeros((128, 128), F32)
    for j in range(4):
        den2 = split_dot(both_rows(weights, j=j), pool)
        gains.append(1.0 / jnp.maximum(den2, weight_floor))
        den4 = den4 + split_dot(den2, quarter[j])
    gain4 = 1.0 / jnp.maximum(den4, weight_floor)
    for t in range(TR):
        num4 = jnp.zeros((128, 128), F32)
        for j in range(4):
            num2 = split_dot(both_rows(acc, t, j=j), pool)
            keep(t * 4 + j, num2 * gains[j])
            num4 = num4 + split_dot(num2, quarter[j])
        keep(16 + t, num4 * gain4)

    for n in range(CHUNKS // 2):
        placed = jnp.dot(
            placing[...], chunks[:, pl.ds(n * 256, 256)], preferred_element_type=F32
        )
        for part in range(2):
            for m in range(32):
                send[pl.ds(m * 8 * CHUNKS + 2 * n + part, 8, stride=CHUNKS), :] = placed[
                    m * 8 : m * 8 + 8, part * 128 : part * 128 + 128
                ]


def kernel_second_call(*args):
    vmem = pl.BlockSpec(memory_space=pltpu.VMEM)
    return pl.pallas_call(
        kernel_second,
        name="second",
        out_shape=(
            jax.ShapeDtypeStruct((DEV * CAP * CHUNKS, 128), F32),
            jax.ShapeDtypeStruct((16, 8, 128), F32),
            jax.ShapeDtypeStruct((2, 64, 128), F32),
        ),
        in_specs=[vmem] * 8 + [pl.BlockSpec(memory_space=pltpu.SMEM), vmem],
        out_specs=(vmem,) * 3,
        scratch_shapes=[
            pltpu.VMEM((8, 8, 128), F32),
            pltpu.VMEM((TR, 8, 128, 128), F32),
            pltpu.VMEM((256, 2560), BF16),
        ],
        compiler_params=pltpu.CompilerParams(vmem_limit_bytes=16 * MIB),
        cost_estimate=pl.CostEstimate(flops=60_000_000, bytes_accessed=6 * MIB, transcendentals=0),
    )(*args)


def kernel_third(
    tr, fill, mask, east, north, diff, area, d_ew, d_ns,
    out,
    tr_s, fill_s, mask_s, east_s, north_s, area_s, out_s, coef, sems, area_sem, out_sems,
):
    hbm, vmem = (tr, fill, mask, east, north), (tr_s, fill_s, mask_s, east_s, north_s)
    copies = input_copies(hbm, vmem, sems)
    area_copy = pltpu.make_async_copy(area, area_s, area_sem)
    for group in range(GROUPS):
        for copy in copies(group):
            copy.start()
        if group == 0:
            area_copy.start()
    area_copy.wait()
    lane, sub = lane_iota(), sub_iota()
    ends = (lane == 0) | (lane == 127)
    per = LV // GROUPS

    def out_copy(group):
        levels = pl.ds(group * per, per)
        return pltpu.make_async_copy(out_s.at[:, levels], out.at[:, levels], out_sems.at[group])

    def level(k):
        mixing = diff[k]

        def seen(i, h, u, v, cell_area):
            coef[4, i] = time_step / (cell_area * jnp.maximum(h, depth_floor))

        level_coefficients(k, mixing, (fill_s, mask_s, east_s, north_s), area_s, coef, seen)

        def done(i, cells, divs):
            rate = coef[4, i]
            edge = d_ew[i]
            for t in range(TR):
                moved = pltpu.roll(edge, 127 - 2 * k + (128 - 32 * t), 1)
                div = divs[t] + jnp.where(ends, moved, 0.0)
                if i == 0:
                    div = div + jnp.where(sub == 0, d_ns[1, pl.ds(t * 16 + k, 1), :], 0.0)
                if i == 15:
                    div = div + jnp.where(sub == 7, d_ns[0, pl.ds(t * 16 + k, 1), :], 0.0)
                out_s[t, k, pl.ds(i, 8, stride=16), :] = cells[t] + rate * div

        interior(k, tr_s, coef, done)

    def group_body(group, carry):
        for copy in copies(group):
            copy.wait()
        for n in range(per):
            level(group * per + n)
        out_copy(group).start()
        return carry

    lax.fori_loop(0, GROUPS, group_body, 0)
    for group in range(GROUPS):
        out_copy(group).wait()


def kernel_third_call(tracers, fill, mask, east, north, diff, area, d_ew, d_ns):
    any_spec = pl.BlockSpec(memory_space=pltpu.HBM)
    vmem = pl.BlockSpec(memory_space=pltpu.VMEM)
    return pl.pallas_call(
        kernel_third,
        name="third",
        out_shape=jax.ShapeDtypeStruct((TR, LV, ROWS, LANES), F32),
        in_specs=[any_spec] * 5
        + [pl.BlockSpec(memory_space=pltpu.SMEM), any_spec, vmem, vmem],
        out_specs=any_spec,
        scratch_shapes=[
            pltpu.VMEM((TR, LV, ROWS, LANES), F32),
            pltpu.VMEM((LV, ROWS, LANES), F32),
            pltpu.VMEM((LV, ROWS, LANES), jnp.int32),
            pltpu.VMEM((LV, ROWS, LANES), F32),
            pltpu.VMEM((LV, ROWS, LANES), F32),
            pltpu.VMEM((ROWS, LANES), F32),
            pltpu.VMEM((TR, LV, ROWS, LANES), F32),
            pltpu.VMEM((5, 16, 8, 128), F32),
            pltpu.SemaphoreType.DMA((5, GROUPS)),
            pltpu.SemaphoreType.DMA,
            pltpu.SemaphoreType.DMA((GROUPS,)),
        ],
        compiler_params=pltpu.CompilerParams(vmem_limit_bytes=24 * MIB),
        cost_estimate=pl.CostEstimate(flops=60_000_000, bytes_accessed=12 * MIB, transcendentals=0),
    )(tracers, fill, mask, east, north, diff, area, d_ew, d_ns)


SPLITS = 4


def kernel_last(got, two, four):
    for m in range(32 // SPLITS):
        for n in range(CHUNKS):
            value = got[pl.ds(m * 8 * CHUNKS + n, 8, stride=CHUNKS), :]
            if n < 16:
                two[pl.ds(m * 8, 8), pl.ds(n * 128, 128)] = value
            else:
                four[pl.ds(m * 8, 8), pl.ds((n - 16) * 128, 128)] = value


def kernel_last_call(got):
    return pl.pallas_call(
        kernel_last,
        name="last",
        grid=(SPLITS,),
        out_shape=(
            jax.ShapeDtypeStruct((DEV * CAP, 2048), F32),
            jax.ShapeDtypeStruct((DEV * CAP, 512), F32),
        ),
        in_specs=[pl.BlockSpec((DEV * 40 // SPLITS, 128), lambda s: (s, 0))],
        out_specs=(
            pl.BlockSpec((DEV * CAP // SPLITS, 2048), lambda s: (s, 0)),
            pl.BlockSpec((DEV * CAP // SPLITS, 512), lambda s: (s, 0)),
        ),
        compiler_params=pltpu.CompilerParams(vmem_limit_bytes=8 * MIB),
    )(got)


def local(
    tracers, fill_fraction, ocean_mask, east_speed, north_speed, diffusivity, cell_area, owner_map
):
    lon_count = lax.axis_size("lon")
    lat_count = lax.axis_size("lat")
    *fields, diffusivity, cell_area = (
        pltpu.with_memory_space_constraint(x, pltpu.HBM)
        for x in (
            tracers, fill_fraction, ocean_mask, east_speed, north_speed, diffusivity, cell_area
        )
    )
    sums, weights, ew, ns, placing = kernel_first_call(
        *fields, diffusivity, cell_area, owner_map.reshape(1, DEV)
    )
    ring = [(i, (i + 1) % lon_count) for i in range(lon_count)]
    from_west = lax.ppermute(ew, "lon", ring)
    from_east = lax.ppermute(ew, "lon", [(b, a) for a, b in ring])
    chain = []
    for low in range(lon_count // 2):
        high = lon_count - 1 - low
        up = [low * lat_count + a for a in range(lat_count)]
        path = up + [high * lat_count + a for a in reversed(range(lat_count))]
        chain += list(zip(path[:-1], path[1:]))
    both = ("lon", "lat")
    got_fwd = lax.ppermute(ns[0], both, chain)
    got_bwd = lax.ppermute(ns[1], both, [(b, a) for a, b in chain])
    send, d_ew, d_ns = kernel_second_call(
        sums, weights, ew, from_east, from_west, ns, got_fwd, got_bwd, diffusivity, placing
    )
    got = lax.all_to_all(
        send.reshape(DEV, CAP * CHUNKS, 128), both, split_axis=0, concat_axis=0, tiled=True
    )
    updated = kernel_third_call(*fields, diffusivity, cell_area, d_ew, d_ns)
    two, four = kernel_last_call(got.reshape(DEV * CAP * CHUNKS, 128))
    return (updated, two[None], four[None])


def solution(mesh):
    in_specs = (
        P(None, None, "lat", "lon"),
        P(None, "lat", "lon"),
        P(None, "lat", "lon"),
        P(None, "lat", "lon"),
        P(None, "lat", "lon"),
        P(),
        P("lat", "lon"),
        P(("lon", "lat"), None),
    )
    out_specs = (
        P(None, None, "lat", "lon"),
        P(("lon", "lat"), None, None),
        P(("lon", "lat"), None, None),
    )
    return jax.shard_map(local, mesh=mesh, in_specs=in_specs, out_specs=out_specs, check_vma=False)
```

```python
import jax
import jax.numpy as jnp
from jax import lax
from jax.experimental import pallas as pl
from jax.experimental.pallas import tpu as pltpu
from jax.sharding import PartitionSpec as P


time_step = 0.05
depth_floor = 0.25
weight_floor = 0.25

TR, LV = 4, 16
ROWS, LANES = 128, 128
GROUPS = 8
DEV, CAP = 128, 2
CHUNKS = 20
PARTS = 2
F32, BF16 = jnp.float32, jnp.bfloat16
MIB = 1 << 20


def lane_iota(shape=(8, 128)):
    return lax.broadcasted_iota(jnp.int32, shape, len(shape) - 1)


def sub_iota(shape=(8, 128)):
    return lax.broadcasted_iota(jnp.int32, shape, len(shape) - 2)


def face(lower_h, upper_h, lower_speed, upper_speed, mixing, keep=None):
    open_depth = jnp.minimum(lower_h, upper_h)
    if keep is not None:
        open_depth = jnp.where(keep, open_depth, 0.0)
    speed = 0.5 * (lower_speed + upper_speed)
    ahead = jnp.maximum(speed, 0.0)
    back = ahead - speed
    return open_depth * (ahead + mixing), open_depth * (back + mixing)


def halves(values):
    high = values.astype(BF16)
    return high, (values - high.astype(F32)).astype(BF16)


def split_dot(left, right):
    high, low = halves(left)
    return jnp.dot(high, right, preferred_element_type=F32) + jnp.dot(
        low, right, preferred_element_type=F32
    )


def input_copies(hbm, vmem, sems):
    per = LV // GROUPS

    def copies(group):
        levels = pl.ds(group * per, per)
        out = [pltpu.make_async_copy(hbm[0].at[:, levels], vmem[0].at[:, levels], sems.at[0, group])]
        for n in range(1, 5):
            out.append(
                pltpu.make_async_copy(hbm[n].at[levels], vmem[n].at[levels], sems.at[n, group])
            )
        return out

    return copies


def row_set(start):
    return (pl.ds(start, 8, stride=4), slice(None))


def kernel_rows(tr, fill, mask, north, ns_fwd, ns_bwd, tr_s, fill_s, mask_s, north_s, sems):
    copies = []
    for n, (src, dst) in enumerate(((tr, tr_s), (fill, fill_s), (mask, mask_s), (north, north_s))):
        for side in range(2):
            rows = pl.ds(side * (ROWS - 8), 8)
            if n == 0:
                copies.append(
                    pltpu.make_async_copy(src.at[:, :, rows], dst.at[side], sems.at[n, side])
                )
            else:
                copies.append(
                    pltpu.make_async_copy(src.at[:, rows], dst.at[side], sems.at[n, side])
                )
            copies[-1].start()
    for copy in copies:
        copy.wait()
    flip = lax.axis_index("lon") >= lax.axis_size("lon") // 2
    for n in range(6):
        for half in range(2):
            levels = range(8 * half, 8 * half + 8)
            lines = []
            for side in range(2):
                row = 7 * side
                pick = lambda ref, k: ref[side, k, pl.ds(row, 1), :]
                if n < TR:
                    parts = [tr_s[side, n, k, pl.ds(row, 1), :] for k in levels]
                elif n == TR:
                    parts = [pick(fill_s, k) * pick(mask_s, k).astype(F32) for k in levels]
                else:
                    parts = [pick(north_s, k) for k in levels]
                lines.append(jnp.concatenate(parts, axis=0))
            at = pl.ds(n * 16 + 8 * half, 8)
            ns_fwd[at, :] = jnp.where(flip, lines[0], lines[1])
            ns_bwd[at, :] = jnp.where(flip, lines[1], lines[0])


def kernel_rows_call(tracers, fill, mask, north):
    hbm = pl.BlockSpec(memory_space=pltpu.HBM)
    vmem = pl.BlockSpec(memory_space=pltpu.VMEM)
    return pl.pallas_call(
        kernel_rows,
        name="rows",
        out_shape=(jax.ShapeDtypeStruct((96, 128), F32),) * 2,
        in_specs=[hbm] * 4,
        out_specs=(vmem,) * 2,
        scratch_shapes=[
            pltpu.VMEM((2, TR, LV, 8, LANES), F32),
            pltpu.VMEM((2, LV, 8, LANES), F32),
            pltpu.VMEM((2, LV, 8, LANES), jnp.int32),
            pltpu.VMEM((2, LV, 8, LANES), F32),
            pltpu.SemaphoreType.DMA((4, 2)),
        ],
        compiler_params=pltpu.CompilerParams(vmem_limit_bytes=4 * MIB),
        cost_estimate=pl.CostEstimate(flops=1_000_000, bytes_accessed=MIB, transcendentals=0),
    )(tracers, fill, mask, north)


def kernel_first(
    tr, fill, mask, east, north, diff, area, owner,
    num2, den2, ew, placing,
    tr_s, fill_s, mask_s, east_s, north_s, area_s, owner_s, even_s, odd_s, sems, area_sem, owner_sem,
):
    hbm, vmem = (tr, fill, mask, east, north), (tr_s, fill_s, mask_s, east_s, north_s)
    copies = input_copies(hbm, vmem, sems)
    area_copy = pltpu.make_async_copy(area, area_s, area_sem)
    owner_copy = pltpu.make_async_copy(owner, owner_s, owner_sem)
    owner_copy.start()
    for group in range(GROUPS):
        for copy in copies(group):
            copy.start()
        if group == 0:
            area_copy.start()

    across = lane_iota((DEV, DEV))
    down = sub_iota((DEV, DEV))
    source = sub_iota((256, 128))
    target = lane_iota((256, 128))
    pool = jnp.where(target == (source >> 7) * 64 + ((source & 127) >> 1), 1.0, 0.0).astype(BF16)
    owner_copy.wait()
    who_row = owner_s[...]
    who = jnp.sum(jnp.where(down == across, who_row, 0), axis=1, keepdims=True)
    same = jnp.where((who == who_row) & (down < across), 1, 0)
    rank = jnp.sum(same, axis=0, keepdims=True)
    row_of = who_row * CAP + rank
    for part in range(CAP):
        here = jnp.where(down + part * DEV == row_of, 1.0, 0.0).astype(BF16)
        placing[pl.ds(part * DEV, DEV), 0:DEV] = here
        placing[pl.ds(part * DEV, DEV), DEV : 2 * DEV] = here

    area_copy.wait()
    lane, sub = lane_iota(), sub_iota()
    is_even = (lane & 1) == 0
    not_last = lane < 127
    not_top = sub < 7
    swap = jnp.where(is_even, lane + 127, lane + 1) & 127

    def level(k, store):
        mixing = diff[k]

        def load(ref, start):
            return ref[(k, *row_set(start))]

        def depth(start):
            return load(fill_s, start) * load(mask_s, start).astype(F32)

        def north_face(q, h, v):
            if q < 3:
                return face(h, depth(32 * q + 4), v, load(north_s, 32 * q + 4), mixing)
            h_up, v_up = pltpu.roll(depth(96), 7, 0), pltpu.roll(load(north_s, 96), 7, 0)
            return face(h, h_up, v, v_up, mixing, keep=not_top)

        where_t = [(lane >> 1) == t * 16 + k for t in range(TR)]
        before = jnp.zeros((8, 128), F32), jnp.zeros((8, 128), F32)
        for q in range(4):
            hs = [depth(32 * q + j) for j in range(4)]
            vs = [load(north_s, 32 * q + j) for j in range(4)]
            norths = [face(hs[j], hs[j + 1], vs[j], vs[j + 1], mixing) for j in range(3)]
            norths.append(north_face(q, hs[3], vs[3]))
            turned = tuple(pltpu.roll(x, 1, 0) for x in norths[3])
            south = tuple(jnp.where(sub > 0, a, b) for a, b in zip(turned, before))
            before = turned
            centre, cross, gain_n, gain_s, weights = [], [], [], [], []
            for j in range(4):
                v = 4 * q + j
                h = hs[j]
                u = load(east_s, 32 * q + j)
                base = 64 * (v % 2)
                packed = ew[16 + v // 2]
                packed = jnp.where(
                    (lane >> 1) == k + base // 2, pltpu.roll(h, 2 * k + 1 + base, 1), packed
                )
                ew[16 + v // 2] = jnp.where(
                    (lane >> 1) == k + 16 + base // 2, pltpu.roll(u, 2 * k + 33 + base, 1), packed
                )
                w = area_s[row_set(32 * q + j)] * h
                g = (time_step * h) / jnp.maximum(h, depth_floor)
                p_e, q_e = face(
                    h, pltpu.roll(h, 127, 1), u, pltpu.roll(u, 127, 1), mixing, keep=not_last
                )
                q_w = pltpu.roll(q_e, 1, 1)
                p_n, q_n = norths[j]
                p_s, q_s = norths[j - 1] if j else south
                to_west = pltpu.roll(g, 1, 1) * q_w
                to_east = pltpu.roll(g, 127, 1) * p_e
                own = w - g * ((p_e + q_w) + (p_n + q_s))
                centre.append(own + jnp.where(is_even, to_east, to_west))
                cross.append(jnp.where(is_even, to_west, to_east))
                gain_n.append(g * q_n)
                gain_s.append(g * p_s)
                weights.append(w)
            for j in range(4):
                packed = ew[4 * q + j]
                for t in range(TR):
                    cell = tr_s[(t, k, *row_set(32 * q + j))]
                    packed = jnp.where(where_t[t], pltpu.roll(cell, 2 * k + 32 * t + 1, 1), packed)
                ew[4 * q + j] = packed
            first = [centre[2 * par] + gain_s[2 * par + 1] for par in range(2)]
            second = [centre[2 * par + 1] + gain_n[2 * par] for par in range(2)]
            for t in range(TR):
                cells = [tr_s[(t, k, *row_set(32 * q + j))] for j in range(4)]
                if q:
                    below = tr_s[(t, k, *row_set(32 * q - 1))]
                else:
                    below = pltpu.roll(cells[3], 1, 0)
                if q < 3:
                    above = tr_s[(t, k, *row_set(32 * q + 4))]
                else:
                    above = pltpu.roll(cells[0], 7, 0)
                around = [below, *cells, above]
                for par in range(2):
                    low, a, b, high = around[2 * par : 2 * par + 4]
                    value = (first[par] * a + second[par] * b) + (
                        gain_s[2 * par] * low + gain_n[2 * par + 1] * high
                    )
                    side = cross[2 * par] * a + cross[2 * par + 1] * b
                    value = value + jnp.take_along_axis(side, swap, axis=1)
                    store[pl.ds(t * 32 + q * 8, 8), pl.ds(par * 128, 128)] = value
            for par in range(2):
                store[pl.ds(128 + q * 8, 8), pl.ds(par * 128, 128)] = (
                    weights[2 * par] + weights[2 * par + 1]
                )

    def pooled(k, store):
        values = split_dot(store[...], pool)
        rows = pl.ds(pl.multiple_of(k * 32, 32), 32)
        for t in range(TR):
            num2[t, rows, :] = values[t * 32 : t * 32 + 32]
        den2[rows, :] = values[128:160]

    def group_body(group, carry):
        for copy in copies(group):
            copy.wait()
        pooled((group * 2 + LV - 1) % LV, odd_s)
        level(group * 2, even_s)
        pooled(group * 2, even_s)
        level(group * 2 + 1, odd_s)
        return carry

    odd_s[...] = jnp.zeros_like(odd_s)
    lax.fori_loop(0, GROUPS, group_body, 0)
    pooled(LV - 1, odd_s)


def kernel_first_call(tracers, fill, mask, east, north, diff, area, owner):
    hbm = pl.BlockSpec(memory_space=pltpu.HBM)
    vmem = pl.BlockSpec(memory_space=pltpu.VMEM)
    return pl.pallas_call(
        kernel_first,
        name="first",
        out_shape=(
            jax.ShapeDtypeStruct((TR, 512, 128), F32),
            jax.ShapeDtypeStruct((512, 128), F32),
            jax.ShapeDtypeStruct((24, 8, 128), F32),
            jax.ShapeDtypeStruct((CAP * DEV, 2 * DEV), BF16),
        ),
        in_specs=[hbm] * 5 + [pl.BlockSpec(memory_space=pltpu.SMEM), hbm, hbm],
        out_specs=(vmem,) * 4,
        scratch_shapes=[
            pltpu.VMEM((TR, LV, ROWS, LANES), F32),
            pltpu.VMEM((LV, ROWS, LANES), F32),
            pltpu.VMEM((LV, ROWS, LANES), jnp.int32),
            pltpu.VMEM((LV, ROWS, LANES), F32),
            pltpu.VMEM((LV, ROWS, LANES), F32),
            pltpu.VMEM((ROWS, LANES), F32),
            pltpu.VMEM((1, DEV), jnp.int32),
            pltpu.VMEM((160, 256), F32),
            pltpu.VMEM((160, 256), F32),
            pltpu.SemaphoreType.DMA((5, GROUPS)),
            pltpu.SemaphoreType.DMA,
            pltpu.SemaphoreType.DMA,
        ],
        compiler_params=pltpu.CompilerParams(vmem_limit_bytes=24 * MIB),
        cost_estimate=pl.CostEstimate(flops=60_000_000, bytes_accessed=11 * MIB, transcendentals=0),
    )(tracers, fill, mask, east, north, diff, area, owner)


def spread(values, offset):
    index = (lane_iota() & 31) + offset
    return jnp.take_along_axis(values, index, axis=1)


def kernel_second(
    num2, den2, ew, from_east, from_west, ns_fwd, ns_bwd, got_fwd, got_bwd, diff, placing,
    send, d_ew, d_ns,
    work, acc, chunks, send_s, sems,
):
    lane, sub = lane_iota(), sub_iota()
    flip = lax.axis_index("lon") >= lax.axis_size("lon") // 2
    at_fold = lax.axis_index("lat") == lax.axis_size("lat") - 1
    is_east = (lane & 1) == 0
    level_of = (lane >> 1) & 15
    mixing = jnp.zeros((8, 128), F32)
    for k in range(LV):
        mixing = jnp.where(level_of == k, diff[k], mixing)

    def neighbour(n):
        return jnp.where(
            is_east, pltpu.roll(from_east[n], 127, 1), pltpu.roll(from_west[n], 1, 1)
        )

    pending = None
    for v in range(16):
        own_hu, near_hu = ew[16 + v // 2], neighbour(16 + v // 2)
        base = 64 * (v % 2)
        h = spread(own_hu, base)
        p, q = face(
            h, spread(near_hu, base), spread(own_hu, base + 32), spread(near_hu, base + 32), mixing
        )
        div = jnp.where(is_east, q, p) * neighbour(v) - jnp.where(is_east, p, q) * ew[v]
        d_ew[v] = div
        value = (time_step * h) / jnp.maximum(h, depth_floor) * div
        if v % 2 == 0:
            pending = value
        else:
            value = pending + value
            work[v // 2] = jnp.where(is_east, value, pltpu.roll(value, 64, 1))

    low_ends = (lane == 0) | (lane == 63)
    high_ends = (lane == 64) | (lane == 127)

    def add_ends(k, carry):
        for t in range(TR):
            for q in range(4):
                rows = pl.ds(pl.multiple_of(k * 32 + q * 8, 8), 8)
                shift = 127 - 2 * k + (128 - 32 * t)
                low = pltpu.roll(work[2 * q], shift - 64, 1)
                high = pltpu.roll(work[2 * q + 1], shift, 1)
                edge = jnp.where(low_ends, low, jnp.where(high_ends, high, 0.0))
                acc[t, rows, :] = num2[t, rows, :] + edge
        return carry

    lax.fori_loop(0, LV, add_ends, 0)

    source = sub_iota((128, 128))
    target = lane_iota((128, 128))
    pools = [
        jnp.where(target == par * 64 + (source >> 1), 1.0, 0.0).astype(BF16) for par in range(2)
    ]
    quarter = [
        jnp.where(target == j * 32 + ((source & 63) >> 1), 1.0, 0.0).astype(BF16) for j in range(4)
    ]

    back = 127 - lane
    for half in range(2):
        mix = jnp.zeros((8, 128), F32)
        for k in range(8):
            mix = jnp.where(sub == k, diff[8 * half + k], mix)

        def rows_of(ref, n):
            return ref[pl.ds(n * 16 + 8 * half, 8), :]

        def own(n, top):
            pair = (ns_bwd, ns_fwd) if top else (ns_fwd, ns_bwd)
            return jnp.where(flip, rows_of(pair[0], n), rows_of(pair[1], n))

        def near(n, top, sign=1.0):
            if not top:
                return jnp.where(flip, rows_of(got_bwd, n), rows_of(got_fwd, n))
            value = jnp.where(flip, rows_of(got_fwd, n), rows_of(got_bwd, n))
            turned = sign * jnp.take_along_axis(value, back, axis=1)
            return jnp.where(at_fold, turned, value)

        for top in (False, True):
            h = own(4, top)
            p, q = face(h, near(4, top), own(5, top), near(5, top, -1.0), mix)
            gain = (time_step * h) / jnp.maximum(h, depth_floor)
            for t in range(TR):
                if top:
                    div = q * near(t, top) - p * own(t, top)
                else:
                    div = p * near(t, top) - q * own(t, top)
                d_ns[int(top), pl.ds(t * 16 + 8 * half, 8), :] = div
                at = (t, pl.ds(256 * half + 31 * int(top), 8, stride=32), slice(None))
                acc[at] = acc[at] + split_dot(gain * div, pools[int(top)])

    def keep(n, values):
        high, low = halves(values)
        chunks[0:128, pl.ds(n * 128, 128)] = high
        chunks[128:256, pl.ds(n * 128, 128)] = low

    def every_fourth(ref, *lead, j):
        return jnp.concatenate(
            [ref[(*lead, pl.ds(32 * m + j, 8, stride=4), slice(None))] for m in range(16)], axis=0
        )

    gains = []
    den4 = jnp.zeros((128, 128), F32)
    for j in range(4):
        den = every_fourth(den2, j=j)
        gains.append(1.0 / jnp.maximum(den, weight_floor))
        den4 = den4 + split_dot(den, quarter[j])
    gain4 = 1.0 / jnp.maximum(den4, weight_floor)
    for t in range(TR):
        num4 = jnp.zeros((128, 128), F32)
        for j in range(4):
            num = every_fourth(acc, t, j=j)
            keep(t * 4 + j, num * gains[j])
            num4 = num4 + split_dot(num, quarter[j])
        keep(16 + t, num4 * gain4)

    each = CAP * DEV // PARTS
    copies = []
    for part in range(PARTS):
        left = placing[pl.ds(part * each, each), :]
        for n in range(CHUNKS // 2):
            placed = jnp.dot(left, chunks[:, pl.ds(n * 256, 256)], preferred_element_type=F32)
            for c in range(2):
                for m in range(each // 8):
                    start = (part * each + m * 8) * CHUNKS + 2 * n + c
                    send_s[pl.ds(start, 8, stride=CHUNKS), :] = placed[
                        m * 8 : m * 8 + 8, c * 128 : c * 128 + 128
                    ]
        rows = pl.ds(part * each * CHUNKS, each * CHUNKS)
        copies.append(pltpu.make_async_copy(send_s.at[rows], send.at[rows], sems.at[part]))
        copies[-1].start()
    for copy in copies:
        copy.wait()


def kernel_second_call(*args):
    vmem = pl.BlockSpec(memory_space=pltpu.VMEM)
    return pl.pallas_call(
        kernel_second,
        name="second",
        out_shape=(
            pltpu.HBM((DEV * CAP * CHUNKS, 128), F32),
            jax.ShapeDtypeStruct((16, 8, 128), F32),
            jax.ShapeDtypeStruct((2, 64, 128), F32),
        ),
        in_specs=[vmem] * 9 + [pl.BlockSpec(memory_space=pltpu.SMEM), vmem],
        out_specs=(pl.BlockSpec(memory_space=pltpu.HBM), vmem, vmem),
        scratch_shapes=[
            pltpu.VMEM((8, 8, 128), F32),
            pltpu.VMEM((TR, 512, 128), F32),
            pltpu.VMEM((256, 2560), BF16),
            pltpu.VMEM((DEV * CAP * CHUNKS, 128), F32),
            pltpu.SemaphoreType.DMA((PARTS,)),
        ],
        compiler_params=pltpu.CompilerParams(vmem_limit_bytes=16 * MIB),
        cost_estimate=pl.CostEstimate(flops=60_000_000, bytes_accessed=6 * MIB, transcendentals=0),
    )(*args)


def kernel_third(
    tr, fill, mask, east, north, diff, area, d_ew, d_ns,
    out,
    tr_s, fill_s, mask_s, east_s, north_s, area_s, out_s, sems, area_sem, out_sems,
):
    hbm, vmem = (tr, fill, mask, east, north), (tr_s, fill_s, mask_s, east_s, north_s)
    copies = input_copies(hbm, vmem, sems)
    area_copy = pltpu.make_async_copy(area, area_s, area_sem)
    for group in range(GROUPS):
        for copy in copies(group):
            copy.start()
        if group == 0:
            area_copy.start()
    area_copy.wait()
    lane, sub = lane_iota(), sub_iota()
    ends = (lane == 0) | (lane == 127)
    not_last, not_top = lane < 127, sub < 7
    per = LV // GROUPS

    def out_copy(group):
        levels = pl.ds(group * per, per)
        return pltpu.make_async_copy(out_s.at[:, levels], out.at[:, levels], out_sems.at[group])

    def level(k):
        mixing = diff[k]

        def load(ref, start):
            return ref[(k, *row_set(start))]

        def depth(start):
            return load(fill_s, start) * load(mask_s, start).astype(F32)

        before = [jnp.zeros((8, 128), F32)] * TR
        for q in range(4):
            hs = [depth(32 * q + j) for j in range(4)]
            vs = [load(north_s, 32 * q + j) for j in range(4)]
            if q < 3:
                hs.append(depth(32 * q + 4))
                vs.append(load(north_s, 32 * q + 4))
            else:
                hs.append(pltpu.roll(hs[0], 7, 0))
                vs.append(pltpu.roll(vs[0], 7, 0))
            coefs = []
            for j in range(4):
                top = q == 3 and j == 3
                h, u = hs[j], load(east_s, 32 * q + j)
                rate = time_step / (area_s[row_set(32 * q + j)] * jnp.maximum(h, depth_floor))
                coefs.append(
                    face(h, pltpu.roll(h, 127, 1), u, pltpu.roll(u, 127, 1), mixing, keep=not_last)
                    + face(h, hs[j + 1], vs[j], vs[j + 1], mixing, keep=not_top if top else None)
                    + (rate,)
                )
            for t in range(TR):
                cells = [tr_s[(t, k, *row_set(32 * q + j))] for j in range(4)]
                if q < 3:
                    cells.append(tr_s[(t, k, *row_set(32 * q + 4))])
                else:
                    cells.append(pltpu.roll(cells[0], 7, 0))
                norths = [coefs[j][2] * cells[j] - coefs[j][3] * cells[j + 1] for j in range(4)]
                turned = pltpu.roll(norths[3], 1, 0)
                souths = [jnp.where(sub > 0, turned, before[t])] + norths[:3]
                before[t] = turned
                for j in range(4):
                    p_e, q_e, _, _, rate = coefs[j]
                    cell = cells[j]
                    flux = p_e * cell - q_e * pltpu.roll(cell, 127, 1)
                    div = (pltpu.roll(flux, 1, 1) - flux) + (souths[j] - norths[j])
                    moved = pltpu.roll(d_ew[4 * q + j], 127 - 2 * k + (128 - 32 * t), 1)
                    div = div + jnp.where(ends, moved, 0.0)
                    if q == 0 and j == 0:
                        div = div + jnp.where(sub == 0, d_ns[0, pl.ds(t * 16 + k, 1), :], 0.0)
                    if q == 3 and j == 3:
                        div = div + jnp.where(sub == 7, d_ns[1, pl.ds(t * 16 + k, 1), :], 0.0)
                    out_s[(t, k, *row_set(32 * q + j))] = cell + rate * div

    def group_body(group, carry):
        for copy in copies(group):
            copy.wait()
        for n in range(per):
            level(group * per + n)
        out_copy(group).start()
        return carry

    lax.fori_loop(0, GROUPS, group_body, 0)
    for group in range(GROUPS):
        out_copy(group).wait()


def kernel_third_call(tracers, fill, mask, east, north, diff, area, d_ew, d_ns):
    hbm = pl.BlockSpec(memory_space=pltpu.HBM)
    vmem = pl.BlockSpec(memory_space=pltpu.VMEM)
    return pl.pallas_call(
        kernel_third,
        name="third",
        out_shape=jax.ShapeDtypeStruct((TR, LV, ROWS, LANES), F32),
        in_specs=[hbm] * 5 + [pl.BlockSpec(memory_space=pltpu.SMEM), hbm, vmem, vmem],
        out_specs=hbm,
        scratch_shapes=[
            pltpu.VMEM((TR, LV, ROWS, LANES), F32),
            pltpu.VMEM((LV, ROWS, LANES), F32),
            pltpu.VMEM((LV, ROWS, LANES), jnp.int32),
            pltpu.VMEM((LV, ROWS, LANES), F32),
            pltpu.VMEM((LV, ROWS, LANES), F32),
            pltpu.VMEM((ROWS, LANES), F32),
            pltpu.VMEM((TR, LV, ROWS, LANES), F32),
            pltpu.SemaphoreType.DMA((5, GROUPS)),
            pltpu.SemaphoreType.DMA,
            pltpu.SemaphoreType.DMA((GROUPS,)),
        ],
        compiler_params=pltpu.CompilerParams(vmem_limit_bytes=24 * MIB),
        cost_estimate=pl.CostEstimate(flops=60_000_000, bytes_accessed=12 * MIB, transcendentals=0),
    )(tracers, fill, mask, east, north, diff, area, d_ew, d_ns)


SPLITS = 4


def kernel_last(got, two, four):
    for m in range(32 // SPLITS):
        for n in range(CHUNKS):
            value = got[pl.ds(m * 8 * CHUNKS + n, 8, stride=CHUNKS), :]
            if n < 16:
                two[pl.ds(m * 8, 8), pl.ds(n * 128, 128)] = value
            else:
                four[pl.ds(m * 8, 8), pl.ds((n - 16) * 128, 128)] = value


def kernel_last_call(got):
    return pl.pallas_call(
        kernel_last,
        name="last",
        grid=(SPLITS,),
        out_shape=(
            jax.ShapeDtypeStruct((DEV * CAP, 2048), F32),
            jax.ShapeDtypeStruct((DEV * CAP, 512), F32),
        ),
        in_specs=[pl.BlockSpec((DEV * 40 // SPLITS, 128), lambda s: (s, 0))],
        out_specs=(
            pl.BlockSpec((DEV * CAP // SPLITS, 2048), lambda s: (s, 0)),
            pl.BlockSpec((DEV * CAP // SPLITS, 512), lambda s: (s, 0)),
        ),
        compiler_params=pltpu.CompilerParams(vmem_limit_bytes=8 * MIB),
    )(got)


def local(
    tracers, fill_fraction, ocean_mask, east_speed, north_speed, diffusivity, cell_area, owner_map
):
    lon_count = lax.axis_size("lon")
    lat_count = lax.axis_size("lat")
    *fields, diffusivity, cell_area, owners = (
        pltpu.with_memory_space_constraint(x, pltpu.HBM)
        for x in (
            tracers, fill_fraction, ocean_mask, east_speed, north_speed, diffusivity, cell_area,
            owner_map.reshape(1, DEV),
        )
    )
    tracers, fill_fraction, ocean_mask, east_speed, north_speed = fields
    ns_fwd, ns_bwd = kernel_rows_call(tracers, fill_fraction, ocean_mask, north_speed)
    both = ("lon", "lat")
    chain = []
    for low in range(lon_count // 2):
        high = lon_count - 1 - low
        up = [low * lat_count + a for a in range(lat_count)]
        path = up + [high * lat_count + a for a in reversed(range(lat_count))]
        chain += list(zip(path[:-1], path[1:]))
    got_fwd = lax.ppermute(ns_fwd, both, chain)
    got_bwd = lax.ppermute(ns_bwd, both, [(b, a) for a, b in chain])
    num2, den2, ew, placing = kernel_first_call(*fields, diffusivity, cell_area, owners)
    ring = [(i, (i + 1) % lon_count) for i in range(lon_count)]
    from_west = lax.ppermute(ew, "lon", ring)
    from_east = lax.ppermute(ew, "lon", [(b, a) for a, b in ring])
    send, d_ew, d_ns = kernel_second_call(
        num2, den2, ew, from_east, from_west, ns_fwd, ns_bwd, got_fwd, got_bwd, diffusivity, placing
    )
    got = lax.all_to_all(
        send.reshape(DEV, CAP * CHUNKS, 128), both, split_axis=0, concat_axis=0, tiled=True
    )
    updated = kernel_third_call(*fields, diffusivity, cell_area, d_ew, d_ns)
    two, four = kernel_last_call(got.reshape(DEV * CAP * CHUNKS, 128))
    return (updated, two[None], four[None])


def solution(mesh):
    in_specs = (
        P(None, None, "lat", "lon"),
        P(None, "lat", "lon"),
        P(None, "lat", "lon"),
        P(None, "lat", "lon"),
        P(None, "lat", "lon"),
        P(),
        P("lat", "lon"),
        P(("lon", "lat"), None),
    )
    out_specs = (
        P(None, None, "lat", "lon"),
        P(("lon", "lat"), None, None),
        P(("lon", "lat"), None, None),
    )
    return jax.shard_map(
        local,
        mesh=mesh, in_specs=in_specs, out_specs=out_specs, check_vma=False,
    )
```

```python
import jax
import jax.numpy as jnp
from jax import lax
from jax.experimental import pallas as pl
from jax.experimental.pallas import tpu as pltpu
from jax.sharding import PartitionSpec as P


time_step = 0.05
depth_floor = 0.25
weight_floor = 0.25

TR, LV = 4, 16
ROWS, LANES = 128, 128
GROUPS = 16
DEV, CAP = 128, 2
CHUNKS = 20
PARTS = 2
F32, BF16 = jnp.float32, jnp.bfloat16
MIB = 1 << 20


def lane_iota(shape=(8, 128)):
    return lax.broadcasted_iota(jnp.int32, shape, len(shape) - 1)


def sub_iota(shape=(8, 128)):
    return lax.broadcasted_iota(jnp.int32, shape, len(shape) - 2)


def face(lower_h, upper_h, lower_speed, upper_speed, mixing, keep=None):
    open_depth = jnp.minimum(lower_h, upper_h)
    if keep is not None:
        open_depth = jnp.where(keep, open_depth, 0.0)
    speed = 0.5 * (lower_speed + upper_speed)
    ahead = jnp.maximum(speed, 0.0)
    back = ahead - speed
    return open_depth * (ahead + mixing), open_depth * (back + mixing)


def halves(values):
    high = values.astype(BF16)
    return high, (values - high.astype(F32)).astype(BF16)


def split_dot(left, right):
    high, low = halves(left)
    return jnp.dot(high, right, preferred_element_type=F32) + jnp.dot(
        low, right, preferred_element_type=F32
    )


def input_copies(hbm, vmem, sems):
    per = LV // GROUPS

    def copies(group):
        levels = pl.ds(group * per, per)
        out = [pltpu.make_async_copy(hbm[0].at[:, levels], vmem[0].at[:, levels], sems.at[0, group])]
        for n in range(1, 5):
            out.append(
                pltpu.make_async_copy(hbm[n].at[levels], vmem[n].at[levels], sems.at[n, group])
            )
        return out

    return copies


def row_set(start):
    return (pl.ds(start, 8, stride=4), slice(None))


def kernel_rows(tr, fill, mask, north, ns_fwd, ns_bwd, tr_s, fill_s, mask_s, north_s, sems):
    copies = []
    for n, (src, dst) in enumerate(((tr, tr_s), (fill, fill_s), (mask, mask_s), (north, north_s))):
        for side in range(2):
            rows = pl.ds(side * (ROWS - 8), 8)
            if n == 0:
                copies.append(
                    pltpu.make_async_copy(src.at[:, :, rows], dst.at[side], sems.at[n, side])
                )
            else:
                copies.append(
                    pltpu.make_async_copy(src.at[:, rows], dst.at[side], sems.at[n, side])
                )
            copies[-1].start()
    for copy in copies:
        copy.wait()
    flip = lax.axis_index("lon") >= lax.axis_size("lon") // 2
    for n in range(6):
        for half in range(2):
            levels = range(8 * half, 8 * half + 8)
            lines = []
            for side in range(2):
                row = 7 * side
                pick = lambda ref, k: ref[side, k, pl.ds(row, 1), :]
                if n < TR:
                    parts = [tr_s[side, n, k, pl.ds(row, 1), :] for k in levels]
                elif n == TR:
                    parts = [pick(fill_s, k) * pick(mask_s, k).astype(F32) for k in levels]
                else:
                    parts = [pick(north_s, k) for k in levels]
                lines.append(jnp.concatenate(parts, axis=0))
            at = pl.ds(n * 16 + 8 * half, 8)
            ns_fwd[at, :] = jnp.where(flip, lines[0], lines[1])
            ns_bwd[at, :] = jnp.where(flip, lines[1], lines[0])


def kernel_rows_call(tracers, fill, mask, north):
    hbm = pl.BlockSpec(memory_space=pltpu.HBM)
    vmem = pl.BlockSpec(memory_space=pltpu.VMEM)
    return pl.pallas_call(
        kernel_rows,
        name="rows",
        out_shape=(jax.ShapeDtypeStruct((96, 128), F32),) * 2,
        in_specs=[hbm] * 4,
        out_specs=(vmem,) * 2,
        scratch_shapes=[
            pltpu.VMEM((2, TR, LV, 8, LANES), F32),
            pltpu.VMEM((2, LV, 8, LANES), F32),
            pltpu.VMEM((2, LV, 8, LANES), jnp.int32),
            pltpu.VMEM((2, LV, 8, LANES), F32),
            pltpu.SemaphoreType.DMA((4, 2)),
        ],
        compiler_params=pltpu.CompilerParams(vmem_limit_bytes=4 * MIB),
        cost_estimate=pl.CostEstimate(flops=1_000_000, bytes_accessed=MIB, transcendentals=0),
    )(tracers, fill, mask, north)


def kernel_first(
    tr, fill, mask, east, north, diff, area, owner,
    num2, den2, ew, placing,
    tr_s, fill_s, mask_s, east_s, north_s, area_s, owner_s, h_s, g_s, face_s, coef, store, cross,
    sems, area_sem, owner_sem,
):
    hbm, vmem = (tr, fill, mask, east, north), (tr_s, fill_s, mask_s, east_s, north_s)
    copies = input_copies(hbm, vmem, sems)
    area_copy = pltpu.make_async_copy(area, area_s, area_sem)
    owner_copy = pltpu.make_async_copy(owner, owner_s, owner_sem)
    owner_copy.start()
    for group in range(GROUPS):
        for copy in copies(group):
            copy.start()
        if group == 0:
            area_copy.start()

    across = lane_iota((DEV, DEV))
    down = sub_iota((DEV, DEV))
    source = sub_iota((256, 128))
    target = lane_iota((256, 128))
    pool = jnp.where(target == (source >> 7) * 64 + ((source & 127) >> 1), 1.0, 0.0).astype(BF16)
    beside = (source >> 7) * 64 + (((source & 127) + 1) >> 1) - jnp.where((source & 1) == 0, 1, 0)
    inside = ((source & 127) != 0) & ((source & 127) != 127)
    pool_cross = jnp.where((target == beside) & inside, 1.0, 0.0).astype(BF16)
    owner_copy.wait()
    who_row = owner_s[...]
    who = jnp.sum(jnp.where(down == across, who_row, 0), axis=1, keepdims=True)
    same = jnp.where((who == who_row) & (down < across), 1, 0)
    rank = jnp.sum(same, axis=0, keepdims=True)
    row_of = who_row * CAP + rank
    for part in range(CAP):
        here = jnp.where(down + part * DEV == row_of, 1.0, 0.0).astype(BF16)
        placing[pl.ds(part * DEV, DEV), 0:DEV] = here
        placing[pl.ds(part * DEV, DEV), DEV : 2 * DEV] = here

    area_copy.wait()
    lane, sub = lane_iota(), sub_iota()
    is_even = (lane & 1) == 0
    not_last = lane < 127
    not_top = sub < 7

    def level(k):
        mixing = diff[k]

        def load(ref, start):
            return ref[(k, *row_set(start))]

        def depth(start):
            return load(fill_s, start) * load(mask_s, start).astype(F32)

        for v in range(16):
            start = 32 * (v // 4) + v % 4
            h, u = depth(start), load(east_s, start)
            base = 64 * (v % 2)
            packed = ew[16 + v // 2]
            packed = jnp.where(
                (lane >> 1) == k + base // 2, pltpu.roll(h, 2 * k + 1 + base, 1), packed
            )
            ew[16 + v // 2] = jnp.where(
                (lane >> 1) == k + 16 + base // 2, pltpu.roll(u, 2 * k + 33 + base, 1), packed
            )
            p_e, q_e = face(
                h, pltpu.roll(h, 127, 1), u, pltpu.roll(u, 127, 1), mixing, keep=not_last
            )
            h_s[v] = h
            g_s[v] = (time_step * h) / jnp.maximum(h, depth_floor)
            face_s[0, v] = p_e
            face_s[1, v] = q_e

        for v in range(16):
            q, j = v // 4, v % 4
            start = 32 * q + j
            h, speed = h_s[v], load(north_s, start)
            if j < 3:
                p_n, q_n = face(h, h_s[v + 1], speed, load(north_s, start + 1), mixing)
            elif q < 3:
                p_n, q_n = face(h, depth(start + 1), speed, load(north_s, start + 1), mixing)
            else:
                h_up, speed_up = pltpu.roll(h_s[12], 7, 0), pltpu.roll(load(north_s, 96), 7, 0)
                p_n, q_n = face(h, h_up, speed, speed_up, mixing, keep=not_top)
            face_s[2, v] = p_n
            face_s[3, v] = q_n

        for q in range(4):
            south = []
            for n in (2, 3):
                low = pltpu.roll(face_s[n, 4 * q + 3], 1, 0)
                under = pltpu.roll(face_s[n, 4 * q - 1], 1, 0) if q else 0.0
                south.append(jnp.where(sub > 0, low, under))
            for par in range(2):
                centre, weight = [], 0.0
                for n in range(2):
                    v = 4 * q + 2 * par + n
                    h, g = h_s[v], g_s[v]
                    w = area_s[row_set(32 * q + 2 * par + n)] * h
                    p_e, q_w = face_s[0, v], pltpu.roll(face_s[1, v], 1, 1)
                    p_n, q_n = face_s[2, v], face_s[3, v]
                    p_s, q_s = south if v % 4 == 0 else (face_s[2, v - 1], face_s[3, v - 1])
                    to_west = pltpu.roll(g, 1, 1) * q_w
                    to_east = pltpu.roll(g, 127, 1) * p_e
                    own = w - g * ((p_e + q_w) + (p_n + q_s))
                    centre.append(own + jnp.where(is_even, to_east, to_west))
                    coef[4 + n, 2 * q + par] = jnp.where(is_even, to_west, to_east)
                    if n == 0:
                        low, up = g * p_s, g * q_n
                    else:
                        down, high = g * p_s, g * q_n
                    weight = weight + w
                coef[0, 2 * q + par] = low
                coef[1, 2 * q + par] = centre[0] + down
                coef[2, 2 * q + par] = centre[1] + up
                coef[3, 2 * q + par] = high
                store[pl.ds(128 + q * 8, 8), pl.ds(par * 128, 128)] = weight

        where_t = [(lane >> 1) == t * 16 + k for t in range(TR)]
        for q in range(4):
            for j in range(4):
                packed = ew[4 * q + j]
                for t in range(TR):
                    cell = tr_s[(t, k, *row_set(32 * q + j))]
                    packed = jnp.where(where_t[t], pltpu.roll(cell, 2 * k + 32 * t + 1, 1), packed)
                ew[4 * q + j] = packed
            for par in range(2):
                low_c, a_c, b_c, high_c, a_x, b_x = [coef[n, 2 * q + par] for n in range(6)]
                for t in range(TR):
                    cell = lambda start: tr_s[(t, k, *row_set(start))]
                    start = 32 * q + 2 * par
                    a, b = cell(start), cell(start + 1)
                    low = cell(start - 1) if start else pltpu.roll(cell(3), 1, 0)
                    high = cell(start + 2) if start < 98 else pltpu.roll(cell(96), 7, 0)
                    side = a_x * a + b_x * b
                    value = (a_c * a + b_c * b) + (low_c * low + high_c * high)
                    cross[pl.ds(t * 32 + q * 8, 8), pl.ds(par * 128, 128)] = side
                    store[pl.ds(t * 32 + q * 8, 8), pl.ds(par * 128, 128)] = value

    def pooled(k):
        values = split_dot(store[...], pool)
        sides = split_dot(cross[...], pool_cross)
        rows = pl.ds(pl.multiple_of(k * 32, 32), 32)
        for t in range(TR):
            part = slice(t * 32, t * 32 + 32)
            num2[t, rows, :] = values[part] + sides[part]
        den2[rows, :] = values[128:160]

    def group_body(k, carry):
        for copy in copies(k):
            copy.wait()
        pooled((k + LV - 1) % LV)
        level(k)
        return carry

    store[...] = jnp.zeros_like(store)
    cross[...] = jnp.zeros_like(cross)
    lax.fori_loop(0, LV, group_body, 0)
    pooled(LV - 1)


def kernel_first_call(tracers, fill, mask, east, north, diff, area, owner):
    hbm = pl.BlockSpec(memory_space=pltpu.HBM)
    vmem = pl.BlockSpec(memory_space=pltpu.VMEM)
    return pl.pallas_call(
        kernel_first,
        name="first",
        out_shape=(
            jax.ShapeDtypeStruct((TR, 512, 128), F32),
            jax.ShapeDtypeStruct((512, 128), F32),
            jax.ShapeDtypeStruct((24, 8, 128), F32),
            jax.ShapeDtypeStruct((CAP * DEV, 2 * DEV), BF16),
        ),
        in_specs=[hbm] * 5 + [pl.BlockSpec(memory_space=pltpu.SMEM), hbm, hbm],
        out_specs=(vmem,) * 4,
        scratch_shapes=[
            pltpu.VMEM((TR, LV, ROWS, LANES), F32),
            pltpu.VMEM((LV, ROWS, LANES), F32),
            pltpu.VMEM((LV, ROWS, LANES), jnp.int32),
            pltpu.VMEM((LV, ROWS, LANES), F32),
            pltpu.VMEM((LV, ROWS, LANES), F32),
            pltpu.VMEM((ROWS, LANES), F32),
            pltpu.VMEM((1, DEV), jnp.int32),
            pltpu.VMEM((16, 8, 128), F32),
            pltpu.VMEM((16, 8, 128), F32),
            pltpu.VMEM((4, 16, 8, 128), F32),
            pltpu.VMEM((6, 8, 8, 128), F32),
            pltpu.VMEM((160, 256), F32),
            pltpu.VMEM((128, 256), F32),
            pltpu.SemaphoreType.DMA((5, GROUPS)),
            pltpu.SemaphoreType.DMA,
            pltpu.SemaphoreType.DMA,
        ],
        compiler_params=pltpu.CompilerParams(vmem_limit_bytes=24 * MIB),
        cost_estimate=pl.CostEstimate(flops=60_000_000, bytes_accessed=11 * MIB, transcendentals=0),
    )(tracers, fill, mask, east, north, diff, area, owner)


def spread(values, offset):
    index = (lane_iota() & 31) + offset
    return jnp.take_along_axis(values, index, axis=1)


def kernel_second(
    num2, den2, ew, from_east, from_west, ns_fwd, ns_bwd, got_fwd, got_bwd, diff, placing,
    send, d_ew, d_ns,
    work, acc, chunks, send_s, sems,
):
    lane, sub = lane_iota(), sub_iota()
    flip = lax.axis_index("lon") >= lax.axis_size("lon") // 2
    at_fold = lax.axis_index("lat") == lax.axis_size("lat") - 1
    is_east = (lane & 1) == 0
    level_of = (lane >> 1) & 15
    mixing = jnp.zeros((8, 128), F32)
    for k in range(LV):
        mixing = jnp.where(level_of == k, diff[k], mixing)

    def neighbour(n):
        return jnp.where(
            is_east, pltpu.roll(from_east[n], 127, 1), pltpu.roll(from_west[n], 1, 1)
        )

    pending = None
    for v in range(16):
        own_hu, near_hu = ew[16 + v // 2], neighbour(16 + v // 2)
        base = 64 * (v % 2)
        h = spread(own_hu, base)
        p, q = face(
            h, spread(near_hu, base), spread(own_hu, base + 32), spread(near_hu, base + 32), mixing
        )
        div = jnp.where(is_east, q, p) * neighbour(v) - jnp.where(is_east, p, q) * ew[v]
        d_ew[v] = div
        value = (time_step * h) / jnp.maximum(h, depth_floor) * div
        if v % 2 == 0:
            pending = value
        else:
            value = pending + value
            work[v // 2] = jnp.where(is_east, value, pltpu.roll(value, 64, 1))

    low_ends = (lane == 0) | (lane == 63)
    high_ends = (lane == 64) | (lane == 127)

    def add_ends(k, carry):
        for t in range(TR):
            for q in range(4):
                rows = pl.ds(pl.multiple_of(k * 32 + q * 8, 8), 8)
                shift = 127 - 2 * k + (128 - 32 * t)
                low = pltpu.roll(work[2 * q], shift - 64, 1)
                high = pltpu.roll(work[2 * q + 1], shift, 1)
                edge = jnp.where(low_ends, low, jnp.where(high_ends, high, 0.0))
                acc[t, rows, :] = num2[t, rows, :] + edge
        return carry

    lax.fori_loop(0, LV, add_ends, 0)

    source = sub_iota((128, 128))
    target = lane_iota((128, 128))
    pools = [
        jnp.where(target == par * 64 + (source >> 1), 1.0, 0.0).astype(BF16) for par in range(2)
    ]
    quarter = [
        jnp.where(target == j * 32 + ((source & 63) >> 1), 1.0, 0.0).astype(BF16) for j in range(4)
    ]

    back = 127 - lane
    for half in range(2):
        mix = jnp.zeros((8, 128), F32)
        for k in range(8):
            mix = jnp.where(sub == k, diff[8 * half + k], mix)

        def rows_of(ref, n):
            return ref[pl.ds(n * 16 + 8 * half, 8), :]

        def own(n, top):
            pair = (ns_bwd, ns_fwd) if top else (ns_fwd, ns_bwd)
            return jnp.where(flip, rows_of(pair[0], n), rows_of(pair[1], n))

        def near(n, top, sign=1.0):
            if not top:
                return jnp.where(flip, rows_of(got_bwd, n), rows_of(got_fwd, n))
            value = jnp.where(flip, rows_of(got_fwd, n), rows_of(got_bwd, n))
            turned = sign * jnp.take_along_axis(value, back, axis=1)
            return jnp.where(at_fold, turned, value)

        for top in (False, True):
            h = own(4, top)
            p, q = face(h, near(4, top), own(5, top), near(5, top, -1.0), mix)
            gain = (time_step * h) / jnp.maximum(h, depth_floor)
            for t in range(TR):
                if top:
                    div = q * near(t, top) - p * own(t, top)
                else:
                    div = p * near(t, top) - q * own(t, top)
                d_ns[int(top), pl.ds(t * 16 + 8 * half, 8), :] = div
                at = (t, pl.ds(256 * half + 31 * int(top), 8, stride=32), slice(None))
                acc[at] = acc[at] + split_dot(gain * div, pools[int(top)])

    def keep(n, values):
        high, low = halves(values)
        chunks[0:128, pl.ds(n * 128, 128)] = high
        chunks[128:256, pl.ds(n * 128, 128)] = low

    def every_fourth(ref, *lead, j):
        return jnp.concatenate(
            [ref[(*lead, pl.ds(32 * m + j, 8, stride=4), slice(None))] for m in range(16)], axis=0
        )

    gains = []
    den4 = jnp.zeros((128, 128), F32)
    for j in range(4):
        den = every_fourth(den2, j=j)
        gains.append(1.0 / jnp.maximum(den, weight_floor))
        den4 = den4 + split_dot(den, quarter[j])
    gain4 = 1.0 / jnp.maximum(den4, weight_floor)
    for t in range(TR):
        num4 = jnp.zeros((128, 128), F32)
        for j in range(4):
            num = every_fourth(acc, t, j=j)
            keep(t * 4 + j, num * gains[j])
            num4 = num4 + split_dot(num, quarter[j])
        keep(16 + t, num4 * gain4)

    each = CAP * DEV // PARTS
    copies = []
    for part in range(PARTS):
        left = placing[pl.ds(part * each, each), :]
        for n in range(CHUNKS // 2):
            placed = jnp.dot(left, chunks[:, pl.ds(n * 256, 256)], preferred_element_type=F32)
            for c in range(2):
                for m in range(each // 8):
                    start = (part * each + m * 8) * CHUNKS + 2 * n + c
                    send_s[pl.ds(start, 8, stride=CHUNKS), :] = placed[
                        m * 8 : m * 8 + 8, c * 128 : c * 128 + 128
                    ]
        rows = pl.ds(part * each * CHUNKS, each * CHUNKS)
        copies.append(pltpu.make_async_copy(send_s.at[rows], send.at[rows], sems.at[part]))
        copies[-1].start()
    for copy in copies:
        copy.wait()


def kernel_second_call(*args):
    vmem = pl.BlockSpec(memory_space=pltpu.VMEM)
    return pl.pallas_call(
        kernel_second,
        name="second",
        out_shape=(
            pltpu.HBM((DEV * CAP * CHUNKS, 128), F32),
            jax.ShapeDtypeStruct((16, 8, 128), F32),
            jax.ShapeDtypeStruct((2, 64, 128), F32),
        ),
        in_specs=[vmem] * 9 + [pl.BlockSpec(memory_space=pltpu.SMEM), vmem],
        out_specs=(pl.BlockSpec(memory_space=pltpu.HBM), vmem, vmem),
        scratch_shapes=[
            pltpu.VMEM((8, 8, 128), F32),
            pltpu.VMEM((TR, 512, 128), F32),
            pltpu.VMEM((256, 2560), BF16),
            pltpu.VMEM((DEV * CAP * CHUNKS, 128), F32),
            pltpu.SemaphoreType.DMA((PARTS,)),
        ],
        compiler_params=pltpu.CompilerParams(vmem_limit_bytes=16 * MIB),
        cost_estimate=pl.CostEstimate(flops=60_000_000, bytes_accessed=6 * MIB, transcendentals=0),
    )(*args)


def kernel_third(
    tr, fill, mask, east, north, diff, area, d_ew, d_ns,
    out,
    tr_s, fill_s, mask_s, east_s, north_s, area_s, out_s, sems, area_sem, out_sems,
):
    hbm, vmem = (tr, fill, mask, east, north), (tr_s, fill_s, mask_s, east_s, north_s)
    copies = input_copies(hbm, vmem, sems)
    area_copy = pltpu.make_async_copy(area, area_s, area_sem)
    for group in range(GROUPS):
        for copy in copies(group):
            copy.start()
        if group == 0:
            area_copy.start()
    area_copy.wait()
    lane, sub = lane_iota(), sub_iota()
    ends = (lane == 0) | (lane == 127)
    not_last, not_top = lane < 127, sub < 7
    per = LV // GROUPS

    def out_copy(group):
        levels = pl.ds(group * per, per)
        return pltpu.make_async_copy(out_s.at[:, levels], out.at[:, levels], out_sems.at[group])

    def level(k):
        mixing = diff[k]

        def load(ref, start):
            return ref[(k, *row_set(start))]

        def depth(start):
            return load(fill_s, start) * load(mask_s, start).astype(F32)

        before = [jnp.zeros((8, 128), F32)] * TR
        for q in range(4):
            hs = [depth(32 * q + j) for j in range(4)]
            vs = [load(north_s, 32 * q + j) for j in range(4)]
            if q < 3:
                hs.append(depth(32 * q + 4))
                vs.append(load(north_s, 32 * q + 4))
            else:
                hs.append(pltpu.roll(hs[0], 7, 0))
                vs.append(pltpu.roll(vs[0], 7, 0))
            coefs = []
            for j in range(4):
                top = q == 3 and j == 3
                h, u = hs[j], load(east_s, 32 * q + j)
                rate = time_step / (area_s[row_set(32 * q + j)] * jnp.maximum(h, depth_floor))
                coefs.append(
                    face(h, pltpu.roll(h, 127, 1), u, pltpu.roll(u, 127, 1), mixing, keep=not_last)
                    + face(h, hs[j + 1], vs[j], vs[j + 1], mixing, keep=not_top if top else None)
                    + (rate,)
                )
            for t in range(TR):
                cells = [tr_s[(t, k, *row_set(32 * q + j))] for j in range(4)]
                if q < 3:
                    cells.append(tr_s[(t, k, *row_set(32 * q + 4))])
                else:
                    cells.append(pltpu.roll(cells[0], 7, 0))
                norths = [coefs[j][2] * cells[j] - coefs[j][3] * cells[j + 1] for j in range(4)]
                turned = pltpu.roll(norths[3], 1, 0)
                souths = [jnp.where(sub > 0, turned, before[t])] + norths[:3]
                before[t] = turned
                for j in range(4):
                    p_e, q_e, _, _, rate = coefs[j]
                    cell = cells[j]
                    flux = p_e * cell - q_e * pltpu.roll(cell, 127, 1)
                    div = (pltpu.roll(flux, 1, 1) - flux) + (souths[j] - norths[j])
                    moved = pltpu.roll(d_ew[4 * q + j], 127 - 2 * k + (128 - 32 * t), 1)
                    div = div + jnp.where(ends, moved, 0.0)
                    if q == 0 and j == 0:
                        div = div + jnp.where(sub == 0, d_ns[0, pl.ds(t * 16 + k, 1), :], 0.0)
                    if q == 3 and j == 3:
                        div = div + jnp.where(sub == 7, d_ns[1, pl.ds(t * 16 + k, 1), :], 0.0)
                    out_s[(t, k, *row_set(32 * q + j))] = cell + rate * div

    def group_body(group, carry):
        for copy in copies(group):
            copy.wait()
        for n in range(per):
            level(group * per + n)
        out_copy(group).start()
        return carry

    lax.fori_loop(0, GROUPS, group_body, 0)
    for group in range(GROUPS):
        out_copy(group).wait()


def kernel_third_call(tracers, fill, mask, east, north, diff, area, d_ew, d_ns):
    hbm = pl.BlockSpec(memory_space=pltpu.HBM)
    vmem = pl.BlockSpec(memory_space=pltpu.VMEM)
    return pl.pallas_call(
        kernel_third,
        name="third",
        out_shape=jax.ShapeDtypeStruct((TR, LV, ROWS, LANES), F32),
        in_specs=[hbm] * 5 + [pl.BlockSpec(memory_space=pltpu.SMEM), hbm, vmem, vmem],
        out_specs=hbm,
        scratch_shapes=[
            pltpu.VMEM((TR, LV, ROWS, LANES), F32),
            pltpu.VMEM((LV, ROWS, LANES), F32),
            pltpu.VMEM((LV, ROWS, LANES), jnp.int32),
            pltpu.VMEM((LV, ROWS, LANES), F32),
            pltpu.VMEM((LV, ROWS, LANES), F32),
            pltpu.VMEM((ROWS, LANES), F32),
            pltpu.VMEM((TR, LV, ROWS, LANES), F32),
            pltpu.SemaphoreType.DMA((5, GROUPS)),
            pltpu.SemaphoreType.DMA,
            pltpu.SemaphoreType.DMA((GROUPS,)),
        ],
        compiler_params=pltpu.CompilerParams(vmem_limit_bytes=24 * MIB),
        cost_estimate=pl.CostEstimate(flops=60_000_000, bytes_accessed=12 * MIB, transcendentals=0),
    )(tracers, fill, mask, east, north, diff, area, d_ew, d_ns)


SPLITS = 4


def kernel_last(got, two, four):
    for m in range(32 // SPLITS):
        for n in range(CHUNKS):
            value = got[pl.ds(m * 8 * CHUNKS + n, 8, stride=CHUNKS), :]
            if n < 16:
                two[pl.ds(m * 8, 8), pl.ds(n * 128, 128)] = value
            else:
                four[pl.ds(m * 8, 8), pl.ds((n - 16) * 128, 128)] = value


def kernel_last_call(got):
    return pl.pallas_call(
        kernel_last,
        name="last",
        grid=(SPLITS,),
        out_shape=(
            jax.ShapeDtypeStruct((DEV * CAP, 2048), F32),
            jax.ShapeDtypeStruct((DEV * CAP, 512), F32),
        ),
        in_specs=[pl.BlockSpec((DEV * 40 // SPLITS, 128), lambda s: (s, 0))],
        out_specs=(
            pl.BlockSpec((DEV * CAP // SPLITS, 2048), lambda s: (s, 0)),
            pl.BlockSpec((DEV * CAP // SPLITS, 512), lambda s: (s, 0)),
        ),
        compiler_params=pltpu.CompilerParams(vmem_limit_bytes=8 * MIB),
    )(got)


def local(
    tracers, fill_fraction, ocean_mask, east_speed, north_speed, diffusivity, cell_area, owner_map
):
    lon_count = lax.axis_size("lon")
    lat_count = lax.axis_size("lat")
    *fields, diffusivity, cell_area, owners = (
        pltpu.with_memory_space_constraint(x, pltpu.HBM)
        for x in (
            tracers, fill_fraction, ocean_mask, east_speed, north_speed, diffusivity, cell_area,
            owner_map.reshape(1, DEV),
        )
    )
    tracers, fill_fraction, ocean_mask, east_speed, north_speed = fields
    ns_fwd, ns_bwd = kernel_rows_call(tracers, fill_fraction, ocean_mask, north_speed)
    both = ("lon", "lat")
    chain = []
    for low in range(lon_count // 2):
        high = lon_count - 1 - low
        up = [low * lat_count + a for a in range(lat_count)]
        path = up + [high * lat_count + a for a in reversed(range(lat_count))]
        chain += list(zip(path[:-1], path[1:]))
    got_fwd = lax.ppermute(ns_fwd, both, chain)
    got_bwd = lax.ppermute(ns_bwd, both, [(b, a) for a, b in chain])
    num2, den2, ew, placing = kernel_first_call(*fields, diffusivity, cell_area, owners)
    ring = [(i, (i + 1) % lon_count) for i in range(lon_count)]
    from_west = lax.ppermute(ew, "lon", ring)
    from_east = lax.ppermute(ew, "lon", [(b, a) for a, b in ring])
    send, d_ew, d_ns = kernel_second_call(
        num2, den2, ew, from_east, from_west, ns_fwd, ns_bwd, got_fwd, got_bwd, diffusivity, placing
    )
    got = lax.all_to_all(
        send.reshape(DEV, CAP * CHUNKS, 128), both, split_axis=0, concat_axis=0, tiled=True
    )
    updated = kernel_third_call(*fields, diffusivity, cell_area, d_ew, d_ns)
    two, four = kernel_last_call(got.reshape(DEV * CAP * CHUNKS, 128))
    return (updated, two[None], four[None])


def solution(mesh):
    in_specs = (
        P(None, None, "lat", "lon"),
        P(None, "lat", "lon"),
        P(None, "lat", "lon"),
        P(None, "lat", "lon"),
        P(None, "lat", "lon"),
        P(),
        P("lat", "lon"),
        P(("lon", "lat"), None),
    )
    out_specs = (
        P(None, None, "lat", "lon"),
        P(("lon", "lat"), None, None),
        P(("lon", "lat"), None, None),
    )
    return jax.shard_map(
        local,
        mesh=mesh, in_specs=in_specs, out_specs=out_specs, check_vma=False,
    )
```

```python
import jax
import jax.numpy as jnp
from jax import lax
from jax.experimental import pallas as pl
from jax.experimental.pallas import tpu as pltpu
from jax.sharding import PartitionSpec as P


time_step = 0.05
depth_floor = 0.25
weight_floor = 0.25

TR, LV = 4, 16
ROWS, LANES = 128, 128
GROUPS = 16
DEV, CAP = 128, 2
CHUNKS = 20
PARTS = 2
F32, BF16 = jnp.float32, jnp.bfloat16
MIB = 1 << 20


def lane_iota(shape=(8, 128)):
    return lax.broadcasted_iota(jnp.int32, shape, len(shape) - 1)


def sub_iota(shape=(8, 128)):
    return lax.broadcasted_iota(jnp.int32, shape, len(shape) - 2)


def face(lower_h, upper_h, lower_speed, upper_speed, mixing, keep=None):
    open_depth = jnp.minimum(lower_h, upper_h)
    if keep is not None:
        open_depth = jnp.where(keep, open_depth, 0.0)
    speed = 0.5 * (lower_speed + upper_speed)
    ahead = jnp.maximum(speed, 0.0)
    back = ahead - speed
    return open_depth * (ahead + mixing), open_depth * (back + mixing)


def halves(values):
    high = values.astype(BF16)
    return high, (values - high.astype(F32)).astype(BF16)


def split_dot(left, right):
    high, low = halves(left)
    return jnp.dot(high, right, preferred_element_type=F32) + jnp.dot(
        low, right, preferred_element_type=F32
    )


def input_copies(hbm, vmem, sems):
    per = LV // GROUPS

    def copies(group):
        levels = pl.ds(group * per, per)
        out = [pltpu.make_async_copy(hbm[0].at[:, levels], vmem[0].at[:, levels], sems.at[0, group])]
        for n in range(1, 5):
            out.append(
                pltpu.make_async_copy(hbm[n].at[levels], vmem[n].at[levels], sems.at[n, group])
            )
        return out

    return copies


def row_set(start):
    return (pl.ds(start, 8, stride=4), slice(None))


def kernel_rows(tr, fill, mask, north, ns_one, ns_two, tr_s, fill_s, mask_s, north_s, sems):
    copies = []
    for n, (src, dst) in enumerate(((tr, tr_s), (fill, fill_s), (mask, mask_s), (north, north_s))):
        for side in range(2):
            rows = pl.ds(side * (ROWS - 8), 8)
            if n == 0:
                copies.append(
                    pltpu.make_async_copy(src.at[:, :, rows], dst.at[side], sems.at[n, side])
                )
            else:
                copies.append(
                    pltpu.make_async_copy(src.at[:, rows], dst.at[side], sems.at[n, side])
                )
            copies[-1].start()
    for copy in copies:
        copy.wait()
    odd = lax.axis_index("lat") % 2 == 1
    for n in range(6):
        for half in range(2):
            levels = range(8 * half, 8 * half + 8)
            lines = []
            for side in range(2):
                row = 7 * side
                pick = lambda ref, k: ref[side, k, pl.ds(row, 1), :]
                if n < TR:
                    parts = [tr_s[side, n, k, pl.ds(row, 1), :] for k in levels]
                elif n == TR:
                    parts = [pick(fill_s, k) * pick(mask_s, k).astype(F32) for k in levels]
                else:
                    parts = [pick(north_s, k) for k in levels]
                lines.append(jnp.concatenate(parts, axis=0))
            at = pl.ds(n * 16 + 8 * half, 8)
            ns_one[at, :] = jnp.where(odd, lines[0], lines[1])
            ns_two[at, :] = jnp.where(odd, lines[1], lines[0])


def kernel_rows_call(tracers, fill, mask, north):
    hbm = pl.BlockSpec(memory_space=pltpu.HBM)
    vmem = pl.BlockSpec(memory_space=pltpu.VMEM)
    return pl.pallas_call(
        kernel_rows,
        name="rows",
        out_shape=(jax.ShapeDtypeStruct((96, 128), F32),) * 2,
        in_specs=[hbm] * 4,
        out_specs=(vmem,) * 2,
        scratch_shapes=[
            pltpu.VMEM((2, TR, LV, 8, LANES), F32),
            pltpu.VMEM((2, LV, 8, LANES), F32),
            pltpu.VMEM((2, LV, 8, LANES), jnp.int32),
            pltpu.VMEM((2, LV, 8, LANES), F32),
            pltpu.SemaphoreType.DMA((4, 2)),
        ],
        compiler_params=pltpu.CompilerParams(vmem_limit_bytes=4 * MIB),
        cost_estimate=pl.CostEstimate(flops=1_000_000, bytes_accessed=MIB, transcendentals=0),
    )(tracers, fill, mask, north)


def kernel_first(
    tr, fill, mask, east, north, diff, area, owner,
    num2, den2, ew, placing,
    tr_s, fill_s, mask_s, east_s, north_s, area_s, owner_s, h_s, g_s, face_s, coef, store, cross,
    sems, area_sem, owner_sem,
):
    hbm, vmem = (tr, fill, mask, east, north), (tr_s, fill_s, mask_s, east_s, north_s)
    copies = input_copies(hbm, vmem, sems)
    area_copy = pltpu.make_async_copy(area, area_s, area_sem)
    owner_copy = pltpu.make_async_copy(owner, owner_s, owner_sem)
    owner_copy.start()
    for group in range(GROUPS):
        for copy in copies(group):
            copy.start()
        if group == 0:
            area_copy.start()

    across = lane_iota((DEV, DEV))
    down = sub_iota((DEV, DEV))
    source = sub_iota((256, 128))
    target = lane_iota((256, 128))
    pool = jnp.where(target == (source >> 7) * 64 + ((source & 127) >> 1), 1.0, 0.0).astype(BF16)
    beside = (source >> 7) * 64 + (((source & 127) + 1) >> 1) - jnp.where((source & 1) == 0, 1, 0)
    inside = ((source & 127) != 0) & ((source & 127) != 127)
    pool_cross = jnp.where((target == beside) & inside, 1.0, 0.0).astype(BF16)
    owner_copy.wait()
    who_row = owner_s[...]
    who = jnp.sum(jnp.where(down == across, who_row, 0), axis=1, keepdims=True)
    same = jnp.where((who == who_row) & (down < across), 1, 0)
    rank = jnp.sum(same, axis=0, keepdims=True)
    row_of = who_row * CAP + rank
    for part in range(CAP):
        here = jnp.where(down + part * DEV == row_of, 1.0, 0.0).astype(BF16)
        placing[pl.ds(part * DEV, DEV), 0:DEV] = here
        placing[pl.ds(part * DEV, DEV), DEV : 2 * DEV] = here

    area_copy.wait()
    lane, sub = lane_iota(), sub_iota()
    is_even = (lane & 1) == 0
    not_last = lane < 127
    not_top = sub < 7

    def level(k):
        mixing = diff[k]

        def load(ref, start):
            return ref[(k, *row_set(start))]

        def depth(start):
            return load(fill_s, start) * load(mask_s, start).astype(F32)

        for v in range(16):
            start = 32 * (v // 4) + v % 4
            h, u = depth(start), load(east_s, start)
            base = 64 * (v % 2)
            packed = ew[16 + v // 2]
            packed = jnp.where(
                (lane >> 1) == k + base // 2, pltpu.roll(h, 2 * k + 1 + base, 1), packed
            )
            ew[16 + v // 2] = jnp.where(
                (lane >> 1) == k + 16 + base // 2, pltpu.roll(u, 2 * k + 33 + base, 1), packed
            )
            p_e, q_e = face(
                h, pltpu.roll(h, 127, 1), u, pltpu.roll(u, 127, 1), mixing, keep=not_last
            )
            h_s[v] = h
            g_s[v] = (time_step * h) / jnp.maximum(h, depth_floor)
            face_s[0, v] = p_e
            face_s[1, v] = q_e

        for v in range(16):
            q, j = v // 4, v % 4
            start = 32 * q + j
            h, speed = h_s[v], load(north_s, start)
            if j < 3:
                p_n, q_n = face(h, h_s[v + 1], speed, load(north_s, start + 1), mixing)
            elif q < 3:
                p_n, q_n = face(h, depth(start + 1), speed, load(north_s, start + 1), mixing)
            else:
                h_up, speed_up = pltpu.roll(h_s[12], 7, 0), pltpu.roll(load(north_s, 96), 7, 0)
                p_n, q_n = face(h, h_up, speed, speed_up, mixing, keep=not_top)
            face_s[2, v] = p_n
            face_s[3, v] = q_n

        for q in range(4):
            south = []
            for n in (2, 3):
                low = pltpu.roll(face_s[n, 4 * q + 3], 1, 0)
                under = pltpu.roll(face_s[n, 4 * q - 1], 1, 0) if q else 0.0
                south.append(jnp.where(sub > 0, low, under))
            for par in range(2):
                centre, weight = [], 0.0
                for n in range(2):
                    v = 4 * q + 2 * par + n
                    h, g = h_s[v], g_s[v]
                    w = area_s[row_set(32 * q + 2 * par + n)] * h
                    p_e, q_w = face_s[0, v], pltpu.roll(face_s[1, v], 1, 1)
                    p_n, q_n = face_s[2, v], face_s[3, v]
                    p_s, q_s = south if v % 4 == 0 else (face_s[2, v - 1], face_s[3, v - 1])
                    to_west = pltpu.roll(g, 1, 1) * q_w
                    to_east = pltpu.roll(g, 127, 1) * p_e
                    own = w - g * ((p_e + q_w) + (p_n + q_s))
                    centre.append(own + jnp.where(is_even, to_east, to_west))
                    coef[4 + n, 2 * q + par] = jnp.where(is_even, to_west, to_east)
                    if n == 0:
                        low, up = g * p_s, g * q_n
                    else:
                        down, high = g * p_s, g * q_n
                    weight = weight + w
                coef[0, 2 * q + par] = low
                coef[1, 2 * q + par] = centre[0] + down
                coef[2, 2 * q + par] = centre[1] + up
                coef[3, 2 * q + par] = high
                store[pl.ds(128 + q * 8, 8), pl.ds(par * 128, 128)] = weight

        where_t = [(lane >> 1) == t * 16 + k for t in range(TR)]
        for q in range(4):
            for j in range(4):
                packed = ew[4 * q + j]
                for t in range(TR):
                    cell = tr_s[(t, k, *row_set(32 * q + j))]
                    packed = jnp.where(where_t[t], pltpu.roll(cell, 2 * k + 32 * t + 1, 1), packed)
                ew[4 * q + j] = packed
            for par in range(2):
                low_c, a_c, b_c, high_c, a_x, b_x = [coef[n, 2 * q + par] for n in range(6)]
                for t in range(TR):
                    cell = lambda start: tr_s[(t, k, *row_set(start))]
                    start = 32 * q + 2 * par
                    a, b = cell(start), cell(start + 1)
                    low = cell(start - 1) if start else pltpu.roll(cell(3), 1, 0)
                    high = cell(start + 2) if start < 98 else pltpu.roll(cell(96), 7, 0)
                    side = a_x * a + b_x * b
                    value = (a_c * a + b_c * b) + (low_c * low + high_c * high)
                    cross[pl.ds(t * 32 + q * 8, 8), pl.ds(par * 128, 128)] = side
                    store[pl.ds(t * 32 + q * 8, 8), pl.ds(par * 128, 128)] = value

    def pooled(k):
        values = split_dot(store[...], pool)
        sides = split_dot(cross[...], pool_cross)
        rows = pl.ds(pl.multiple_of(k * 32, 32), 32)
        for t in range(TR):
            part = slice(t * 32, t * 32 + 32)
            num2[t, rows, :] = values[part] + sides[part]
        den2[rows, :] = values[128:160]

    def group_body(k, carry):
        for copy in copies(k):
            copy.wait()
        pooled((k + LV - 1) % LV)
        level(k)
        return carry

    store[...] = jnp.zeros_like(store)
    cross[...] = jnp.zeros_like(cross)
    lax.fori_loop(0, LV, group_body, 0)
    pooled(LV - 1)


def kernel_first_call(tracers, fill, mask, east, north, diff, area, owner):
    hbm = pl.BlockSpec(memory_space=pltpu.HBM)
    vmem = pl.BlockSpec(memory_space=pltpu.VMEM)
    return pl.pallas_call(
        kernel_first,
        name="first",
        out_shape=(
            jax.ShapeDtypeStruct((TR, 512, 128), F32),
            jax.ShapeDtypeStruct((512, 128), F32),
            jax.ShapeDtypeStruct((24, 8, 128), F32),
            jax.ShapeDtypeStruct((CAP * DEV, 2 * DEV), BF16),
        ),
        in_specs=[hbm] * 5 + [pl.BlockSpec(memory_space=pltpu.SMEM), hbm, hbm],
        out_specs=(vmem,) * 4,
        scratch_shapes=[
            pltpu.VMEM((TR, LV, ROWS, LANES), F32),
            pltpu.VMEM((LV, ROWS, LANES), F32),
            pltpu.VMEM((LV, ROWS, LANES), jnp.int32),
            pltpu.VMEM((LV, ROWS, LANES), F32),
            pltpu.VMEM((LV, ROWS, LANES), F32),
            pltpu.VMEM((ROWS, LANES), F32),
            pltpu.VMEM((1, DEV), jnp.int32),
            pltpu.VMEM((16, 8, 128), F32),
            pltpu.VMEM((16, 8, 128), F32),
            pltpu.VMEM((4, 16, 8, 128), F32),
            pltpu.VMEM((6, 8, 8, 128), F32),
            pltpu.VMEM((160, 256), F32),
            pltpu.VMEM((128, 256), F32),
            pltpu.SemaphoreType.DMA((5, GROUPS)),
            pltpu.SemaphoreType.DMA,
            pltpu.SemaphoreType.DMA,
        ],
        compiler_params=pltpu.CompilerParams(vmem_limit_bytes=24 * MIB),
        cost_estimate=pl.CostEstimate(flops=60_000_000, bytes_accessed=11 * MIB, transcendentals=0),
    )(tracers, fill, mask, east, north, diff, area, owner)


def spread(values, offset):
    index = (lane_iota() & 31) + offset
    return jnp.take_along_axis(values, index, axis=1)


def kernel_second(
    num2, den2, ew, ew_one, ew_two, ns_one, ns_two, got_one, got_two, diff, placing,
    send, d_ew, d_ns,
    work, acc, chunks, send_s, sems,
):
    lane, sub = lane_iota(), sub_iota()
    odd = lax.axis_index("lat") % 2 == 1
    odd_lon = lax.axis_index("lon") % 2 == 1
    at_fold = lax.axis_index("lat") == lax.axis_size("lat") - 1
    is_east = (lane & 1) == 0
    level_of = (lane >> 1) & 15
    mixing = jnp.zeros((8, 128), F32)
    for k in range(LV):
        mixing = jnp.where(level_of == k, diff[k], mixing)

    def neighbour(n):
        one, two = ew_one[n], ew_two[n]
        from_east, from_west = jnp.where(odd_lon, two, one), jnp.where(odd_lon, one, two)
        return jnp.where(is_east, pltpu.roll(from_east, 127, 1), pltpu.roll(from_west, 1, 1))

    pending = None
    for v in range(16):
        own_hu, near_hu = ew[16 + v // 2], neighbour(16 + v // 2)
        base = 64 * (v % 2)
        h = spread(own_hu, base)
        p, q = face(
            h, spread(near_hu, base), spread(own_hu, base + 32), spread(near_hu, base + 32), mixing
        )
        div = jnp.where(is_east, q, p) * neighbour(v) - jnp.where(is_east, p, q) * ew[v]
        d_ew[v] = div
        value = (time_step * h) / jnp.maximum(h, depth_floor) * div
        if v % 2 == 0:
            pending = value
        else:
            value = pending + value
            work[v // 2] = jnp.where(is_east, value, pltpu.roll(value, 64, 1))

    low_ends = (lane == 0) | (lane == 63)
    high_ends = (lane == 64) | (lane == 127)

    def add_ends(k, carry):
        for t in range(TR):
            for q in range(4):
                rows = pl.ds(pl.multiple_of(k * 32 + q * 8, 8), 8)
                shift = 127 - 2 * k + (128 - 32 * t)
                low = pltpu.roll(work[2 * q], shift - 64, 1)
                high = pltpu.roll(work[2 * q + 1], shift, 1)
                edge = jnp.where(low_ends, low, jnp.where(high_ends, high, 0.0))
                acc[t, rows, :] = num2[t, rows, :] + edge
        return carry

    lax.fori_loop(0, LV, add_ends, 0)

    source = sub_iota((128, 128))
    target = lane_iota((128, 128))
    pools = [
        jnp.where(target == par * 64 + (source >> 1), 1.0, 0.0).astype(BF16) for par in range(2)
    ]
    quarter = [
        jnp.where(target == j * 32 + ((source & 63) >> 1), 1.0, 0.0).astype(BF16) for j in range(4)
    ]

    back = 127 - lane
    for half in range(2):
        mix = jnp.zeros((8, 128), F32)
        for k in range(8):
            mix = jnp.where(sub == k, diff[8 * half + k], mix)

        def rows_of(ref, n):
            return ref[pl.ds(n * 16 + 8 * half, 8), :]

        def own(n, top):
            pair = (ns_two, ns_one) if top else (ns_one, ns_two)
            return jnp.where(odd, rows_of(pair[0], n), rows_of(pair[1], n))

        def near(n, top, sign=1.0):
            if not top:
                return jnp.where(odd, rows_of(got_one, n), rows_of(got_two, n))
            value = jnp.where(odd, rows_of(got_two, n), rows_of(got_one, n))
            turned = sign * jnp.take_along_axis(value, back, axis=1)
            return jnp.where(at_fold, turned, value)

        for top in (False, True):
            h = own(4, top)
            p, q = face(h, near(4, top), own(5, top), near(5, top, -1.0), mix)
            gain = (time_step * h) / jnp.maximum(h, depth_floor)
            for t in range(TR):
                if top:
                    div = q * near(t, top) - p * own(t, top)
                else:
                    div = p * near(t, top) - q * own(t, top)
                d_ns[int(top), pl.ds(t * 16 + 8 * half, 8), :] = div
                at = (t, pl.ds(256 * half + 31 * int(top), 8, stride=32), slice(None))
                acc[at] = acc[at] + split_dot(gain * div, pools[int(top)])

    def keep(n, values):
        high, low = halves(values)
        chunks[0:128, pl.ds(n * 128, 128)] = high
        chunks[128:256, pl.ds(n * 128, 128)] = low

    def every_fourth(ref, *lead, j):
        return jnp.concatenate(
            [ref[(*lead, pl.ds(32 * m + j, 8, stride=4), slice(None))] for m in range(16)], axis=0
        )

    gains = []
    den4 = jnp.zeros((128, 128), F32)
    for j in range(4):
        den = every_fourth(den2, j=j)
        gains.append(1.0 / jnp.maximum(den, weight_floor))
        den4 = den4 + split_dot(den, quarter[j])
    gain4 = 1.0 / jnp.maximum(den4, weight_floor)
    for t in range(TR):
        num4 = jnp.zeros((128, 128), F32)
        for j in range(4):
            num = every_fourth(acc, t, j=j)
            keep(t * 4 + j, num * gains[j])
            num4 = num4 + split_dot(num, quarter[j])
        keep(16 + t, num4 * gain4)

    each = CAP * DEV // PARTS
    copies = []
    for part in range(PARTS):
        left = placing[pl.ds(part * each, each), :]
        for n in range(CHUNKS // 2):
            placed = jnp.dot(left, chunks[:, pl.ds(n * 256, 256)], preferred_element_type=F32)
            for c in range(2):
                for m in range(each // 8):
                    start = (part * each + m * 8) * CHUNKS + 2 * n + c
                    send_s[pl.ds(start, 8, stride=CHUNKS), :] = placed[
                        m * 8 : m * 8 + 8, c * 128 : c * 128 + 128
                    ]
        rows = pl.ds(part * each * CHUNKS, each * CHUNKS)
        copies.append(pltpu.make_async_copy(send_s.at[rows], send.at[rows], sems.at[part]))
        copies[-1].start()
    for copy in copies:
        copy.wait()


def kernel_second_call(*args):
    vmem = pl.BlockSpec(memory_space=pltpu.VMEM)
    return pl.pallas_call(
        kernel_second,
        name="second",
        out_shape=(
            pltpu.HBM((DEV * CAP * CHUNKS, 128), F32),
            jax.ShapeDtypeStruct((16, 8, 128), F32),
            jax.ShapeDtypeStruct((2, 64, 128), F32),
        ),
        in_specs=[vmem] * 9 + [pl.BlockSpec(memory_space=pltpu.SMEM), vmem],
        out_specs=(pl.BlockSpec(memory_space=pltpu.HBM), vmem, vmem),
        scratch_shapes=[
            pltpu.VMEM((8, 8, 128), F32),
            pltpu.VMEM((TR, 512, 128), F32),
            pltpu.VMEM((256, 2560), BF16),
            pltpu.VMEM((DEV * CAP * CHUNKS, 128), F32),
            pltpu.SemaphoreType.DMA((PARTS,)),
        ],
        compiler_params=pltpu.CompilerParams(vmem_limit_bytes=16 * MIB),
        cost_estimate=pl.CostEstimate(flops=60_000_000, bytes_accessed=6 * MIB, transcendentals=0),
    )(*args)


def kernel_third(
    tr, fill, mask, east, north, diff, area, d_ew, d_ns,
    out,
    tr_s, fill_s, mask_s, east_s, north_s, area_s, out_s, sems, area_sem, out_sems,
):
    hbm, vmem = (tr, fill, mask, east, north), (tr_s, fill_s, mask_s, east_s, north_s)
    copies = input_copies(hbm, vmem, sems)
    area_copy = pltpu.make_async_copy(area, area_s, area_sem)
    for group in range(GROUPS):
        for copy in copies(group):
            copy.start()
        if group == 0:
            area_copy.start()
    area_copy.wait()
    lane, sub = lane_iota(), sub_iota()
    ends = (lane == 0) | (lane == 127)
    not_last, not_top = lane < 127, sub < 7
    per = LV // GROUPS

    def out_copy(group):
        levels = pl.ds(group * per, per)
        return pltpu.make_async_copy(out_s.at[:, levels], out.at[:, levels], out_sems.at[group])

    def level(k):
        mixing = diff[k]

        def load(ref, start):
            return ref[(k, *row_set(start))]

        def depth(start):
            return load(fill_s, start) * load(mask_s, start).astype(F32)

        before = [jnp.zeros((8, 128), F32)] * TR
        for q in range(4):
            hs = [depth(32 * q + j) for j in range(4)]
            vs = [load(north_s, 32 * q + j) for j in range(4)]
            if q < 3:
                hs.append(depth(32 * q + 4))
                vs.append(load(north_s, 32 * q + 4))
            else:
                hs.append(pltpu.roll(hs[0], 7, 0))
                vs.append(pltpu.roll(vs[0], 7, 0))
            coefs = []
            for j in range(4):
                top = q == 3 and j == 3
                h, u = hs[j], load(east_s, 32 * q + j)
                rate = time_step / (area_s[row_set(32 * q + j)] * jnp.maximum(h, depth_floor))
                coefs.append(
                    face(h, pltpu.roll(h, 127, 1), u, pltpu.roll(u, 127, 1), mixing, keep=not_last)
                    + face(h, hs[j + 1], vs[j], vs[j + 1], mixing, keep=not_top if top else None)
                    + (rate,)
                )
            for t in range(TR):
                cells = [tr_s[(t, k, *row_set(32 * q + j))] for j in range(4)]
                if q < 3:
                    cells.append(tr_s[(t, k, *row_set(32 * q + 4))])
                else:
                    cells.append(pltpu.roll(cells[0], 7, 0))
                norths = [coefs[j][2] * cells[j] - coefs[j][3] * cells[j + 1] for j in range(4)]
                turned = pltpu.roll(norths[3], 1, 0)
                souths = [jnp.where(sub > 0, turned, before[t])] + norths[:3]
                before[t] = turned
                for j in range(4):
                    p_e, q_e, _, _, rate = coefs[j]
                    cell = cells[j]
                    flux = p_e * cell - q_e * pltpu.roll(cell, 127, 1)
                    div = (pltpu.roll(flux, 1, 1) - flux) + (souths[j] - norths[j])
                    moved = pltpu.roll(d_ew[4 * q + j], 127 - 2 * k + (128 - 32 * t), 1)
                    div = div + jnp.where(ends, moved, 0.0)
                    if q == 0 and j == 0:
                        div = div + jnp.where(sub == 0, d_ns[0, pl.ds(t * 16 + k, 1), :], 0.0)
                    if q == 3 and j == 3:
                        div = div + jnp.where(sub == 7, d_ns[1, pl.ds(t * 16 + k, 1), :], 0.0)
                    out_s[(t, k, *row_set(32 * q + j))] = cell + rate * div

    def group_body(group, carry):
        for copy in copies(group):
            copy.wait()
        for n in range(per):
            level(group * per + n)
        out_copy(group).start()
        return carry

    lax.fori_loop(0, GROUPS, group_body, 0)
    for group in range(GROUPS):
        out_copy(group).wait()


def kernel_third_call(tracers, fill, mask, east, north, diff, area, d_ew, d_ns):
    hbm = pl.BlockSpec(memory_space=pltpu.HBM)
    vmem = pl.BlockSpec(memory_space=pltpu.VMEM)
    return pl.pallas_call(
        kernel_third,
        name="third",
        out_shape=jax.ShapeDtypeStruct((TR, LV, ROWS, LANES), F32),
        in_specs=[hbm] * 5 + [pl.BlockSpec(memory_space=pltpu.SMEM), hbm, vmem, vmem],
        out_specs=hbm,
        scratch_shapes=[
            pltpu.VMEM((TR, LV, ROWS, LANES), F32),
            pltpu.VMEM((LV, ROWS, LANES), F32),
            pltpu.VMEM((LV, ROWS, LANES), jnp.int32),
            pltpu.VMEM((LV, ROWS, LANES), F32),
            pltpu.VMEM((LV, ROWS, LANES), F32),
            pltpu.VMEM((ROWS, LANES), F32),
            pltpu.VMEM((TR, LV, ROWS, LANES), F32),
            pltpu.SemaphoreType.DMA((5, GROUPS)),
            pltpu.SemaphoreType.DMA,
            pltpu.SemaphoreType.DMA((GROUPS,)),
        ],
        compiler_params=pltpu.CompilerParams(vmem_limit_bytes=24 * MIB),
        cost_estimate=pl.CostEstimate(flops=60_000_000, bytes_accessed=12 * MIB, transcendentals=0),
    )(tracers, fill, mask, east, north, diff, area, d_ew, d_ns)


SPLITS = 4


def kernel_last(got, two, four):
    for m in range(32 // SPLITS):
        for n in range(CHUNKS):
            value = got[pl.ds(m * 8 * CHUNKS + n, 8, stride=CHUNKS), :]
            if n < 16:
                two[pl.ds(m * 8, 8), pl.ds(n * 128, 128)] = value
            else:
                four[pl.ds(m * 8, 8), pl.ds((n - 16) * 128, 128)] = value


def kernel_last_call(got):
    return pl.pallas_call(
        kernel_last,
        name="last",
        grid=(SPLITS,),
        out_shape=(
            jax.ShapeDtypeStruct((DEV * CAP, 2048), F32),
            jax.ShapeDtypeStruct((DEV * CAP, 512), F32),
        ),
        in_specs=[pl.BlockSpec((DEV * 40 // SPLITS, 128), lambda s: (s, 0))],
        out_specs=(
            pl.BlockSpec((DEV * CAP // SPLITS, 2048), lambda s: (s, 0)),
            pl.BlockSpec((DEV * CAP // SPLITS, 512), lambda s: (s, 0)),
        ),
        compiler_params=pltpu.CompilerParams(vmem_limit_bytes=8 * MIB),
    )(got)


def local(
    tracers, fill_fraction, ocean_mask, east_speed, north_speed, diffusivity, cell_area, owner_map
):
    lon_count = lax.axis_size("lon")
    lat_count = lax.axis_size("lat")
    *fields, diffusivity, cell_area, owners = (
        pltpu.with_memory_space_constraint(x, pltpu.HBM)
        for x in (
            tracers, fill_fraction, ocean_mask, east_speed, north_speed, diffusivity, cell_area,
            owner_map.reshape(1, DEV),
        )
    )
    tracers, fill_fraction, ocean_mask, east_speed, north_speed = fields
    ns_one, ns_two = kernel_rows_call(tracers, fill_fraction, ocean_mask, north_speed)
    both = ("lon", "lat")

    def swapped(pairs):
        return [pair for a, b in pairs for pair in ((a, b), (b, a))]

    def at(lon, lat):
        return lon * lat_count + lat

    lons = range(lon_count)
    step_one = [(at(n, a), at(n, a + 1)) for n in lons for a in range(0, lat_count, 2)]
    step_two = [(at(n, a), at(n, a + 1)) for n in lons for a in range(1, lat_count - 1, 2)]
    fold = [
        (at(n, lat_count - 1), at(lon_count - 1 - n, lat_count - 1)) for n in range(lon_count // 2)
    ]
    got_one = lax.ppermute(ns_one, both, swapped(step_one))
    got_two = lax.ppermute(ns_two, both, swapped(step_two + fold))
    num2, den2, ew, placing = kernel_first_call(*fields, diffusivity, cell_area, owners)
    ew_one = lax.ppermute(ew, "lon", swapped([(n, n + 1) for n in range(0, lon_count, 2)]))
    ew_two = lax.ppermute(
        ew, "lon", swapped([(n, (n + 1) % lon_count) for n in range(1, lon_count, 2)])
    )
    send, d_ew, d_ns = kernel_second_call(
        num2, den2, ew, ew_one, ew_two, ns_one, ns_two, got_one, got_two, diffusivity, placing
    )
    got = lax.all_to_all(
        send.reshape(DEV, CAP * CHUNKS, 128), both, split_axis=0, concat_axis=0, tiled=True
    )
    updated = kernel_third_call(*fields, diffusivity, cell_area, d_ew, d_ns)
    two, four = kernel_last_call(got.reshape(DEV * CAP * CHUNKS, 128))
    return (updated, two[None], four[None])


def solution(mesh):
    in_specs = (
        P(None, None, "lat", "lon"),
        P(None, "lat", "lon"),
        P(None, "lat", "lon"),
        P(None, "lat", "lon"),
        P(None, "lat", "lon"),
        P(),
        P("lat", "lon"),
        P(("lon", "lat"), None),
    )
    out_specs = (
        P(None, None, "lat", "lon"),
        P(("lon", "lat"), None, None),
        P(("lon", "lat"), None, None),
    )
    return jax.shard_map(
        local,
        mesh=mesh, in_specs=in_specs, out_specs=out_specs, check_vma=False,
    )
```

```python
import jax
import jax.numpy as jnp
from jax import lax
from jax.experimental import pallas as pl
from jax.experimental.pallas import tpu as pltpu
from jax.sharding import PartitionSpec as P


time_step = 0.05
depth_floor = 0.25
weight_floor = 0.25

TR, LV = 4, 16
ROWS, LANES = 128, 128
GROUPS = 16
DEV, CAP = 128, 2
CHUNKS = 20
PARTS = 2
F32, BF16 = jnp.float32, jnp.bfloat16
MIB = 1 << 20


def lane_iota(shape=(8, 128)):
    return lax.broadcasted_iota(jnp.int32, shape, len(shape) - 1)


def sub_iota(shape=(8, 128)):
    return lax.broadcasted_iota(jnp.int32, shape, len(shape) - 2)


def face(lower_h, upper_h, lower_speed, upper_speed, mixing, keep=None):
    open_depth = jnp.minimum(lower_h, upper_h)
    if keep is not None:
        open_depth = jnp.where(keep, open_depth, 0.0)
    speed = 0.5 * (lower_speed + upper_speed)
    ahead = jnp.maximum(speed, 0.0)
    back = ahead - speed
    return open_depth * (ahead + mixing), open_depth * (back + mixing)


def halves(values):
    high = values.astype(BF16)
    return high, (values - high.astype(F32)).astype(BF16)


def split_dot(left, right):
    high, low = halves(left)
    return jnp.dot(high, right, preferred_element_type=F32) + jnp.dot(
        low, right, preferred_element_type=F32
    )


def input_copies(hbm, vmem, sems):
    per = LV // GROUPS

    def copies(group):
        levels = pl.ds(group * per, per)
        out = [pltpu.make_async_copy(hbm[0].at[:, levels], vmem[0].at[:, levels], sems.at[0, group])]
        for n in range(1, 5):
            out.append(
                pltpu.make_async_copy(hbm[n].at[levels], vmem[n].at[levels], sems.at[n, group])
            )
        return out

    return copies


def row_set(start):
    return (pl.ds(start, 8, stride=4), slice(None))


def kernel_rows(tr, fill, mask, north, ns_one, ns_two, tr_s, fill_s, mask_s, north_s, sems):
    copies = []
    for n, (src, dst) in enumerate(((tr, tr_s), (fill, fill_s), (mask, mask_s), (north, north_s))):
        for side in range(2):
            rows = pl.ds(side * (ROWS - 8), 8)
            if n == 0:
                copies.append(
                    pltpu.make_async_copy(src.at[:, :, rows], dst.at[side], sems.at[n, side])
                )
            else:
                copies.append(
                    pltpu.make_async_copy(src.at[:, rows], dst.at[side], sems.at[n, side])
                )
            copies[-1].start()
    for copy in copies:
        copy.wait()
    odd = lax.axis_index("lat") % 2 == 1
    for n in range(6):
        for half in range(2):
            levels = range(8 * half, 8 * half + 8)
            lines = []
            for side in range(2):
                row = 7 * side
                pick = lambda ref, k: ref[side, k, pl.ds(row, 1), :]
                if n < TR:
                    parts = [tr_s[side, n, k, pl.ds(row, 1), :] for k in levels]
                elif n == TR:
                    parts = [pick(fill_s, k) * pick(mask_s, k).astype(F32) for k in levels]
                else:
                    parts = [pick(north_s, k) for k in levels]
                lines.append(jnp.concatenate(parts, axis=0))
            at = pl.ds(n * 16 + 8 * half, 8)
            ns_one[at, :] = jnp.where(odd, lines[0], lines[1])
            ns_two[at, :] = jnp.where(odd, lines[1], lines[0])


def kernel_rows_call(tracers, fill, mask, north):
    hbm = pl.BlockSpec(memory_space=pltpu.HBM)
    vmem = pl.BlockSpec(memory_space=pltpu.VMEM)
    return pl.pallas_call(
        kernel_rows,
        name="rows",
        out_shape=(jax.ShapeDtypeStruct((96, 128), F32),) * 2,
        in_specs=[hbm] * 4,
        out_specs=(vmem,) * 2,
        scratch_shapes=[
            pltpu.VMEM((2, TR, LV, 8, LANES), F32),
            pltpu.VMEM((2, LV, 8, LANES), F32),
            pltpu.VMEM((2, LV, 8, LANES), jnp.int32),
            pltpu.VMEM((2, LV, 8, LANES), F32),
            pltpu.SemaphoreType.DMA((4, 2)),
        ],
        compiler_params=pltpu.CompilerParams(vmem_limit_bytes=4 * MIB),
        cost_estimate=pl.CostEstimate(flops=1_000_000, bytes_accessed=MIB, transcendentals=0),
    )(tracers, fill, mask, north)


def kernel_edges(
    tr, fill, mask, east, north, area, owner,
    tr_v, h_v, east_v, north_v, area_v, ew, placing,
    fill_s, mask_s, owner_s, sems, area_sem, owner_sem,
):
    copies = input_copies(
        (tr, fill, mask, east, north), (tr_v, fill_s, mask_s, east_v, north_v), sems
    )
    area_copy = pltpu.make_async_copy(area, area_v, area_sem)
    owner_copy = pltpu.make_async_copy(owner, owner_s, owner_sem)
    owner_copy.start()
    for group in range(GROUPS):
        for copy in copies(group):
            copy.start()
    area_copy.start()

    across = lane_iota((DEV, DEV))
    down = sub_iota((DEV, DEV))
    owner_copy.wait()
    who_row = owner_s[...]
    who = jnp.sum(jnp.where(down == across, who_row, 0), axis=1, keepdims=True)
    same = jnp.where((who == who_row) & (down < across), 1, 0)
    rank = jnp.sum(same, axis=0, keepdims=True)
    row_of = who_row * CAP + rank
    for part in range(CAP):
        here = jnp.where(down + part * DEV == row_of, 1.0, 0.0).astype(BF16)
        placing[pl.ds(part * DEV, DEV), 0:DEV] = here
        placing[pl.ds(part * DEV, DEV), DEV : 2 * DEV] = here

    lane = lane_iota()

    def level(k, carry):
        for copy in copies(k):
            copy.wait()
        where_t = [(lane >> 1) == t * 16 + k for t in range(TR)]
        for v in range(16):
            at = row_set(32 * (v // 4) + v % 4)
            h = fill_s[(k, *at)] * mask_s[(k, *at)].astype(F32)
            h_v[k, v] = h
            base = 64 * (v % 2)
            packed = ew[16 + v // 2]
            packed = jnp.where(
                (lane >> 1) == k + base // 2, pltpu.roll(h, 2 * k + 1 + base, 1), packed
            )
            ew[16 + v // 2] = jnp.where(
                (lane >> 1) == k + 16 + base // 2,
                pltpu.roll(east_v[(k, *at)], 2 * k + 33 + base, 1),
                packed,
            )
            packed = ew[v]
            for t in range(TR):
                moved = pltpu.roll(tr_v[(t, k, *at)], 2 * k + 32 * t + 1, 1)
                packed = jnp.where(where_t[t], moved, packed)
            ew[v] = packed
        return carry

    lax.fori_loop(0, LV, level, 0)
    area_copy.wait()


def kernel_edges_call(tracers, fill, mask, east, north, area, owner):
    hbm = pl.BlockSpec(memory_space=pltpu.HBM)
    vmem = pl.BlockSpec(memory_space=pltpu.VMEM)
    return pl.pallas_call(
        kernel_edges,
        name="edges",
        out_shape=(
            jax.ShapeDtypeStruct((TR, LV, ROWS, LANES), F32),
            jax.ShapeDtypeStruct((LV, 16, 8, LANES), F32),
            jax.ShapeDtypeStruct((LV, ROWS, LANES), F32),
            jax.ShapeDtypeStruct((LV, ROWS, LANES), F32),
            jax.ShapeDtypeStruct((ROWS, LANES), F32),
            jax.ShapeDtypeStruct((24, 8, 128), F32),
            jax.ShapeDtypeStruct((CAP * DEV, 2 * DEV), BF16),
        ),
        in_specs=[hbm] * 7,
        out_specs=(vmem,) * 7,
        scratch_shapes=[
            pltpu.VMEM((LV, ROWS, LANES), F32),
            pltpu.VMEM((LV, ROWS, LANES), jnp.int32),
            pltpu.VMEM((1, DEV), jnp.int32),
            pltpu.SemaphoreType.DMA((5, GROUPS)),
            pltpu.SemaphoreType.DMA,
            pltpu.SemaphoreType.DMA,
        ],
        compiler_params=pltpu.CompilerParams(vmem_limit_bytes=24 * MIB),
        cost_estimate=pl.CostEstimate(flops=60_000_000, bytes_accessed=11 * MIB, transcendentals=0),
    )(tracers, fill, mask, east, north, area, owner)


def kernel_first(
    tr_s, h_v, east_s, north_s, area_s, diff,
    num2, den2,
    g_s, face_s, coef, store, cross,
):
    source = sub_iota((256, 128))
    target = lane_iota((256, 128))
    pool = jnp.where(target == (source >> 7) * 64 + ((source & 127) >> 1), 1.0, 0.0).astype(BF16)
    beside = (source >> 7) * 64 + (((source & 127) + 1) >> 1) - jnp.where((source & 1) == 0, 1, 0)
    inside = ((source & 127) != 0) & ((source & 127) != 127)
    pool_cross = jnp.where((target == beside) & inside, 1.0, 0.0).astype(BF16)
    lane, sub = lane_iota(), sub_iota()
    is_even = (lane & 1) == 0
    not_last = lane < 127
    not_top = sub < 7

    def level(k):
        mixing = diff[k]

        def load(ref, start):
            return ref[(k, *row_set(start))]

        for v in range(16):
            start = 32 * (v // 4) + v % 4
            h, u = h_v[k, v], load(east_s, start)
            p_e, q_e = face(
                h, pltpu.roll(h, 127, 1), u, pltpu.roll(u, 127, 1), mixing, keep=not_last
            )
            g_s[v] = (time_step * h) / jnp.maximum(h, depth_floor)
            face_s[0, v] = p_e
            face_s[1, v] = q_e

        for v in range(16):
            q, j = v // 4, v % 4
            start = 32 * q + j
            h, speed = h_v[k, v], load(north_s, start)
            if j < 3:
                p_n, q_n = face(h, h_v[k, v + 1], speed, load(north_s, start + 1), mixing)
            elif q < 3:
                h_up = jnp.where(
                    sub < 7, pltpu.roll(h_v[k, v - 3], 7, 0), pltpu.roll(h_v[k, v + 1], 7, 0)
                )
                p_n, q_n = face(h, h_up, speed, load(north_s, start + 1), mixing)
            else:
                h_up, speed_up = pltpu.roll(h_v[k, 12], 7, 0), pltpu.roll(load(north_s, 96), 7, 0)
                p_n, q_n = face(h, h_up, speed, speed_up, mixing, keep=not_top)
            face_s[2, v] = p_n
            face_s[3, v] = q_n

        for q in range(4):
            south = []
            for n in (2, 3):
                low = pltpu.roll(face_s[n, 4 * q + 3], 1, 0)
                under = pltpu.roll(face_s[n, 4 * q - 1], 1, 0) if q else 0.0
                south.append(jnp.where(sub > 0, low, under))
            for par in range(2):
                centre, weight = [], 0.0
                for n in range(2):
                    v = 4 * q + 2 * par + n
                    h, g = h_v[k, v], g_s[v]
                    w = area_s[row_set(32 * q + 2 * par + n)] * h
                    p_e, q_w = face_s[0, v], pltpu.roll(face_s[1, v], 1, 1)
                    p_n, q_n = face_s[2, v], face_s[3, v]
                    p_s, q_s = south if v % 4 == 0 else (face_s[2, v - 1], face_s[3, v - 1])
                    to_west = pltpu.roll(g, 1, 1) * q_w
                    to_east = pltpu.roll(g, 127, 1) * p_e
                    own = w - g * ((p_e + q_w) + (p_n + q_s))
                    centre.append(own + jnp.where(is_even, to_east, to_west))
                    coef[4 + n, 2 * q + par] = jnp.where(is_even, to_west, to_east)
                    if n == 0:
                        low, up = g * p_s, g * q_n
                    else:
                        down, high = g * p_s, g * q_n
                    weight = weight + w
                coef[0, 2 * q + par] = low
                coef[1, 2 * q + par] = centre[0] + down
                coef[2, 2 * q + par] = centre[1] + up
                coef[3, 2 * q + par] = high
                store[pl.ds(128 + q * 8, 8), pl.ds(par * 128, 128)] = weight

        for q in range(4):
            for par in range(2):
                low_c, a_c, b_c, high_c, a_x, b_x = [coef[n, 2 * q + par] for n in range(6)]
                for t in range(TR):
                    cell = lambda start: tr_s[(t, k, *row_set(start))]
                    start = 32 * q + 2 * par
                    a, b = cell(start), cell(start + 1)
                    low = cell(start - 1) if start else pltpu.roll(cell(3), 1, 0)
                    high = cell(start + 2) if start < 98 else pltpu.roll(cell(96), 7, 0)
                    side = a_x * a + b_x * b
                    value = (a_c * a + b_c * b) + (low_c * low + high_c * high)
                    cross[pl.ds(t * 32 + q * 8, 8), pl.ds(par * 128, 128)] = side
                    store[pl.ds(t * 32 + q * 8, 8), pl.ds(par * 128, 128)] = value

    def pooled(k):
        values = split_dot(store[...], pool)
        sides = split_dot(cross[...], pool_cross)
        rows = pl.ds(pl.multiple_of(k * 32, 32), 32)
        for t in range(TR):
            part = slice(t * 32, t * 32 + 32)
            num2[t, rows, :] = values[part] + sides[part]
        den2[rows, :] = values[128:160]

    def group_body(k, carry):
        pooled((k + LV - 1) % LV)
        level(k)
        return carry

    store[...] = jnp.zeros_like(store)
    cross[...] = jnp.zeros_like(cross)
    lax.fori_loop(0, LV, group_body, 0)
    pooled(LV - 1)


def kernel_first_call(tr_v, h_v, east_v, north_v, area_v, diff):
    vmem = pl.BlockSpec(memory_space=pltpu.VMEM)
    return pl.pallas_call(
        kernel_first,
        name="first",
        out_shape=(
            jax.ShapeDtypeStruct((TR, 512, 128), F32),
            jax.ShapeDtypeStruct((512, 128), F32),
        ),
        in_specs=[vmem] * 5 + [pl.BlockSpec(memory_space=pltpu.SMEM)],
        out_specs=(vmem,) * 2,
        scratch_shapes=[
            pltpu.VMEM((16, 8, 128), F32),
            pltpu.VMEM((4, 16, 8, 128), F32),
            pltpu.VMEM((6, 8, 8, 128), F32),
            pltpu.VMEM((160, 256), F32),
            pltpu.VMEM((128, 256), F32),
        ],
        compiler_params=pltpu.CompilerParams(vmem_limit_bytes=16 * MIB),
        cost_estimate=pl.CostEstimate(flops=60_000_000, bytes_accessed=11 * MIB, transcendentals=0),
    )(tr_v, h_v, east_v, north_v, area_v, diff)


def spread(values, offset):
    index = (lane_iota() & 31) + offset
    return jnp.take_along_axis(values, index, axis=1)


def kernel_second(
    num2, den2, ew, ew_one, ew_two, ns_one, ns_two, got_one, got_two, diff, placing,
    send, d_ew, d_ns,
    work, acc, chunks, send_s, sems,
):
    lane, sub = lane_iota(), sub_iota()
    odd = lax.axis_index("lat") % 2 == 1
    odd_lon = lax.axis_index("lon") % 2 == 1
    at_fold = lax.axis_index("lat") == lax.axis_size("lat") - 1
    is_east = (lane & 1) == 0
    level_of = (lane >> 1) & 15
    mixing = jnp.zeros((8, 128), F32)
    for k in range(LV):
        mixing = jnp.where(level_of == k, diff[k], mixing)

    def neighbour(n):
        one, two = ew_one[n], ew_two[n]
        from_east, from_west = jnp.where(odd_lon, two, one), jnp.where(odd_lon, one, two)
        return jnp.where(is_east, pltpu.roll(from_east, 127, 1), pltpu.roll(from_west, 1, 1))

    pending = None
    for v in range(16):
        own_hu, near_hu = ew[16 + v // 2], neighbour(16 + v // 2)
        base = 64 * (v % 2)
        h = spread(own_hu, base)
        p, q = face(
            h, spread(near_hu, base), spread(own_hu, base + 32), spread(near_hu, base + 32), mixing
        )
        div = jnp.where(is_east, q, p) * neighbour(v) - jnp.where(is_east, p, q) * ew[v]
        d_ew[v] = div
        value = (time_step * h) / jnp.maximum(h, depth_floor) * div
        if v % 2 == 0:
            pending = value
        else:
            value = pending + value
            work[v // 2] = jnp.where(is_east, value, pltpu.roll(value, 64, 1))

    low_ends = (lane == 0) | (lane == 63)
    high_ends = (lane == 64) | (lane == 127)

    def add_ends(k, carry):
        for t in range(TR):
            for q in range(4):
                rows = pl.ds(pl.multiple_of(k * 32 + q * 8, 8), 8)
                shift = 127 - 2 * k + (128 - 32 * t)
                low = pltpu.roll(work[2 * q], shift - 64, 1)
                high = pltpu.roll(work[2 * q + 1], shift, 1)
                edge = jnp.where(low_ends, low, jnp.where(high_ends, high, 0.0))
                acc[t, rows, :] = num2[t, rows, :] + edge
        return carry

    lax.fori_loop(0, LV, add_ends, 0)

    source = sub_iota((128, 128))
    target = lane_iota((128, 128))
    pools = [
        jnp.where(target == par * 64 + (source >> 1), 1.0, 0.0).astype(BF16) for par in range(2)
    ]
    quarter = [
        jnp.where(target == j * 32 + ((source & 63) >> 1), 1.0, 0.0).astype(BF16) for j in range(4)
    ]

    back = 127 - lane
    for half in range(2):
        mix = jnp.zeros((8, 128), F32)
        for k in range(8):
            mix = jnp.where(sub == k, diff[8 * half + k], mix)

        def rows_of(ref, n):
            return ref[pl.ds(n * 16 + 8 * half, 8), :]

        def own(n, top):
            pair = (ns_two, ns_one) if top else (ns_one, ns_two)
            return jnp.where(odd, rows_of(pair[0], n), rows_of(pair[1], n))

        def near(n, top, sign=1.0):
            if not top:
                return jnp.where(odd, rows_of(got_one, n), rows_of(got_two, n))
            value = jnp.where(odd, rows_of(got_two, n), rows_of(got_one, n))
            turned = sign * jnp.take_along_axis(value, back, axis=1)
            return jnp.where(at_fold, turned, value)

        for top in (False, True):
            h = own(4, top)
            p, q = face(h, near(4, top), own(5, top), near(5, top, -1.0), mix)
            gain = (time_step * h) / jnp.maximum(h, depth_floor)
            for t in range(TR):
                if top:
                    div = q * near(t, top) - p * own(t, top)
                else:
                    div = p * near(t, top) - q * own(t, top)
                d_ns[int(top), pl.ds(t * 16 + 8 * half, 8), :] = div
                at = (t, pl.ds(256 * half + 31 * int(top), 8, stride=32), slice(None))
                acc[at] = acc[at] + split_dot(gain * div, pools[int(top)])

    def keep(n, values):
        high, low = halves(values)
        chunks[0:128, pl.ds(n * 128, 128)] = high
        chunks[128:256, pl.ds(n * 128, 128)] = low

    def every_fourth(ref, *lead, j):
        return jnp.concatenate(
            [ref[(*lead, pl.ds(32 * m + j, 8, stride=4), slice(None))] for m in range(16)], axis=0
        )

    gains = []
    den4 = jnp.zeros((128, 128), F32)
    for j in range(4):
        den = every_fourth(den2, j=j)
        gains.append(1.0 / jnp.maximum(den, weight_floor))
        den4 = den4 + split_dot(den, quarter[j])
    gain4 = 1.0 / jnp.maximum(den4, weight_floor)
    for t in range(TR):
        num4 = jnp.zeros((128, 128), F32)
        for j in range(4):
            num = every_fourth(acc, t, j=j)
            keep(t * 4 + j, num * gains[j])
            num4 = num4 + split_dot(num, quarter[j])
        keep(16 + t, num4 * gain4)

    each = CAP * DEV // PARTS
    copies = []
    for part in range(PARTS):
        left = placing[pl.ds(part * each, each), :]
        for n in range(CHUNKS // 2):
            placed = jnp.dot(left, chunks[:, pl.ds(n * 256, 256)], preferred_element_type=F32)
            for c in range(2):
                for m in range(each // 8):
                    start = (part * each + m * 8) * CHUNKS + 2 * n + c
                    send_s[pl.ds(start, 8, stride=CHUNKS), :] = placed[
                        m * 8 : m * 8 + 8, c * 128 : c * 128 + 128
                    ]
        rows = pl.ds(part * each * CHUNKS, each * CHUNKS)
        copies.append(pltpu.make_async_copy(send_s.at[rows], send.at[rows], sems.at[part]))
        copies[-1].start()
    for copy in copies:
        copy.wait()


def kernel_second_call(*args):
    vmem = pl.BlockSpec(memory_space=pltpu.VMEM)
    return pl.pallas_call(
        kernel_second,
        name="second",
        out_shape=(
            pltpu.HBM((DEV * CAP * CHUNKS, 128), F32),
            jax.ShapeDtypeStruct((16, 8, 128), F32),
            jax.ShapeDtypeStruct((2, 64, 128), F32),
        ),
        in_specs=[vmem] * 9 + [pl.BlockSpec(memory_space=pltpu.SMEM), vmem],
        out_specs=(pl.BlockSpec(memory_space=pltpu.HBM), vmem, vmem),
        scratch_shapes=[
            pltpu.VMEM((8, 8, 128), F32),
            pltpu.VMEM((TR, 512, 128), F32),
            pltpu.VMEM((256, 2560), BF16),
            pltpu.VMEM((DEV * CAP * CHUNKS, 128), F32),
            pltpu.SemaphoreType.DMA((PARTS,)),
        ],
        compiler_params=pltpu.CompilerParams(vmem_limit_bytes=16 * MIB),
        cost_estimate=pl.CostEstimate(flops=60_000_000, bytes_accessed=6 * MIB, transcendentals=0),
    )(*args)


def kernel_third(
    tr, fill, mask, east, north, diff, area, d_ew, d_ns,
    out,
    tr_s, fill_s, mask_s, east_s, north_s, area_s, out_s, moved_s, sems, area_sem, out_sems,
):
    hbm, vmem = (tr, fill, mask, east, north), (tr_s, fill_s, mask_s, east_s, north_s)
    copies = input_copies(hbm, vmem, sems)
    area_copy = pltpu.make_async_copy(area, area_s, area_sem)
    for group in range(GROUPS):
        for copy in copies(group):
            copy.start()
        if group == 0:
            area_copy.start()
    area_copy.wait()
    lane, sub = lane_iota(), sub_iota()
    ends = (lane == 0) | (lane == 127)
    not_last, not_top = lane < 127, sub < 7
    per = LV // GROUPS

    def out_copy(group):
        levels = pl.ds(group * per, per)
        return pltpu.make_async_copy(out_s.at[:, levels], out.at[:, levels], out_sems.at[group])

    def level(k):
        mixing = diff[k]

        def load(ref, start):
            return ref[(k, *row_set(start))]

        def depth(start):
            return load(fill_s, start) * load(mask_s, start).astype(F32)

        for v in range(16):
            edge = d_ew[v]
            for t in range(TR):
                moved = pltpu.roll(edge, 127 - 2 * k + (128 - 32 * t), 1)
                moved_s[v, t] = jnp.where(ends, moved, 0.0)

        before = [jnp.zeros((8, 128), F32)] * TR
        for q in range(4):
            hs = [depth(32 * q + j) for j in range(4)]
            vs = [load(north_s, 32 * q + j) for j in range(4)]
            if q < 3:
                hs.append(depth(32 * q + 4))
                vs.append(load(north_s, 32 * q + 4))
            else:
                hs.append(pltpu.roll(hs[0], 7, 0))
                vs.append(pltpu.roll(vs[0], 7, 0))
            coefs = []
            for j in range(4):
                top = q == 3 and j == 3
                h, u = hs[j], load(east_s, 32 * q + j)
                rate = time_step / (area_s[row_set(32 * q + j)] * jnp.maximum(h, depth_floor))
                coefs.append(
                    face(h, pltpu.roll(h, 127, 1), u, pltpu.roll(u, 127, 1), mixing, keep=not_last)
                    + face(h, hs[j + 1], vs[j], vs[j + 1], mixing, keep=not_top if top else None)
                    + (rate,)
                )
            for t in range(TR):
                cells = [tr_s[(t, k, *row_set(32 * q + j))] for j in range(4)]
                if q < 3:
                    cells.append(tr_s[(t, k, *row_set(32 * q + 4))])
                else:
                    cells.append(pltpu.roll(cells[0], 7, 0))
                norths = [coefs[j][2] * cells[j] - coefs[j][3] * cells[j + 1] for j in range(4)]
                turned = pltpu.roll(norths[3], 1, 0)
                souths = [jnp.where(sub > 0, turned, before[t])] + norths[:3]
                before[t] = turned
                for j in range(4):
                    p_e, q_e, _, _, rate = coefs[j]
                    cell = cells[j]
                    flux = p_e * cell - q_e * pltpu.roll(cell, 127, 1)
                    div = (pltpu.roll(flux, 1, 1) - flux) + (souths[j] - norths[j])
                    div = div + moved_s[4 * q + j, t]
                    if q == 0 and j == 0:
                        div = div + jnp.where(sub == 0, d_ns[0, pl.ds(t * 16 + k, 1), :], 0.0)
                    if q == 3 and j == 3:
                        div = div + jnp.where(sub == 7, d_ns[1, pl.ds(t * 16 + k, 1), :], 0.0)
                    out_s[(t, k, *row_set(32 * q + j))] = cell + rate * div

    def group_body(group, carry):
        for copy in copies(group):
            copy.wait()
        for n in range(per):
            level(group * per + n)
        out_copy(group).start()
        return carry

    lax.fori_loop(0, GROUPS, group_body, 0)
    for group in range(GROUPS):
        out_copy(group).wait()


def kernel_third_call(tracers, fill, mask, east, north, diff, area, d_ew, d_ns):
    hbm = pl.BlockSpec(memory_space=pltpu.HBM)
    vmem = pl.BlockSpec(memory_space=pltpu.VMEM)
    return pl.pallas_call(
        kernel_third,
        name="third",
        out_shape=jax.ShapeDtypeStruct((TR, LV, ROWS, LANES), F32),
        in_specs=[hbm] * 5 + [pl.BlockSpec(memory_space=pltpu.SMEM), hbm, vmem, vmem],
        out_specs=hbm,
        scratch_shapes=[
            pltpu.VMEM((TR, LV, ROWS, LANES), F32),
            pltpu.VMEM((LV, ROWS, LANES), F32),
            pltpu.VMEM((LV, ROWS, LANES), jnp.int32),
            pltpu.VMEM((LV, ROWS, LANES), F32),
            pltpu.VMEM((LV, ROWS, LANES), F32),
            pltpu.VMEM((ROWS, LANES), F32),
            pltpu.VMEM((TR, LV, ROWS, LANES), F32),
            pltpu.VMEM((16, TR, 8, 128), F32),
            pltpu.SemaphoreType.DMA((5, GROUPS)),
            pltpu.SemaphoreType.DMA,
            pltpu.SemaphoreType.DMA((GROUPS,)),
        ],
        compiler_params=pltpu.CompilerParams(vmem_limit_bytes=24 * MIB),
        cost_estimate=pl.CostEstimate(flops=60_000_000, bytes_accessed=12 * MIB, transcendentals=0),
    )(tracers, fill, mask, east, north, diff, area, d_ew, d_ns)


SPLITS = 4


def kernel_last(got, two, four):
    for m in range(32 // SPLITS):
        for n in range(CHUNKS):
            value = got[pl.ds(m * 8 * CHUNKS + n, 8, stride=CHUNKS), :]
            if n < 16:
                two[pl.ds(m * 8, 8), pl.ds(n * 128, 128)] = value
            else:
                four[pl.ds(m * 8, 8), pl.ds((n - 16) * 128, 128)] = value


def kernel_last_call(got):
    return pl.pallas_call(
        kernel_last,
        name="last",
        grid=(SPLITS,),
        out_shape=(
            jax.ShapeDtypeStruct((DEV * CAP, 2048), F32),
            jax.ShapeDtypeStruct((DEV * CAP, 512), F32),
        ),
        in_specs=[pl.BlockSpec((DEV * 40 // SPLITS, 128), lambda s: (s, 0))],
        out_specs=(
            pl.BlockSpec((DEV * CAP // SPLITS, 2048), lambda s: (s, 0)),
            pl.BlockSpec((DEV * CAP // SPLITS, 512), lambda s: (s, 0)),
        ),
        compiler_params=pltpu.CompilerParams(vmem_limit_bytes=8 * MIB),
    )(got)


def local(
    tracers, fill_fraction, ocean_mask, east_speed, north_speed, diffusivity, cell_area, owner_map
):
    lon_count = lax.axis_size("lon")
    lat_count = lax.axis_size("lat")
    *fields, diffusivity, cell_area, owners = (
        pltpu.with_memory_space_constraint(x, pltpu.HBM)
        for x in (
            tracers, fill_fraction, ocean_mask, east_speed, north_speed, diffusivity, cell_area,
            owner_map.reshape(1, DEV),
        )
    )
    tracers, fill_fraction, ocean_mask, east_speed, north_speed = fields
    ns_one, ns_two = kernel_rows_call(tracers, fill_fraction, ocean_mask, north_speed)
    both = ("lon", "lat")

    def swapped(pairs):
        return [pair for a, b in pairs for pair in ((a, b), (b, a))]

    def at(lon, lat):
        return lon * lat_count + lat

    lons = range(lon_count)
    step_one = [(at(n, a), at(n, a + 1)) for n in lons for a in range(0, lat_count, 2)]
    step_two = [(at(n, a), at(n, a + 1)) for n in lons for a in range(1, lat_count - 1, 2)]
    fold = [
        (at(n, lat_count - 1), at(lon_count - 1 - n, lat_count - 1)) for n in range(lon_count // 2)
    ]
    got_one = lax.ppermute(ns_one, both, swapped(step_one))
    got_two = lax.ppermute(ns_two, both, swapped(step_two + fold))
    *held, ew, placing = kernel_edges_call(*fields, cell_area, owners)
    ew_one = lax.ppermute(ew, "lon", swapped([(n, n + 1) for n in range(0, lon_count, 2)]))
    ew_two = lax.ppermute(
        ew, "lon", swapped([(n, (n + 1) % lon_count) for n in range(1, lon_count, 2)])
    )
    num2, den2 = kernel_first_call(*held, diffusivity)
    send, d_ew, d_ns = kernel_second_call(
        num2, den2, ew, ew_one, ew_two, ns_one, ns_two, got_one, got_two, diffusivity, placing
    )
    got = lax.all_to_all(
        send.reshape(DEV, CAP * CHUNKS, 128), both, split_axis=0, concat_axis=0, tiled=True
    )
    updated = kernel_third_call(*fields, diffusivity, cell_area, d_ew, d_ns)
    two, four = kernel_last_call(got.reshape(DEV * CAP * CHUNKS, 128))
    return (updated, two[None], four[None])


def solution(mesh):
    in_specs = (
        P(None, None, "lat", "lon"),
        P(None, "lat", "lon"),
        P(None, "lat", "lon"),
        P(None, "lat", "lon"),
        P(None, "lat", "lon"),
        P(),
        P("lat", "lon"),
        P(("lon", "lat"), None),
    )
    out_specs = (
        P(None, None, "lat", "lon"),
        P(("lon", "lat"), None, None),
        P(("lon", "lat"), None, None),
    )
    return jax.shard_map(
        local,
        mesh=mesh, in_specs=in_specs, out_specs=out_specs, check_vma=False,
    )
```

```python
import jax
import jax.numpy as jnp
from jax import lax
from jax.experimental import pallas as pl
from jax.experimental.pallas import tpu as pltpu
from jax.sharding import PartitionSpec as P


time_step = 0.05
depth_floor = 0.25
weight_floor = 0.25

TR, LV = 4, 16
ROWS, LANES = 128, 128
GROUPS = 16
DEV, CAP = 128, 2
CHUNKS = 20
PARTS = 2
F32, BF16 = jnp.float32, jnp.bfloat16
MIB = 1 << 20


def lane_iota(shape=(8, 128)):
    return lax.broadcasted_iota(jnp.int32, shape, len(shape) - 1)


def sub_iota(shape=(8, 128)):
    return lax.broadcasted_iota(jnp.int32, shape, len(shape) - 2)


def face(lower_h, upper_h, lower_speed, upper_speed, mixing, keep=None):
    open_depth = jnp.minimum(lower_h, upper_h)
    if keep is not None:
        open_depth = jnp.where(keep, open_depth, 0.0)
    speed = 0.5 * (lower_speed + upper_speed)
    ahead = jnp.maximum(speed, 0.0)
    back = ahead - speed
    return open_depth * (ahead + mixing), open_depth * (back + mixing)


def halves(values):
    high = values.astype(BF16)
    return high, (values - high.astype(F32)).astype(BF16)


def split_dot(left, right):
    high, low = halves(left)
    return jnp.dot(high, right, preferred_element_type=F32) + jnp.dot(
        low, right, preferred_element_type=F32
    )


def input_copies(hbm, vmem, sems):
    per = LV // GROUPS

    def copies(group):
        levels = pl.ds(group * per, per)
        out = [pltpu.make_async_copy(hbm[0].at[:, levels], vmem[0].at[:, levels], sems.at[0, group])]
        for n in range(1, 5):
            out.append(
                pltpu.make_async_copy(hbm[n].at[levels], vmem[n].at[levels], sems.at[n, group])
            )
        return out

    return copies


def row_set(start):
    return (pl.ds(start, 8, stride=4), slice(None))


def kernel_rows(tr, fill, mask, north, ns_one, ns_two, tr_s, fill_s, mask_s, north_s, sems):
    copies = []
    for n, (src, dst) in enumerate(((tr, tr_s), (fill, fill_s), (mask, mask_s), (north, north_s))):
        for side in range(2):
            rows = pl.ds(side * (ROWS - 8), 8)
            if n == 0:
                copies.append(
                    pltpu.make_async_copy(src.at[:, :, rows], dst.at[side], sems.at[n, side])
                )
            else:
                copies.append(
                    pltpu.make_async_copy(src.at[:, rows], dst.at[side], sems.at[n, side])
                )
            copies[-1].start()
    for copy in copies:
        copy.wait()
    odd = lax.axis_index("lat") % 2 == 1
    for n in range(6):
        for half in range(2):
            levels = range(8 * half, 8 * half + 8)
            lines = []
            for side in range(2):
                row = 7 * side
                pick = lambda ref, k: ref[side, k, pl.ds(row, 1), :]
                if n < TR:
                    parts = [tr_s[side, n, k, pl.ds(row, 1), :] for k in levels]
                elif n == TR:
                    parts = [pick(fill_s, k) * pick(mask_s, k).astype(F32) for k in levels]
                else:
                    parts = [pick(north_s, k) for k in levels]
                lines.append(jnp.concatenate(parts, axis=0))
            at = pl.ds(n * 16 + 8 * half, 8)
            ns_one[at, :] = jnp.where(odd, lines[0], lines[1])
            ns_two[at, :] = jnp.where(odd, lines[1], lines[0])


def kernel_rows_call(tracers, fill, mask, north):
    hbm = pl.BlockSpec(memory_space=pltpu.HBM)
    vmem = pl.BlockSpec(memory_space=pltpu.VMEM)
    return pl.pallas_call(
        kernel_rows,
        name="rows",
        out_shape=(jax.ShapeDtypeStruct((96, 128), F32),) * 2,
        in_specs=[hbm] * 4,
        out_specs=(vmem,) * 2,
        scratch_shapes=[
            pltpu.VMEM((2, TR, LV, 8, LANES), F32),
            pltpu.VMEM((2, LV, 8, LANES), F32),
            pltpu.VMEM((2, LV, 8, LANES), jnp.int32),
            pltpu.VMEM((2, LV, 8, LANES), F32),
            pltpu.SemaphoreType.DMA((4, 2)),
        ],
        compiler_params=pltpu.CompilerParams(vmem_limit_bytes=4 * MIB),
        cost_estimate=pl.CostEstimate(flops=1_000_000, bytes_accessed=MIB, transcendentals=0),
    )(tracers, fill, mask, north)


def kernel_edges(tr_v, fill_v, mask_v, east_v, owner, h_v, ew, placing):
    across = lane_iota((DEV, DEV))
    down = sub_iota((DEV, DEV))
    who_row = owner[...]
    who = jnp.sum(jnp.where(down == across, who_row, 0), axis=1, keepdims=True)
    same = jnp.where((who == who_row) & (down < across), 1, 0)
    rank = jnp.sum(same, axis=0, keepdims=True)
    row_of = who_row * CAP + rank
    for part in range(CAP):
        here = jnp.where(down + part * DEV == row_of, 1.0, 0.0).astype(BF16)
        placing[pl.ds(part * DEV, DEV), 0:DEV] = here
        placing[pl.ds(part * DEV, DEV), DEV : 2 * DEV] = here

    lane = lane_iota()

    def level(k, carry):
        where_t = [(lane >> 1) == t * 16 + k for t in range(TR)]
        for v in range(16):
            at = row_set(32 * (v // 4) + v % 4)
            h = fill_v[(k, *at)] * mask_v[(k, *at)].astype(F32)
            h_v[k, v] = h
            base = 64 * (v % 2)
            packed = ew[16 + v // 2]
            packed = jnp.where(
                (lane >> 1) == k + base // 2, pltpu.roll(h, 2 * k + 1 + base, 1), packed
            )
            ew[16 + v // 2] = jnp.where(
                (lane >> 1) == k + 16 + base // 2,
                pltpu.roll(east_v[(k, *at)], 2 * k + 33 + base, 1),
                packed,
            )
            packed = ew[v]
            for t in range(TR):
                moved = pltpu.roll(tr_v[(t, k, *at)], 2 * k + 32 * t + 1, 1)
                packed = jnp.where(where_t[t], moved, packed)
            ew[v] = packed
        return carry

    lax.fori_loop(0, LV, level, 0)


def kernel_edges_call(tracers, fill, mask, east, owner):
    vmem = pl.BlockSpec(memory_space=pltpu.VMEM)
    return pl.pallas_call(
        kernel_edges,
        name="edges",
        out_shape=(
            jax.ShapeDtypeStruct((LV, 16, 8, LANES), F32),
            jax.ShapeDtypeStruct((24, 8, 128), F32),
            jax.ShapeDtypeStruct((CAP * DEV, 2 * DEV), BF16),
        ),
        in_specs=[vmem] * 5,
        out_specs=(vmem,) * 3,
        compiler_params=pltpu.CompilerParams(vmem_limit_bytes=16 * MIB),
        cost_estimate=pl.CostEstimate(flops=60_000_000, bytes_accessed=11 * MIB, transcendentals=0),
    )(tracers, fill, mask, east, owner)


def kernel_first(
    tr_s, h_v, east_s, north_s, area_s, diff,
    num2, den2,
    g_s, face_s, coef, store, cross,
):
    source = sub_iota((256, 128))
    target = lane_iota((256, 128))
    pool = jnp.where(target == (source >> 7) * 64 + ((source & 127) >> 1), 1.0, 0.0).astype(BF16)
    beside = (source >> 7) * 64 + (((source & 127) + 1) >> 1) - jnp.where((source & 1) == 0, 1, 0)
    inside = ((source & 127) != 0) & ((source & 127) != 127)
    pool_cross = jnp.where((target == beside) & inside, 1.0, 0.0).astype(BF16)
    lane, sub = lane_iota(), sub_iota()
    is_even = (lane & 1) == 0
    not_last = lane < 127
    not_top = sub < 7

    def level(k):
        mixing = diff[k]

        def load(ref, start):
            return ref[(k, *row_set(start))]

        for v in range(16):
            start = 32 * (v // 4) + v % 4
            h, u = h_v[k, v], load(east_s, start)
            p_e, q_e = face(
                h, pltpu.roll(h, 127, 1), u, pltpu.roll(u, 127, 1), mixing, keep=not_last
            )
            g_s[v] = (time_step * h) / jnp.maximum(h, depth_floor)
            face_s[0, v] = p_e
            face_s[1, v] = q_e

        for v in range(16):
            q, j = v // 4, v % 4
            start = 32 * q + j
            h, speed = h_v[k, v], load(north_s, start)
            if j < 3:
                p_n, q_n = face(h, h_v[k, v + 1], speed, load(north_s, start + 1), mixing)
            elif q < 3:
                h_up = jnp.where(
                    sub < 7, pltpu.roll(h_v[k, v - 3], 7, 0), pltpu.roll(h_v[k, v + 1], 7, 0)
                )
                p_n, q_n = face(h, h_up, speed, load(north_s, start + 1), mixing)
            else:
                h_up, speed_up = pltpu.roll(h_v[k, 12], 7, 0), pltpu.roll(load(north_s, 96), 7, 0)
                p_n, q_n = face(h, h_up, speed, speed_up, mixing, keep=not_top)
            face_s[2, v] = p_n
            face_s[3, v] = q_n

        for q in range(4):
            south = []
            for n in (2, 3):
                low = pltpu.roll(face_s[n, 4 * q + 3], 1, 0)
                under = pltpu.roll(face_s[n, 4 * q - 1], 1, 0) if q else 0.0
                south.append(jnp.where(sub > 0, low, under))
            for par in range(2):
                centre, weight = [], 0.0
                for n in range(2):
                    v = 4 * q + 2 * par + n
                    h, g = h_v[k, v], g_s[v]
                    w = area_s[row_set(32 * q + 2 * par + n)] * h
                    p_e, q_w = face_s[0, v], pltpu.roll(face_s[1, v], 1, 1)
                    p_n, q_n = face_s[2, v], face_s[3, v]
                    p_s, q_s = south if v % 4 == 0 else (face_s[2, v - 1], face_s[3, v - 1])
                    to_west = pltpu.roll(g, 1, 1) * q_w
                    to_east = pltpu.roll(g, 127, 1) * p_e
                    own = w - g * ((p_e + q_w) + (p_n + q_s))
                    centre.append(own + jnp.where(is_even, to_east, to_west))
                    coef[4 + n, 2 * q + par] = jnp.where(is_even, to_west, to_east)
                    if n == 0:
                        low, up = g * p_s, g * q_n
                    else:
                        down, high = g * p_s, g * q_n
                    weight = weight + w
                coef[0, 2 * q + par] = low
                coef[1, 2 * q + par] = centre[0] + down
                coef[2, 2 * q + par] = centre[1] + up
                coef[3, 2 * q + par] = high
                store[pl.ds(128 + q * 8, 8), pl.ds(par * 128, 128)] = weight

        for q in range(4):
            for par in range(2):
                low_c, a_c, b_c, high_c, a_x, b_x = [coef[n, 2 * q + par] for n in range(6)]
                for t in range(TR):
                    cell = lambda start: tr_s[(t, k, *row_set(start))]
                    start = 32 * q + 2 * par
                    a, b = cell(start), cell(start + 1)
                    low = cell(start - 1) if start else pltpu.roll(cell(3), 1, 0)
                    high = cell(start + 2) if start < 98 else pltpu.roll(cell(96), 7, 0)
                    side = a_x * a + b_x * b
                    value = (a_c * a + b_c * b) + (low_c * low + high_c * high)
                    cross[pl.ds(t * 32 + q * 8, 8), pl.ds(par * 128, 128)] = side
                    store[pl.ds(t * 32 + q * 8, 8), pl.ds(par * 128, 128)] = value

    def pooled(k):
        values = split_dot(store[...], pool)
        sides = split_dot(cross[...], pool_cross)
        rows = pl.ds(pl.multiple_of(k * 32, 32), 32)
        for t in range(TR):
            part = slice(t * 32, t * 32 + 32)
            num2[t, rows, :] = values[part] + sides[part]
        den2[rows, :] = values[128:160]

    def group_body(k, carry):
        pooled((k + LV - 1) % LV)
        level(k)
        return carry

    store[...] = jnp.zeros_like(store)
    cross[...] = jnp.zeros_like(cross)
    lax.fori_loop(0, LV, group_body, 0)
    pooled(LV - 1)


def kernel_first_call(tr_v, h_v, east_v, north_v, area_v, diff):
    vmem = pl.BlockSpec(memory_space=pltpu.VMEM)
    return pl.pallas_call(
        kernel_first,
        name="first",
        out_shape=(
            jax.ShapeDtypeStruct((TR, 512, 128), F32),
            jax.ShapeDtypeStruct((512, 128), F32),
        ),
        in_specs=[vmem] * 5 + [pl.BlockSpec(memory_space=pltpu.SMEM)],
        out_specs=(vmem,) * 2,
        scratch_shapes=[
            pltpu.VMEM((16, 8, 128), F32),
            pltpu.VMEM((4, 16, 8, 128), F32),
            pltpu.VMEM((6, 8, 8, 128), F32),
            pltpu.VMEM((160, 256), F32),
            pltpu.VMEM((128, 256), F32),
        ],
        compiler_params=pltpu.CompilerParams(vmem_limit_bytes=16 * MIB),
        cost_estimate=pl.CostEstimate(flops=60_000_000, bytes_accessed=11 * MIB, transcendentals=0),
    )(tr_v, h_v, east_v, north_v, area_v, diff)


def spread(values, offset):
    index = (lane_iota() & 31) + offset
    return jnp.take_along_axis(values, index, axis=1)


def kernel_second(
    num2, den2, ew, ew_one, ew_two, ns_one, ns_two, got_one, got_two, diff, placing,
    send, d_ew, d_ns,
    work, acc, chunks, send_s, sems,
):
    lane, sub = lane_iota(), sub_iota()
    odd = lax.axis_index("lat") % 2 == 1
    odd_lon = lax.axis_index("lon") % 2 == 1
    at_fold = lax.axis_index("lat") == lax.axis_size("lat") - 1
    is_east = (lane & 1) == 0
    level_of = (lane >> 1) & 15
    mixing = jnp.zeros((8, 128), F32)
    for k in range(LV):
        mixing = jnp.where(level_of == k, diff[k], mixing)

    def neighbour(n):
        one, two = ew_one[n], ew_two[n]
        from_east, from_west = jnp.where(odd_lon, two, one), jnp.where(odd_lon, one, two)
        return jnp.where(is_east, pltpu.roll(from_east, 127, 1), pltpu.roll(from_west, 1, 1))

    pending = None
    for v in range(16):
        own_hu, near_hu = ew[16 + v // 2], neighbour(16 + v // 2)
        base = 64 * (v % 2)
        h = spread(own_hu, base)
        p, q = face(
            h, spread(near_hu, base), spread(own_hu, base + 32), spread(near_hu, base + 32), mixing
        )
        div = jnp.where(is_east, q, p) * neighbour(v) - jnp.where(is_east, p, q) * ew[v]
        d_ew[v] = div
        value = (time_step * h) / jnp.maximum(h, depth_floor) * div
        if v % 2 == 0:
            pending = value
        else:
            value = pending + value
            work[v // 2] = jnp.where(is_east, value, pltpu.roll(value, 64, 1))

    low_ends = (lane == 0) | (lane == 63)
    high_ends = (lane == 64) | (lane == 127)

    def add_ends(k, carry):
        for t in range(TR):
            for q in range(4):
                rows = pl.ds(pl.multiple_of(k * 32 + q * 8, 8), 8)
                shift = 127 - 2 * k + (128 - 32 * t)
                low = pltpu.roll(work[2 * q], shift - 64, 1)
                high = pltpu.roll(work[2 * q + 1], shift, 1)
                edge = jnp.where(low_ends, low, jnp.where(high_ends, high, 0.0))
                acc[t, rows, :] = num2[t, rows, :] + edge
        return carry

    lax.fori_loop(0, LV, add_ends, 0)

    source = sub_iota((128, 128))
    target = lane_iota((128, 128))
    pools = [
        jnp.where(target == par * 64 + (source >> 1), 1.0, 0.0).astype(BF16) for par in range(2)
    ]
    quarter = [
        jnp.where(target == j * 32 + ((source & 63) >> 1), 1.0, 0.0).astype(BF16) for j in range(4)
    ]

    back = 127 - lane
    for half in range(2):
        mix = jnp.zeros((8, 128), F32)
        for k in range(8):
            mix = jnp.where(sub == k, diff[8 * half + k], mix)

        def rows_of(ref, n):
            return ref[pl.ds(n * 16 + 8 * half, 8), :]

        def own(n, top):
            pair = (ns_two, ns_one) if top else (ns_one, ns_two)
            return jnp.where(odd, rows_of(pair[0], n), rows_of(pair[1], n))

        def near(n, top, sign=1.0):
            if not top:
                return jnp.where(odd, rows_of(got_one, n), rows_of(got_two, n))
            value = jnp.where(odd, rows_of(got_two, n), rows_of(got_one, n))
            turned = sign * jnp.take_along_axis(value, back, axis=1)
            return jnp.where(at_fold, turned, value)

        for top in (False, True):
            h = own(4, top)
            p, q = face(h, near(4, top), own(5, top), near(5, top, -1.0), mix)
            gain = (time_step * h) / jnp.maximum(h, depth_floor)
            for t in range(TR):
                if top:
                    div = q * near(t, top) - p * own(t, top)
                else:
                    div = p * near(t, top) - q * own(t, top)
                d_ns[int(top), pl.ds(t * 16 + 8 * half, 8), :] = div
                at = (t, pl.ds(256 * half + 31 * int(top), 8, stride=32), slice(None))
                acc[at] = acc[at] + split_dot(gain * div, pools[int(top)])

    def keep(n, values):
        high, low = halves(values)
        chunks[0:128, pl.ds(n * 128, 128)] = high
        chunks[128:256, pl.ds(n * 128, 128)] = low

    def every_fourth(ref, *lead, j):
        return jnp.concatenate(
            [ref[(*lead, pl.ds(32 * m + j, 8, stride=4), slice(None))] for m in range(16)], axis=0
        )

    gains = []
    den4 = jnp.zeros((128, 128), F32)
    for j in range(4):
        den = every_fourth(den2, j=j)
        gains.append(1.0 / jnp.maximum(den, weight_floor))
        den4 = den4 + split_dot(den, quarter[j])
    gain4 = 1.0 / jnp.maximum(den4, weight_floor)
    for t in range(TR):
        num4 = jnp.zeros((128, 128), F32)
        for j in range(4):
            num = every_fourth(acc, t, j=j)
            keep(t * 4 + j, num * gains[j])
            num4 = num4 + split_dot(num, quarter[j])
        keep(16 + t, num4 * gain4)

    each = CAP * DEV // PARTS
    copies = []
    for part in range(PARTS):
        left = placing[pl.ds(part * each, each), :]
        for n in range(CHUNKS // 2):
            placed = jnp.dot(left, chunks[:, pl.ds(n * 256, 256)], preferred_element_type=F32)
            for c in range(2):
                for m in range(each // 8):
                    start = (part * each + m * 8) * CHUNKS + 2 * n + c
                    send_s[pl.ds(start, 8, stride=CHUNKS), :] = placed[
                        m * 8 : m * 8 + 8, c * 128 : c * 128 + 128
                    ]
        rows = pl.ds(part * each * CHUNKS, each * CHUNKS)
        copies.append(pltpu.make_async_copy(send_s.at[rows], send.at[rows], sems.at[part]))
        copies[-1].start()
    for copy in copies:
        copy.wait()


def kernel_second_call(*args):
    vmem = pl.BlockSpec(memory_space=pltpu.VMEM)
    return pl.pallas_call(
        kernel_second,
        name="second",
        out_shape=(
            pltpu.HBM((DEV * CAP * CHUNKS, 128), F32),
            jax.ShapeDtypeStruct((16, 8, 128), F32),
            jax.ShapeDtypeStruct((2, 64, 128), F32),
        ),
        in_specs=[vmem] * 9 + [pl.BlockSpec(memory_space=pltpu.SMEM), vmem],
        out_specs=(pl.BlockSpec(memory_space=pltpu.HBM), vmem, vmem),
        scratch_shapes=[
            pltpu.VMEM((8, 8, 128), F32),
            pltpu.VMEM((TR, 512, 128), F32),
            pltpu.VMEM((256, 2560), BF16),
            pltpu.VMEM((DEV * CAP * CHUNKS, 128), F32),
            pltpu.SemaphoreType.DMA((PARTS,)),
        ],
        compiler_params=pltpu.CompilerParams(vmem_limit_bytes=16 * MIB),
        cost_estimate=pl.CostEstimate(flops=60_000_000, bytes_accessed=6 * MIB, transcendentals=0),
    )(*args)


def kernel_third(
    tr, fill, mask, east, north, diff, area, d_ew, d_ns,
    out,
    tr_s, fill_s, mask_s, east_s, north_s, area_s, out_s, moved_s, sems, area_sem, out_sems,
):
    hbm, vmem = (tr, fill, mask, east, north), (tr_s, fill_s, mask_s, east_s, north_s)
    copies = input_copies(hbm, vmem, sems)
    area_copy = pltpu.make_async_copy(area, area_s, area_sem)
    for group in range(GROUPS):
        for copy in copies(group):
            copy.start()
        if group == 0:
            area_copy.start()
    area_copy.wait()
    lane, sub = lane_iota(), sub_iota()
    ends = (lane == 0) | (lane == 127)
    not_last, not_top = lane < 127, sub < 7
    per = LV // GROUPS

    def out_copy(group):
        levels = pl.ds(group * per, per)
        return pltpu.make_async_copy(out_s.at[:, levels], out.at[:, levels], out_sems.at[group])

    def level(k):
        mixing = diff[k]

        def load(ref, start):
            return ref[(k, *row_set(start))]

        def depth(start):
            return load(fill_s, start) * load(mask_s, start).astype(F32)

        for v in range(16):
            edge = d_ew[v]
            for t in range(TR):
                moved = pltpu.roll(edge, 127 - 2 * k + (128 - 32 * t), 1)
                moved_s[v, t] = jnp.where(ends, moved, 0.0)

        before = [jnp.zeros((8, 128), F32)] * TR
        for q in range(4):
            hs = [depth(32 * q + j) for j in range(4)]
            vs = [load(north_s, 32 * q + j) for j in range(4)]
            if q < 3:
                hs.append(depth(32 * q + 4))
                vs.append(load(north_s, 32 * q + 4))
            else:
                hs.append(pltpu.roll(hs[0], 7, 0))
                vs.append(pltpu.roll(vs[0], 7, 0))
            coefs = []
            for j in range(4):
                top = q == 3 and j == 3
                h, u = hs[j], load(east_s, 32 * q + j)
                rate = time_step / (area_s[row_set(32 * q + j)] * jnp.maximum(h, depth_floor))
                coefs.append(
                    face(h, pltpu.roll(h, 127, 1), u, pltpu.roll(u, 127, 1), mixing, keep=not_last)
                    + face(h, hs[j + 1], vs[j], vs[j + 1], mixing, keep=not_top if top else None)
                    + (rate,)
                )
            for t in range(TR):
                cells = [tr_s[(t, k, *row_set(32 * q + j))] for j in range(4)]
                if q < 3:
                    cells.append(tr_s[(t, k, *row_set(32 * q + 4))])
                else:
                    cells.append(pltpu.roll(cells[0], 7, 0))
                norths = [coefs[j][2] * cells[j] - coefs[j][3] * cells[j + 1] for j in range(4)]
                turned = pltpu.roll(norths[3], 1, 0)
                souths = [jnp.where(sub > 0, turned, before[t])] + norths[:3]
                before[t] = turned
                for j in range(4):
                    p_e, q_e, _, _, rate = coefs[j]
                    cell = cells[j]
                    flux = p_e * cell - q_e * pltpu.roll(cell, 127, 1)
                    div = (pltpu.roll(flux, 1, 1) - flux) + (souths[j] - norths[j])
                    div = div + moved_s[4 * q + j, t]
                    if q == 0 and j == 0:
                        div = div + jnp.where(sub == 0, d_ns[0, pl.ds(t * 16 + k, 1), :], 0.0)
                    if q == 3 and j == 3:
                        div = div + jnp.where(sub == 7, d_ns[1, pl.ds(t * 16 + k, 1), :], 0.0)
                    out_s[(t, k, *row_set(32 * q + j))] = cell + rate * div

    def group_body(group, carry):
        for copy in copies(group):
            copy.wait()
        for n in range(per):
            level(group * per + n)
        out_copy(group).start()
        return carry

    lax.fori_loop(0, GROUPS, group_body, 0)
    for group in range(GROUPS):
        out_copy(group).wait()


def kernel_third_call(tracers, fill, mask, east, north, diff, area, d_ew, d_ns):
    hbm = pl.BlockSpec(memory_space=pltpu.HBM)
    vmem = pl.BlockSpec(memory_space=pltpu.VMEM)
    return pl.pallas_call(
        kernel_third,
        name="third",
        out_shape=jax.ShapeDtypeStruct((TR, LV, ROWS, LANES), F32),
        in_specs=[hbm] * 5 + [pl.BlockSpec(memory_space=pltpu.SMEM), hbm, vmem, vmem],
        out_specs=hbm,
        scratch_shapes=[
            pltpu.VMEM((TR, LV, ROWS, LANES), F32),
            pltpu.VMEM((LV, ROWS, LANES), F32),
            pltpu.VMEM((LV, ROWS, LANES), jnp.int32),
            pltpu.VMEM((LV, ROWS, LANES), F32),
            pltpu.VMEM((LV, ROWS, LANES), F32),
            pltpu.VMEM((ROWS, LANES), F32),
            pltpu.VMEM((TR, LV, ROWS, LANES), F32),
            pltpu.VMEM((16, TR, 8, 128), F32),
            pltpu.SemaphoreType.DMA((5, GROUPS)),
            pltpu.SemaphoreType.DMA,
            pltpu.SemaphoreType.DMA((GROUPS,)),
        ],
        compiler_params=pltpu.CompilerParams(vmem_limit_bytes=24 * MIB),
        cost_estimate=pl.CostEstimate(flops=60_000_000, bytes_accessed=12 * MIB, transcendentals=0),
    )(tracers, fill, mask, east, north, diff, area, d_ew, d_ns)


SPLITS = 4


def kernel_last(got, two, four):
    for m in range(32 // SPLITS):
        for n in range(CHUNKS):
            value = got[pl.ds(m * 8 * CHUNKS + n, 8, stride=CHUNKS), :]
            if n < 16:
                two[pl.ds(m * 8, 8), pl.ds(n * 128, 128)] = value
            else:
                four[pl.ds(m * 8, 8), pl.ds((n - 16) * 128, 128)] = value


def kernel_last_call(got):
    return pl.pallas_call(
        kernel_last,
        name="last",
        grid=(SPLITS,),
        out_shape=(
            jax.ShapeDtypeStruct((DEV * CAP, 2048), F32),
            jax.ShapeDtypeStruct((DEV * CAP, 512), F32),
        ),
        in_specs=[pl.BlockSpec((DEV * 40 // SPLITS, 128), lambda s: (s, 0))],
        out_specs=(
            pl.BlockSpec((DEV * CAP // SPLITS, 2048), lambda s: (s, 0)),
            pl.BlockSpec((DEV * CAP // SPLITS, 512), lambda s: (s, 0)),
        ),
        compiler_params=pltpu.CompilerParams(vmem_limit_bytes=8 * MIB),
    )(got)


def local(
    tracers, fill_fraction, ocean_mask, east_speed, north_speed, diffusivity, cell_area, owner_map
):
    lon_count = lax.axis_size("lon")
    lat_count = lax.axis_size("lat")
    *in_hbm, diffusivity, area_hbm = (
        pltpu.with_memory_space_constraint(x, pltpu.HBM)
        for x in (
            tracers, fill_fraction, ocean_mask, east_speed, north_speed, diffusivity, cell_area
        )
    )
    ns_one, ns_two = kernel_rows_call(in_hbm[0], in_hbm[1], in_hbm[2], in_hbm[4])
    both = ("lon", "lat")

    def swapped(pairs):
        return [pair for a, b in pairs for pair in ((a, b), (b, a))]

    def at(lon, lat):
        return lon * lat_count + lat

    lons = range(lon_count)
    step_one = [(at(n, a), at(n, a + 1)) for n in lons for a in range(0, lat_count, 2)]
    step_two = [(at(n, a), at(n, a + 1)) for n in lons for a in range(1, lat_count - 1, 2)]
    fold = [
        (at(n, lat_count - 1), at(lon_count - 1 - n, lat_count - 1)) for n in range(lon_count // 2)
    ]
    got_one = lax.ppermute(ns_one, both, swapped(step_one))
    got_two = lax.ppermute(ns_two, both, swapped(step_two + fold))
    h_v, ew, placing = kernel_edges_call(
        tracers, fill_fraction, ocean_mask, east_speed, owner_map.reshape(1, DEV)
    )
    ew_one = lax.ppermute(ew, "lon", swapped([(n, n + 1) for n in range(0, lon_count, 2)]))
    ew_two = lax.ppermute(
        ew, "lon", swapped([(n, (n + 1) % lon_count) for n in range(1, lon_count, 2)])
    )
    num2, den2 = kernel_first_call(tracers, h_v, east_speed, north_speed, cell_area, diffusivity)
    send, d_ew, d_ns = kernel_second_call(
        num2, den2, ew, ew_one, ew_two, ns_one, ns_two, got_one, got_two, diffusivity, placing
    )
    got = lax.all_to_all(
        send.reshape(DEV, CAP * CHUNKS, 128), both, split_axis=0, concat_axis=0, tiled=True
    )
    updated = kernel_third_call(*in_hbm, diffusivity, area_hbm, d_ew, d_ns)
    two, four = kernel_last_call(got.reshape(DEV * CAP * CHUNKS, 128))
    return (updated, two[None], four[None])


def solution(mesh):
    in_specs = (
        P(None, None, "lat", "lon"),
        P(None, "lat", "lon"),
        P(None, "lat", "lon"),
        P(None, "lat", "lon"),
        P(None, "lat", "lon"),
        P(),
        P("lat", "lon"),
        P(("lon", "lat"), None),
    )
    out_specs = (
        P(None, None, "lat", "lon"),
        P(("lon", "lat"), None, None),
        P(("lon", "lat"), None, None),
    )
    return jax.shard_map(
        local,
        mesh=mesh, in_specs=in_specs, out_specs=out_specs, check_vma=False,
    )
```

```python
import jax
import jax.numpy as jnp
from jax import lax
from jax.experimental import pallas as pl
from jax.experimental.pallas import tpu as pltpu
from jax.sharding import PartitionSpec as P


time_step = 0.05
depth_floor = 0.25
weight_floor = 0.25

TR, LV = 4, 16
ROWS, LANES = 128, 128
GROUPS = 16
DEV, CAP = 128, 2
CHUNKS = 20
PARTS = 2
EACH = 16
F32, BF16 = jnp.float32, jnp.bfloat16
MIB = 1 << 20


def lane_iota(shape=(8, 128)):
    return lax.broadcasted_iota(jnp.int32, shape, len(shape) - 1)


def sub_iota(shape=(8, 128)):
    return lax.broadcasted_iota(jnp.int32, shape, len(shape) - 2)


def face(lower_h, upper_h, lower_speed, upper_speed, mixing, keep=None):
    open_depth = jnp.minimum(lower_h, upper_h)
    if keep is not None:
        open_depth = jnp.where(keep, open_depth, 0.0)
    speed = 0.5 * (lower_speed + upper_speed)
    ahead = jnp.maximum(speed, 0.0)
    back = ahead - speed
    return open_depth * (ahead + mixing), open_depth * (back + mixing)


def halves(values):
    high = values.astype(BF16)
    return high, (values - high.astype(F32)).astype(BF16)


def split_dot(left, right):
    high, low = halves(left)
    return jnp.dot(high, right, preferred_element_type=F32) + jnp.dot(
        low, right, preferred_element_type=F32
    )


def input_copies(hbm, vmem, sems):
    per = LV // GROUPS

    def copies(group):
        levels = pl.ds(group * per, per)
        out = [pltpu.make_async_copy(hbm[0].at[:, levels], vmem[0].at[:, levels], sems.at[0, group])]
        for n in range(1, 5):
            out.append(
                pltpu.make_async_copy(hbm[n].at[levels], vmem[n].at[levels], sems.at[n, group])
            )
        return out

    return copies


def row_set(start):
    return (pl.ds(start, 8, stride=4), slice(None))


def kernel_rows(tr, fill, mask, north, ns_one, ns_two, tr_s, fill_s, mask_s, north_s, sems):
    copies = []
    for n, (src, dst) in enumerate(((tr, tr_s), (fill, fill_s), (mask, mask_s), (north, north_s))):
        for side in range(2):
            rows = pl.ds(side * (ROWS - 8), 8)
            if n == 0:
                copies.append(
                    pltpu.make_async_copy(src.at[:, :, rows], dst.at[side], sems.at[n, side])
                )
            else:
                copies.append(
                    pltpu.make_async_copy(src.at[:, rows], dst.at[side], sems.at[n, side])
                )
            copies[-1].start()
    for copy in copies:
        copy.wait()
    odd = lax.axis_index("lat") % 2 == 1
    for n in range(6):
        for half in range(2):
            levels = range(8 * half, 8 * half + 8)
            lines = []
            for side in range(2):
                row = 7 * side
                pick = lambda ref, k: ref[side, k, pl.ds(row, 1), :]
                if n < TR:
                    parts = [tr_s[side, n, k, pl.ds(row, 1), :] for k in levels]
                elif n == TR:
                    parts = [pick(fill_s, k) * pick(mask_s, k).astype(F32) for k in levels]
                else:
                    parts = [pick(north_s, k) for k in levels]
                lines.append(jnp.concatenate(parts, axis=0))
            at = pl.ds(n * 16 + 8 * half, 8)
            ns_one[at, :] = jnp.where(odd, lines[0], lines[1])
            ns_two[at, :] = jnp.where(odd, lines[1], lines[0])


def kernel_rows_call(tracers, fill, mask, north):
    hbm = pl.BlockSpec(memory_space=pltpu.HBM)
    vmem = pl.BlockSpec(memory_space=pltpu.VMEM)
    return pl.pallas_call(
        kernel_rows,
        name="rows",
        out_shape=(jax.ShapeDtypeStruct((96, 128), F32),) * 2,
        in_specs=[hbm] * 4,
        out_specs=(vmem,) * 2,
        scratch_shapes=[
            pltpu.VMEM((2, TR, LV, 8, LANES), F32),
            pltpu.VMEM((2, LV, 8, LANES), F32),
            pltpu.VMEM((2, LV, 8, LANES), jnp.int32),
            pltpu.VMEM((2, LV, 8, LANES), F32),
            pltpu.SemaphoreType.DMA((4, 2)),
        ],
        compiler_params=pltpu.CompilerParams(vmem_limit_bytes=4 * MIB),
        cost_estimate=pl.CostEstimate(flops=1_000_000, bytes_accessed=MIB, transcendentals=0),
    )(tracers, fill, mask, north)


def kernel_edges(tr_v, fill_v, mask_v, east_v, owner, h_v, ew, placing):
    across = lane_iota((DEV, DEV))
    down = sub_iota((DEV, DEV))
    who_row = owner[...]
    who = jnp.sum(jnp.where(down == across, who_row, 0), axis=1, keepdims=True)
    same = jnp.where((who == who_row) & (down < across), 1, 0)
    rank = jnp.sum(same, axis=0, keepdims=True)
    row_of = who_row * CAP + rank
    for part in range(CAP):
        here = jnp.where(down + part * DEV == row_of, 1.0, 0.0).astype(BF16)
        placing[pl.ds(part * DEV, DEV), 0:DEV] = here
        placing[pl.ds(part * DEV, DEV), DEV : 2 * DEV] = here

    lane = lane_iota()

    def level(k, carry):
        where_t = [(lane >> 1) == t * 16 + k for t in range(TR)]
        for v in range(16):
            at = row_set(32 * (v // 4) + v % 4)
            h = fill_v[(k, *at)] * mask_v[(k, *at)].astype(F32)
            h_v[k, v] = h
            base = 64 * (v % 2)
            packed = ew[16 + v // 2]
            packed = jnp.where(
                (lane >> 1) == k + base // 2, pltpu.roll(h, 2 * k + 1 + base, 1), packed
            )
            ew[16 + v // 2] = jnp.where(
                (lane >> 1) == k + 16 + base // 2,
                pltpu.roll(east_v[(k, *at)], 2 * k + 33 + base, 1),
                packed,
            )
            packed = ew[v]
            for t in range(TR):
                moved = pltpu.roll(tr_v[(t, k, *at)], 2 * k + 32 * t + 1, 1)
                packed = jnp.where(where_t[t], moved, packed)
            ew[v] = packed
        return carry

    lax.fori_loop(0, LV, level, 0)


def kernel_edges_call(tracers, fill, mask, east, owner):
    vmem = pl.BlockSpec(memory_space=pltpu.VMEM)
    return pl.pallas_call(
        kernel_edges,
        name="edges",
        out_shape=(
            jax.ShapeDtypeStruct((LV, 16, 8, LANES), F32),
            jax.ShapeDtypeStruct((24, 8, 128), F32),
            jax.ShapeDtypeStruct((CAP * DEV, 2 * DEV), BF16),
        ),
        in_specs=[vmem] * 5,
        out_specs=(vmem,) * 3,
        compiler_params=pltpu.CompilerParams(vmem_limit_bytes=16 * MIB),
        cost_estimate=pl.CostEstimate(flops=60_000_000, bytes_accessed=11 * MIB, transcendentals=0),
    )(tracers, fill, mask, east, owner)


def kernel_first(
    tr_s, h_v, east_s, north_s, area_s, diff,
    num2, den2,
    g_s, face_s, coef, store, cross,
):
    source = sub_iota((256, 128))
    target = lane_iota((256, 128))
    pool = jnp.where(target == (source >> 7) * 64 + ((source & 127) >> 1), 1.0, 0.0).astype(BF16)
    beside = (source >> 7) * 64 + (((source & 127) + 1) >> 1) - jnp.where((source & 1) == 0, 1, 0)
    inside = ((source & 127) != 0) & ((source & 127) != 127)
    pool_cross = jnp.where((target == beside) & inside, 1.0, 0.0).astype(BF16)
    lane, sub = lane_iota(), sub_iota()
    is_even = (lane & 1) == 0
    not_last = lane < 127
    not_top = sub < 7

    def level(k):
        mixing = diff[k]

        def load(ref, start):
            return ref[(k, *row_set(start))]

        for v in range(16):
            start = 32 * (v // 4) + v % 4
            h, u = h_v[k, v], load(east_s, start)
            p_e, q_e = face(
                h, pltpu.roll(h, 127, 1), u, pltpu.roll(u, 127, 1), mixing, keep=not_last
            )
            g_s[v] = (time_step * h) / jnp.maximum(h, depth_floor)
            face_s[0, v] = p_e
            face_s[1, v] = q_e

        for v in range(16):
            q, j = v // 4, v % 4
            start = 32 * q + j
            h, speed = h_v[k, v], load(north_s, start)
            if j < 3:
                p_n, q_n = face(h, h_v[k, v + 1], speed, load(north_s, start + 1), mixing)
            elif q < 3:
                h_up = jnp.where(
                    sub < 7, pltpu.roll(h_v[k, v - 3], 7, 0), pltpu.roll(h_v[k, v + 1], 7, 0)
                )
                p_n, q_n = face(h, h_up, speed, load(north_s, start + 1), mixing)
            else:
                h_up, speed_up = pltpu.roll(h_v[k, 12], 7, 0), pltpu.roll(load(north_s, 96), 7, 0)
                p_n, q_n = face(h, h_up, speed, speed_up, mixing, keep=not_top)
            face_s[2, v] = p_n
            face_s[3, v] = q_n

        for q in range(4):
            south = []
            for n in (2, 3):
                low = pltpu.roll(face_s[n, 4 * q + 3], 1, 0)
                under = pltpu.roll(face_s[n, 4 * q - 1], 1, 0) if q else 0.0
                south.append(jnp.where(sub > 0, low, under))
            for par in range(2):
                centre, weight = [], 0.0
                for n in range(2):
                    v = 4 * q + 2 * par + n
                    h, g = h_v[k, v], g_s[v]
                    w = area_s[row_set(32 * q + 2 * par + n)] * h
                    p_e, q_w = face_s[0, v], pltpu.roll(face_s[1, v], 1, 1)
                    p_n, q_n = face_s[2, v], face_s[3, v]
                    p_s, q_s = south if v % 4 == 0 else (face_s[2, v - 1], face_s[3, v - 1])
                    to_west = pltpu.roll(g, 1, 1) * q_w
                    to_east = pltpu.roll(g, 127, 1) * p_e
                    own = w - g * ((p_e + q_w) + (p_n + q_s))
                    centre.append(own + jnp.where(is_even, to_east, to_west))
                    coef[4 + n, 2 * q + par] = jnp.where(is_even, to_west, to_east)
                    if n == 0:
                        low, up = g * p_s, g * q_n
                    else:
                        down, high = g * p_s, g * q_n
                    weight = weight + w
                coef[0, 2 * q + par] = low
                coef[1, 2 * q + par] = centre[0] + down
                coef[2, 2 * q + par] = centre[1] + up
                coef[3, 2 * q + par] = high
                store[pl.ds(128 + q * 8, 8), pl.ds(par * 128, 128)] = weight

        for q in range(4):
            for par in range(2):
                low_c, a_c, b_c, high_c, a_x, b_x = [coef[n, 2 * q + par] for n in range(6)]
                for t in range(TR):
                    cell = lambda start: tr_s[(t, k, *row_set(start))]
                    start = 32 * q + 2 * par
                    a, b = cell(start), cell(start + 1)
                    low = cell(start - 1) if start else pltpu.roll(cell(3), 1, 0)
                    high = cell(start + 2) if start < 98 else pltpu.roll(cell(96), 7, 0)
                    side = a_x * a + b_x * b
                    value = (a_c * a + b_c * b) + (low_c * low + high_c * high)
                    cross[pl.ds(t * 32 + q * 8, 8), pl.ds(par * 128, 128)] = side
                    store[pl.ds(t * 32 + q * 8, 8), pl.ds(par * 128, 128)] = value

    def pooled(k):
        values = split_dot(store[...], pool)
        sides = split_dot(cross[...], pool_cross)
        rows = pl.ds(pl.multiple_of(k * 32, 32), 32)
        for t in range(TR):
            part = slice(t * 32, t * 32 + 32)
            num2[t, rows, :] = values[part] + sides[part]
        den2[rows, :] = values[128:160]

    def group_body(k, carry):
        pooled((k + LV - 1) % LV)
        level(k)
        return carry

    store[...] = jnp.zeros_like(store)
    cross[...] = jnp.zeros_like(cross)
    lax.fori_loop(0, LV, group_body, 0)
    pooled(LV - 1)


def kernel_first_call(tr_v, h_v, east_v, north_v, area_v, diff):
    vmem = pl.BlockSpec(memory_space=pltpu.VMEM)
    return pl.pallas_call(
        kernel_first,
        name="first",
        out_shape=(
            jax.ShapeDtypeStruct((TR, 512, 128), F32),
            jax.ShapeDtypeStruct((512, 128), F32),
        ),
        in_specs=[vmem] * 5 + [pl.BlockSpec(memory_space=pltpu.SMEM)],
        out_specs=(vmem,) * 2,
        scratch_shapes=[
            pltpu.VMEM((16, 8, 128), F32),
            pltpu.VMEM((4, 16, 8, 128), F32),
            pltpu.VMEM((6, 8, 8, 128), F32),
            pltpu.VMEM((160, 256), F32),
            pltpu.VMEM((128, 256), F32),
        ],
        compiler_params=pltpu.CompilerParams(vmem_limit_bytes=16 * MIB),
        cost_estimate=pl.CostEstimate(flops=60_000_000, bytes_accessed=11 * MIB, transcendentals=0),
    )(tr_v, h_v, east_v, north_v, area_v, diff)


def spread(values, offset):
    index = (lane_iota() & 31) + offset
    return jnp.take_along_axis(values, index, axis=1)


def kernel_second(
    num2, den2, ew, ew_one, ew_two, ns_one, ns_two, got_one, got_two, diff, placing,
    send, d_ew, d_ns,
    work, acc, chunks, send_s, sems,
):
    lane, sub = lane_iota(), sub_iota()
    odd = lax.axis_index("lat") % 2 == 1
    odd_lon = lax.axis_index("lon") % 2 == 1
    at_fold = lax.axis_index("lat") == lax.axis_size("lat") - 1
    is_east = (lane & 1) == 0
    level_of = (lane >> 1) & 15
    mixing = jnp.zeros((8, 128), F32)
    for k in range(LV):
        mixing = jnp.where(level_of == k, diff[k], mixing)

    def neighbour(n):
        one, two = ew_one[n], ew_two[n]
        from_east, from_west = jnp.where(odd_lon, two, one), jnp.where(odd_lon, one, two)
        return jnp.where(is_east, pltpu.roll(from_east, 127, 1), pltpu.roll(from_west, 1, 1))

    pending = None
    for v in range(16):
        own_hu, near_hu = ew[16 + v // 2], neighbour(16 + v // 2)
        base = 64 * (v % 2)
        h = spread(own_hu, base)
        p, q = face(
            h, spread(near_hu, base), spread(own_hu, base + 32), spread(near_hu, base + 32), mixing
        )
        div = jnp.where(is_east, q, p) * neighbour(v) - jnp.where(is_east, p, q) * ew[v]
        d_ew[v] = div
        value = (time_step * h) / jnp.maximum(h, depth_floor) * div
        if v % 2 == 0:
            pending = value
        else:
            value = pending + value
            far_value = pltpu.roll(value, 64, 1)
            q, par = v // 4, (v // 2) % 2
            plain = jnp.where(is_east, value, far_value)
            moved = jnp.where(is_east, far_value, value)
            if par == 0:
                lower = plain, moved
            else:
                for half in range(2):
                    first_lanes = (lane < 64) == is_east
                    mine = first_lanes if half == 0 else ~first_lanes
                    work[half, q] = jnp.where(mine, lower[0], moved)

    ends = ((lane & 63) == 0) | ((lane & 63) == 63)

    def add_ends(step, carry):
        for n in range(EACH):
            k = step * EACH + n
            for t in range(TR):
                for q in range(4):
                    rows = pl.ds(pl.multiple_of(k * 32 + q * 8, 8), 8)
                    moved = pltpu.roll(work[t // 2, q], 63 - 2 * k + (128 - 32 * t), 1)
                    acc[t, rows, :] = num2[t, rows, :] + jnp.where(ends, moved, 0.0)
        return carry

    lax.fori_loop(0, LV // EACH, add_ends, 0)

    source = sub_iota((128, 128))
    target = lane_iota((128, 128))
    pools = [
        jnp.where(target == par * 64 + (source >> 1), 1.0, 0.0).astype(BF16) for par in range(2)
    ]
    quarter = [
        jnp.where(target == j * 32 + ((source & 63) >> 1), 1.0, 0.0).astype(BF16) for j in range(4)
    ]

    back = 127 - lane
    for half in range(2):
        mix = jnp.zeros((8, 128), F32)
        for k in range(8):
            mix = jnp.where(sub == k, diff[8 * half + k], mix)

        def rows_of(ref, n):
            return ref[pl.ds(n * 16 + 8 * half, 8), :]

        def own(n, top):
            pair = (ns_two, ns_one) if top else (ns_one, ns_two)
            return jnp.where(odd, rows_of(pair[0], n), rows_of(pair[1], n))

        def near(n, top, sign=1.0):
            if not top:
                return jnp.where(odd, rows_of(got_one, n), rows_of(got_two, n))
            value = jnp.where(odd, rows_of(got_two, n), rows_of(got_one, n))
            turned = sign * jnp.take_along_axis(value, back, axis=1)
            return jnp.where(at_fold, turned, value)

        for top in (False, True):
            h = own(4, top)
            p, q = face(h, near(4, top), own(5, top), near(5, top, -1.0), mix)
            gain = (time_step * h) / jnp.maximum(h, depth_floor)
            for t in range(TR):
                if top:
                    div = q * near(t, top) - p * own(t, top)
                else:
                    div = p * near(t, top) - q * own(t, top)
                d_ns[int(top), pl.ds(t * 16 + 8 * half, 8), :] = div
                at = (t, pl.ds(256 * half + 31 * int(top), 8, stride=32), slice(None))
                acc[at] = acc[at] + split_dot(gain * div, pools[int(top)])

    def keep(n, values):
        high, low = halves(values)
        chunks[0:128, pl.ds(n * 128, 128)] = high
        chunks[128:256, pl.ds(n * 128, 128)] = low

    def every_fourth(ref, *lead, j):
        return jnp.concatenate(
            [ref[(*lead, pl.ds(32 * m + j, 8, stride=4), slice(None))] for m in range(16)], axis=0
        )

    gains = []
    den4 = jnp.zeros((128, 128), F32)
    for j in range(4):
        den = every_fourth(den2, j=j)
        gains.append(1.0 / jnp.maximum(den, weight_floor))
        den4 = den4 + split_dot(den, quarter[j])
    gain4 = 1.0 / jnp.maximum(den4, weight_floor)
    for t in range(TR):
        num4 = jnp.zeros((128, 128), F32)
        for j in range(4):
            num = every_fourth(acc, t, j=j)
            keep(t * 4 + j, num * gains[j])
            num4 = num4 + split_dot(num, quarter[j])
        keep(16 + t, num4 * gain4)

    each = CAP * DEV // PARTS
    copies = []
    for part in range(PARTS):
        left = placing[pl.ds(part * each, each), :]
        for n in range(CHUNKS // 2):
            placed = jnp.dot(left, chunks[:, pl.ds(n * 256, 256)], preferred_element_type=F32)
            for c in range(2):
                for m in range(each // 8):
                    start = (part * each + m * 8) * CHUNKS + 2 * n + c
                    send_s[pl.ds(start, 8, stride=CHUNKS), :] = placed[
                        m * 8 : m * 8 + 8, c * 128 : c * 128 + 128
                    ]
        rows = pl.ds(part * each * CHUNKS, each * CHUNKS)
        copies.append(pltpu.make_async_copy(send_s.at[rows], send.at[rows], sems.at[part]))
        copies[-1].start()
    for copy in copies:
        copy.wait()


def kernel_second_call(*args):
    vmem = pl.BlockSpec(memory_space=pltpu.VMEM)
    return pl.pallas_call(
        kernel_second,
        name="second",
        out_shape=(
            pltpu.HBM((DEV * CAP * CHUNKS, 128), F32),
            jax.ShapeDtypeStruct((16, 8, 128), F32),
            jax.ShapeDtypeStruct((2, 64, 128), F32),
        ),
        in_specs=[vmem] * 9 + [pl.BlockSpec(memory_space=pltpu.SMEM), vmem],
        out_specs=(pl.BlockSpec(memory_space=pltpu.HBM), vmem, vmem),
        scratch_shapes=[
            pltpu.VMEM((2, 4, 8, 128), F32),
            pltpu.VMEM((TR, 512, 128), F32),
            pltpu.VMEM((256, 2560), BF16),
            pltpu.VMEM((DEV * CAP * CHUNKS, 128), F32),
            pltpu.SemaphoreType.DMA((PARTS,)),
        ],
        compiler_params=pltpu.CompilerParams(vmem_limit_bytes=16 * MIB),
        cost_estimate=pl.CostEstimate(flops=60_000_000, bytes_accessed=6 * MIB, transcendentals=0),
    )(*args)


def kernel_third(
    tr, fill, mask, east, north, diff, area, d_ew, d_ns,
    out,
    tr_s, fill_s, mask_s, east_s, north_s, area_s, out_s, moved_s, sems, area_sem, out_sems,
):
    hbm, vmem = (tr, fill, mask, east, north), (tr_s, fill_s, mask_s, east_s, north_s)
    copies = input_copies(hbm, vmem, sems)
    area_copy = pltpu.make_async_copy(area, area_s, area_sem)
    for group in range(GROUPS):
        for copy in copies(group):
            copy.start()
        if group == 0:
            area_copy.start()
    area_copy.wait()
    lane, sub = lane_iota(), sub_iota()
    ends = (lane == 0) | (lane == 127)
    not_last, not_top = lane < 127, sub < 7
    per = LV // GROUPS

    def out_copy(group):
        levels = pl.ds(group * per, per)
        return pltpu.make_async_copy(out_s.at[:, levels], out.at[:, levels], out_sems.at[group])

    def level(k):
        mixing = diff[k]

        def load(ref, start):
            return ref[(k, *row_set(start))]

        def depth(start):
            return load(fill_s, start) * load(mask_s, start).astype(F32)

        for v in range(16):
            edge = d_ew[v]
            for t in range(TR):
                moved = pltpu.roll(edge, 127 - 2 * k + (128 - 32 * t), 1)
                moved_s[v, t] = jnp.where(ends, moved, 0.0)

        before = [jnp.zeros((8, 128), F32)] * TR
        for q in range(4):
            hs = [depth(32 * q + j) for j in range(4)]
            vs = [load(north_s, 32 * q + j) for j in range(4)]
            if q < 3:
                hs.append(depth(32 * q + 4))
                vs.append(load(north_s, 32 * q + 4))
            else:
                hs.append(pltpu.roll(hs[0], 7, 0))
                vs.append(pltpu.roll(vs[0], 7, 0))
            coefs = []
            for j in range(4):
                top = q == 3 and j == 3
                h, u = hs[j], load(east_s, 32 * q + j)
                rate = time_step / (area_s[row_set(32 * q + j)] * jnp.maximum(h, depth_floor))
                coefs.append(
                    face(h, pltpu.roll(h, 127, 1), u, pltpu.roll(u, 127, 1), mixing, keep=not_last)
                    + face(h, hs[j + 1], vs[j], vs[j + 1], mixing, keep=not_top if top else None)
                    + (rate,)
                )
            for t in range(TR):
                cells = [tr_s[(t, k, *row_set(32 * q + j))] for j in range(4)]
                if q < 3:
                    cells.append(tr_s[(t, k, *row_set(32 * q + 4))])
                else:
                    cells.append(pltpu.roll(cells[0], 7, 0))
                norths = [coefs[j][2] * cells[j] - coefs[j][3] * cells[j + 1] for j in range(4)]
                turned = pltpu.roll(norths[3], 1, 0)
                souths = [jnp.where(sub > 0, turned, before[t])] + norths[:3]
                before[t] = turned
                for j in range(4):
                    p_e, q_e, _, _, rate = coefs[j]
                    cell = cells[j]
                    flux = p_e * cell - q_e * pltpu.roll(cell, 127, 1)
                    div = (pltpu.roll(flux, 1, 1) - flux) + (souths[j] - norths[j])
                    div = div + moved_s[4 * q + j, t]
                    if q == 0 and j == 0:
                        div = div + jnp.where(sub == 0, d_ns[0, pl.ds(t * 16 + k, 1), :], 0.0)
                    if q == 3 and j == 3:
                        div = div + jnp.where(sub == 7, d_ns[1, pl.ds(t * 16 + k, 1), :], 0.0)
                    out_s[(t, k, *row_set(32 * q + j))] = cell + rate * div

    def group_body(group, carry):
        for copy in copies(group):
            copy.wait()
        for n in range(per):
            level(group * per + n)
        out_copy(group).start()
        return carry

    lax.fori_loop(0, GROUPS, group_body, 0)
    for group in range(GROUPS):
        out_copy(group).wait()


def kernel_third_call(tracers, fill, mask, east, north, diff, area, d_ew, d_ns):
    hbm = pl.BlockSpec(memory_space=pltpu.HBM)
    vmem = pl.BlockSpec(memory_space=pltpu.VMEM)
    return pl.pallas_call(
        kernel_third,
        name="third",
        out_shape=jax.ShapeDtypeStruct((TR, LV, ROWS, LANES), F32),
        in_specs=[hbm] * 5 + [pl.BlockSpec(memory_space=pltpu.SMEM), hbm, vmem, vmem],
        out_specs=hbm,
        scratch_shapes=[
            pltpu.VMEM((TR, LV, ROWS, LANES), F32),
            pltpu.VMEM((LV, ROWS, LANES), F32),
            pltpu.VMEM((LV, ROWS, LANES), jnp.int32),
            pltpu.VMEM((LV, ROWS, LANES), F32),
            pltpu.VMEM((LV, ROWS, LANES), F32),
            pltpu.VMEM((ROWS, LANES), F32),
            pltpu.VMEM((TR, LV, ROWS, LANES), F32),
            pltpu.VMEM((16, TR, 8, 128), F32),
            pltpu.SemaphoreType.DMA((5, GROUPS)),
            pltpu.SemaphoreType.DMA,
            pltpu.SemaphoreType.DMA((GROUPS,)),
        ],
        compiler_params=pltpu.CompilerParams(vmem_limit_bytes=24 * MIB),
        cost_estimate=pl.CostEstimate(flops=60_000_000, bytes_accessed=12 * MIB, transcendentals=0),
    )(tracers, fill, mask, east, north, diff, area, d_ew, d_ns)


SPLITS = 4


def kernel_last(got, two, four):
    for m in range(32 // SPLITS):
        for n in range(CHUNKS):
            value = got[pl.ds(m * 8 * CHUNKS + n, 8, stride=CHUNKS), :]
            if n < 16:
                two[pl.ds(m * 8, 8), pl.ds(n * 128, 128)] = value
            else:
                four[pl.ds(m * 8, 8), pl.ds((n - 16) * 128, 128)] = value


def kernel_last_call(got):
    return pl.pallas_call(
        kernel_last,
        name="last",
        grid=(SPLITS,),
        out_shape=(
            jax.ShapeDtypeStruct((DEV * CAP, 2048), F32),
            jax.ShapeDtypeStruct((DEV * CAP, 512), F32),
        ),
        in_specs=[pl.BlockSpec((DEV * 40 // SPLITS, 128), lambda s: (s, 0))],
        out_specs=(
            pl.BlockSpec((DEV * CAP // SPLITS, 2048), lambda s: (s, 0)),
            pl.BlockSpec((DEV * CAP // SPLITS, 512), lambda s: (s, 0)),
        ),
        compiler_params=pltpu.CompilerParams(vmem_limit_bytes=8 * MIB),
    )(got)


def local(
    tracers, fill_fraction, ocean_mask, east_speed, north_speed, diffusivity, cell_area, owner_map
):
    lon_count = lax.axis_size("lon")
    lat_count = lax.axis_size("lat")
    *in_hbm, diffusivity, area_hbm = (
        pltpu.with_memory_space_constraint(x, pltpu.HBM)
        for x in (
            tracers, fill_fraction, ocean_mask, east_speed, north_speed, diffusivity, cell_area
        )
    )
    ns_one, ns_two = kernel_rows_call(in_hbm[0], in_hbm[1], in_hbm[2], in_hbm[4])
    both = ("lon", "lat")

    def swapped(pairs):
        return [pair for a, b in pairs for pair in ((a, b), (b, a))]

    def at(lon, lat):
        return lon * lat_count + lat

    lons = range(lon_count)
    step_one = [(at(n, a), at(n, a + 1)) for n in lons for a in range(0, lat_count, 2)]
    step_two = [(at(n, a), at(n, a + 1)) for n in lons for a in range(1, lat_count - 1, 2)]
    fold = [
        (at(n, lat_count - 1), at(lon_count - 1 - n, lat_count - 1)) for n in range(lon_count // 2)
    ]
    got_one = lax.ppermute(ns_one, both, swapped(step_one))
    got_two = lax.ppermute(ns_two, both, swapped(step_two + fold))
    h_v, ew, placing = kernel_edges_call(
        tracers, fill_fraction, ocean_mask, east_speed, owner_map.reshape(1, DEV)
    )
    ew_one = lax.ppermute(ew, "lon", swapped([(n, n + 1) for n in range(0, lon_count, 2)]))
    ew_two = lax.ppermute(
        ew, "lon", swapped([(n, (n + 1) % lon_count) for n in range(1, lon_count, 2)])
    )
    num2, den2 = kernel_first_call(tracers, h_v, east_speed, north_speed, cell_area, diffusivity)
    send, d_ew, d_ns = kernel_second_call(
        num2, den2, ew, ew_one, ew_two, ns_one, ns_two, got_one, got_two, diffusivity, placing
    )
    got = lax.all_to_all(
        send.reshape(DEV, CAP * CHUNKS, 128), both, split_axis=0, concat_axis=0, tiled=True
    )
    updated = kernel_third_call(*in_hbm, diffusivity, area_hbm, d_ew, d_ns)
    two, four = kernel_last_call(got.reshape(DEV * CAP * CHUNKS, 128))
    return (updated, two[None], four[None])


def solution(mesh):
    in_specs = (
        P(None, None, "lat", "lon"),
        P(None, "lat", "lon"),
        P(None, "lat", "lon"),
        P(None, "lat", "lon"),
        P(None, "lat", "lon"),
        P(),
        P("lat", "lon"),
        P(("lon", "lat"), None),
    )
    out_specs = (
        P(None, None, "lat", "lon"),
        P(("lon", "lat"), None, None),
        P(("lon", "lat"), None, None),
    )
    return jax.shard_map(
        local,
        mesh=mesh, in_specs=in_specs, out_specs=out_specs, check_vma=False,
    )
```

```python
import jax
import jax.numpy as jnp
from jax import lax
from jax.experimental import pallas as pl
from jax.experimental.pallas import tpu as pltpu
from jax.sharding import PartitionSpec as P


time_step = 0.05
depth_floor = 0.25
weight_floor = 0.25

TR, LV = 4, 16
ROWS, LANES = 128, 128
GROUPS = 16
DEV, CAP = 128, 2
CHUNKS = 20
PARTS = 2
EACH = 16
F32, BF16 = jnp.float32, jnp.bfloat16
MIB = 1 << 20


def lane_iota(shape=(8, 128)):
    return lax.broadcasted_iota(jnp.int32, shape, len(shape) - 1)


def sub_iota(shape=(8, 128)):
    return lax.broadcasted_iota(jnp.int32, shape, len(shape) - 2)


def face(lower_h, upper_h, lower_speed, upper_speed, mixing, keep=None):
    open_depth = jnp.minimum(lower_h, upper_h)
    if keep is not None:
        open_depth = jnp.where(keep, open_depth, 0.0)
    speed = 0.5 * (lower_speed + upper_speed)
    ahead = jnp.maximum(speed, 0.0)
    back = ahead - speed
    return open_depth * (ahead + mixing), open_depth * (back + mixing)


def half_face(lower_half, upper_half, lower_speed, upper_speed, twice_mixing, keep=None):
    open_half = jnp.minimum(lower_half, upper_half)
    if keep is not None:
        open_half = jnp.where(keep, open_half, 0.0)
    speeds = lower_speed + upper_speed
    ahead = jnp.maximum(speeds, 0.0)
    back = ahead - speeds
    return open_half * (ahead + twice_mixing), open_half * (back + twice_mixing)


def depth_gain(h):
    return time_step * jnp.minimum(h * (1.0 / depth_floor), 1.0)


def halves(values):
    high = values.astype(BF16)
    return high, (values - high.astype(F32)).astype(BF16)


def split_dot(left, right):
    high, low = halves(left)
    return jnp.dot(high, right, preferred_element_type=F32) + jnp.dot(
        low, right, preferred_element_type=F32
    )


def input_copies(hbm, vmem, sems):
    per = LV // GROUPS

    def copies(group):
        levels = pl.ds(group * per, per)
        out = [pltpu.make_async_copy(hbm[0].at[:, levels], vmem[0].at[:, levels], sems.at[0, group])]
        for n in range(1, 5):
            out.append(
                pltpu.make_async_copy(hbm[n].at[levels], vmem[n].at[levels], sems.at[n, group])
            )
        return out

    return copies


def row_set(start):
    return (pl.ds(start, 8, stride=4), slice(None))


def kernel_rows(
    tr, fill, mask, north, owner,
    ns_one, ns_two, placing, pool,
    tr_s, fill_s, mask_s, north_s, owner_s, sems, owner_sem,
):
    copies = []
    for n, (src, dst) in enumerate(((tr, tr_s), (fill, fill_s), (mask, mask_s), (north, north_s))):
        for side in range(2):
            rows = pl.ds(side * (ROWS - 8), 8)
            if n == 0:
                copies.append(
                    pltpu.make_async_copy(src.at[:, :, rows], dst.at[side], sems.at[n, side])
                )
            else:
                copies.append(
                    pltpu.make_async_copy(src.at[:, rows], dst.at[side], sems.at[n, side])
                )
            copies[-1].start()
    owner_copy = pltpu.make_async_copy(owner, owner_s, owner_sem)
    owner_copy.start()
    source = sub_iota((256, 128))
    match = lane_iota((256, 128)) == (source >> 7) * 64 + ((source & 127) >> 1)
    for term in range(2):
        pool[pl.ds(256 * term, 256), :] = jnp.where(match, 1.0, 0.0).astype(BF16)
    across = lane_iota((DEV, DEV))
    down = sub_iota((DEV, DEV))
    owner_copy.wait()
    who_row = owner_s[...]
    who = jnp.sum(jnp.where(down == across, who_row, 0), axis=1, keepdims=True)
    same = jnp.where((who == who_row) & (down < across), 1, 0)
    rank = jnp.sum(same, axis=0, keepdims=True)
    row_of = who_row * CAP + rank
    for part in range(CAP):
        here = jnp.where(down + part * DEV == row_of, 1.0, 0.0).astype(BF16)
        placing[pl.ds(part * DEV, DEV), 0:DEV] = here
        placing[pl.ds(part * DEV, DEV), DEV : 2 * DEV] = here
    for copy in copies:
        copy.wait()
    odd = lax.axis_index("lat") % 2 == 1
    for n in range(6):
        for half in range(2):
            levels = range(8 * half, 8 * half + 8)
            lines = []
            for side in range(2):
                row = 7 * side
                pick = lambda ref, k: ref[side, k, pl.ds(row, 1), :]
                if n < TR:
                    parts = [tr_s[side, n, k, pl.ds(row, 1), :] for k in levels]
                elif n == TR:
                    parts = [pick(fill_s, k) * pick(mask_s, k).astype(F32) for k in levels]
                else:
                    parts = [pick(north_s, k) for k in levels]
                lines.append(jnp.concatenate(parts, axis=0))
            at = pl.ds(n * 16 + 8 * half, 8)
            ns_one[at, :] = jnp.where(odd, lines[0], lines[1])
            ns_two[at, :] = jnp.where(odd, lines[1], lines[0])


def kernel_rows_call(tracers, fill, mask, north, owner):
    hbm = pl.BlockSpec(memory_space=pltpu.HBM)
    vmem = pl.BlockSpec(memory_space=pltpu.VMEM)
    return pl.pallas_call(
        kernel_rows,
        name="rows",
        out_shape=(
            jax.ShapeDtypeStruct((96, 128), F32),
            jax.ShapeDtypeStruct((96, 128), F32),
            jax.ShapeDtypeStruct((CAP * DEV, 2 * DEV), BF16),
            jax.ShapeDtypeStruct((512, 128), BF16),
        ),
        in_specs=[hbm] * 5,
        out_specs=(vmem,) * 4,
        scratch_shapes=[
            pltpu.VMEM((2, TR, LV, 8, LANES), F32),
            pltpu.VMEM((2, LV, 8, LANES), F32),
            pltpu.VMEM((2, LV, 8, LANES), jnp.int32),
            pltpu.VMEM((2, LV, 8, LANES), F32),
            pltpu.VMEM((1, DEV), jnp.int32),
            pltpu.SemaphoreType.DMA((4, 2)),
            pltpu.SemaphoreType.DMA,
        ],
        compiler_params=pltpu.CompilerParams(vmem_limit_bytes=4 * MIB),
        cost_estimate=pl.CostEstimate(flops=1_000_000, bytes_accessed=MIB, transcendentals=0),
    )(tracers, fill, mask, north, owner)


def kernel_edges(tr_v, fill_v, mask_v, east_v, h_v, ew):
    lane = lane_iota()

    def level(k, carry):
        where_t = [(lane >> 1) == t * 16 + k for t in range(TR)]

        for v in range(16):
            at = row_set(32 * (v // 4) + v % 4)
            h = 0.5 * (fill_v[(k, *at)] * mask_v[(k, *at)].astype(F32))
            h_v[k, v] = h
            base = 64 * (v % 2)
            packed = ew[16 + v // 2]
            packed = jnp.where(
                (lane >> 1) == k + base // 2, pltpu.roll(h, 2 * k + 1 + base, 1), packed
            )
            ew[16 + v // 2] = jnp.where(
                (lane >> 1) == k + 16 + base // 2,
                pltpu.roll(east_v[(k, *at)], 2 * k + 33 + base, 1),
                packed,
            )
            packed = ew[v]
            for t in range(TR):
                moved = pltpu.roll(tr_v[(t, k, *at)], 2 * k + 32 * t + 1, 1)
                packed = jnp.where(where_t[t], moved, packed)
            ew[v] = packed
        return carry

    lax.fori_loop(0, LV, level, 0)


def kernel_edges_call(tracers, fill, mask, east):
    vmem = pl.BlockSpec(memory_space=pltpu.VMEM)
    return pl.pallas_call(
        kernel_edges,
        name="edges",
        out_shape=(
            jax.ShapeDtypeStruct((LV, 16, 8, LANES), F32),
            jax.ShapeDtypeStruct((24, 8, 128), F32),
        ),
        in_specs=[vmem] * 4,
        out_specs=(vmem,) * 2,
        compiler_params=pltpu.CompilerParams(vmem_limit_bytes=16 * MIB),
        cost_estimate=pl.CostEstimate(flops=60_000_000, bytes_accessed=11 * MIB, transcendentals=0),
    )(tracers, fill, mask, east)


def kernel_first(
    tr_s, h_v, east_s, north_s, area_v, diff, pool,
    num2, den2,
    area_s, g_s, face_s, coef, store,
):
    lane, sub = lane_iota(), sub_iota()
    is_even = (lane & 1) == 0
    not_last, not_top = lane < 127, sub < 7
    swap = jnp.where(is_even, lane + 127, lane + 1) & 127
    for v in range(16):
        area_s[v] = 2.0 * area_v[row_set(32 * (v // 4) + v % 4)]

    def level(k):
        twice_mixing = 2.0 * diff[k]

        for v in range(16):
            h, u = h_v[k, v], east_s[(k, *row_set(32 * (v // 4) + v % 4))]
            p_e, q_e = half_face(
                h, pltpu.roll(h, 127, 1), u, pltpu.roll(u, 127, 1), twice_mixing, keep=not_last
            )
            g_s[v] = depth_gain(2.0 * h)
            face_s[0, v] = p_e
            face_s[1, v] = q_e

        for v in range(16):
            start = 32 * (v // 4) + v % 4
            h, speed = h_v[k, v], north_s[(k, *row_set(start))]
            keep = None
            if v == 15:
                h_up, keep = pltpu.roll(h_v[k, 12], 7, 0), not_top
                speed_up = pltpu.roll(north_s[(k, *row_set(96))], 7, 0)
            else:
                speed_up = north_s[(k, *row_set(start + 1))]
                if v % 4 < 3:
                    h_up = h_v[k, v + 1]
                else:
                    h_up = jnp.where(
                        not_top, pltpu.roll(h_v[k, v - 3], 7, 0), pltpu.roll(h_v[k, v + 1], 7, 0)
                    )
            p_n, q_n = half_face(h, h_up, speed, speed_up, twice_mixing, keep)
            face_s[2, v] = p_n
            face_s[3, v] = q_n

        for q in range(4):
            south = []
            for n in (2, 3):
                low = pltpu.roll(face_s[n, 4 * q + 3], 1, 0)
                under = pltpu.roll(face_s[n, 4 * q - 1], 1, 0) if q else 0.0
                south.append(jnp.where(sub > 0, low, under))
            for par in range(2):
                centre, weight = [], 0.0
                for n in range(2):
                    v = 4 * q + 2 * par + n
                    h, g = h_v[k, v], g_s[v]
                    w = area_s[v] * h
                    p_e, q_w = face_s[0, v], pltpu.roll(face_s[1, v], 1, 1)
                    p_n, q_n = face_s[2, v], face_s[3, v]
                    p_s, q_s = south if v % 4 == 0 else (
                        face_s[2, v - 1], face_s[3, v - 1]
                    )
                    to_west = pltpu.roll(g, 1, 1) * q_w
                    to_east = pltpu.roll(g, 127, 1) * p_e
                    own = w - g * ((p_e + q_w) + (p_n + q_s))
                    centre.append(own + jnp.where(is_even, to_east, to_west))
                    coef[4 + n, 2 * q + par] = jnp.where(is_even, to_west, to_east)
                    if n == 0:
                        low, up = g * p_s, g * q_n
                    else:
                        down, high = g * p_s, g * q_n
                    weight = weight + w
                coef[0, 2 * q + par] = low
                coef[1, 2 * q + par] = centre[0] + down
                coef[2, 2 * q + par] = centre[1] + up
                coef[3, 2 * q + par] = high
                store[pl.ds(128 + q * 8, 8), pl.ds(par * 128, 128)] = weight

        for q in range(4):
            for par in range(2):
                low_c, a_c, b_c, high_c, a_x, b_x = [coef[n, 2 * q + par] for n in range(6)]
                for t in range(TR):
                    cell = lambda start: tr_s[(t, k, *row_set(start))]
                    start = 32 * q + 2 * par
                    a, b = cell(start), cell(start + 1)
                    low = cell(start - 1) if start else pltpu.roll(cell(3), 1, 0)
                    high = cell(start + 2) if start < 98 else pltpu.roll(cell(96), 7, 0)
                    side = a_x * a + b_x * b
                    value = (a_c * a + b_c * b) + (low_c * low + high_c * high)
                    value = value + jnp.take_along_axis(side, swap, axis=1)
                    store[pl.ds(t * 32 + q * 8, 8), pl.ds(par * 128, 128)] = value

    def pooled(k):
        both = jnp.concatenate(halves(store[...]), axis=1)
        values = jnp.dot(both, pool[...], preferred_element_type=F32)
        rows = pl.ds(pl.multiple_of(k * 32, 32), 32)
        for t in range(TR):
            num2[t, rows, :] = values[t * 32 : t * 32 + 32]
        den2[rows, :] = values[128:160]

    def group_body(k, carry):
        pooled((k + LV - 1) % LV)
        level(k)
        return carry

    store[...] = jnp.zeros_like(store)
    lax.fori_loop(0, LV, group_body, 0)
    pooled(LV - 1)


def kernel_first_call(tr_v, h_v, east_v, north_v, area_v, diff, pool):
    vmem = pl.BlockSpec(memory_space=pltpu.VMEM)
    return pl.pallas_call(
        kernel_first,
        name="first",
        out_shape=(
            jax.ShapeDtypeStruct((TR, 512, 128), F32),
            jax.ShapeDtypeStruct((512, 128), F32),
        ),
        in_specs=[vmem] * 5 + [pl.BlockSpec(memory_space=pltpu.SMEM), vmem],
        out_specs=(vmem,) * 2,
        scratch_shapes=[
            pltpu.VMEM((16, 8, 128), F32),
            pltpu.VMEM((16, 8, 128), F32),
            pltpu.VMEM((4, 16, 8, 128), F32),
            pltpu.VMEM((6, 8, 8, 128), F32),
            pltpu.VMEM((160, 256), F32),
        ],
        compiler_params=pltpu.CompilerParams(vmem_limit_bytes=16 * MIB),
        cost_estimate=pl.CostEstimate(flops=60_000_000, bytes_accessed=11 * MIB, transcendentals=0),
    )(tr_v, h_v, east_v, north_v, area_v, diff, pool)


def spread(values, offset):
    index = (lane_iota() & 31) + offset
    return jnp.take_along_axis(values, index, axis=1)


def kernel_second(
    num2, den2, ew, ew_one, ew_two, ns_one, ns_two, got_one, got_two, diff, placing,
    send, d_ew, d_ns,
    work, acc, chunks, send_s, sems,
):
    lane, sub = lane_iota(), sub_iota()
    odd = lax.axis_index("lat") % 2 == 1
    odd_lon = lax.axis_index("lon") % 2 == 1
    at_fold = lax.axis_index("lat") == lax.axis_size("lat") - 1
    is_east = (lane & 1) == 0
    level_of = (lane >> 1) & 15
    mixing = jnp.zeros((8, 128), F32)
    for k in range(LV):
        mixing = jnp.where(level_of == k, 2.0 * diff[k], mixing)

    def neighbour(n):
        one, two = ew_one[n], ew_two[n]
        from_east, from_west = jnp.where(odd_lon, two, one), jnp.where(odd_lon, one, two)
        return jnp.where(is_east, pltpu.roll(from_east, 127, 1), pltpu.roll(from_west, 1, 1))

    pending = None
    for v in range(16):
        own_hu, near_hu = ew[16 + v // 2], neighbour(16 + v // 2)
        base = 64 * (v % 2)
        h = spread(own_hu, base)
        p, q = half_face(
            h, spread(near_hu, base), spread(own_hu, base + 32), spread(near_hu, base + 32), mixing
        )
        div = jnp.where(is_east, q, p) * neighbour(v) - jnp.where(is_east, p, q) * ew[v]
        d_ew[v] = div
        value = depth_gain(2.0 * h) * div
        if v % 2 == 0:
            pending = value
        else:
            value = pending + value
            far_value = pltpu.roll(value, 64, 1)
            q, par = v // 4, (v // 2) % 2
            plain = jnp.where(is_east, value, far_value)
            moved = jnp.where(is_east, far_value, value)
            if par == 0:
                lower = plain, moved
            else:
                for half in range(2):
                    first_lanes = (lane < 64) == is_east
                    mine = first_lanes if half == 0 else ~first_lanes
                    work[half, q] = jnp.where(mine, lower[0], moved)

    ends = ((lane & 63) == 0) | ((lane & 63) == 63)

    def add_ends(step, carry):
        for n in range(EACH):
            k = step * EACH + n
            for t in range(TR):
                for q in range(4):
                    rows = pl.ds(pl.multiple_of(k * 32 + q * 8, 8), 8)
                    moved = pltpu.roll(work[t // 2, q], 63 - 2 * k + (128 - 32 * t), 1)
                    acc[t, rows, :] = num2[t, rows, :] + jnp.where(ends, moved, 0.0)
        return carry

    lax.fori_loop(0, LV // EACH, add_ends, 0)

    source = sub_iota((128, 128))
    target = lane_iota((128, 128))
    pools = [
        jnp.where(target == par * 64 + (source >> 1), 1.0, 0.0).astype(BF16) for par in range(2)
    ]
    quarter = [
        jnp.where(target == j * 32 + ((source & 63) >> 1), 1.0, 0.0).astype(BF16) for j in range(4)
    ]

    back = 127 - lane
    for half in range(2):
        mix = jnp.zeros((8, 128), F32)
        for k in range(8):
            mix = jnp.where(sub == k, diff[8 * half + k], mix)

        def rows_of(ref, n):
            return ref[pl.ds(n * 16 + 8 * half, 8), :]

        def own(n, top):
            pair = (ns_two, ns_one) if top else (ns_one, ns_two)
            return jnp.where(odd, rows_of(pair[0], n), rows_of(pair[1], n))

        def near(n, top, sign=1.0):
            if not top:
                return jnp.where(odd, rows_of(got_one, n), rows_of(got_two, n))
            value = jnp.where(odd, rows_of(got_two, n), rows_of(got_one, n))
            turned = sign * jnp.take_along_axis(value, back, axis=1)
            return jnp.where(at_fold, turned, value)

        for top in (False, True):
            h = own(4, top)
            p, q = face(h, near(4, top), own(5, top), near(5, top, -1.0), mix)
            gain = depth_gain(h)
            for t in range(TR):
                if top:
                    div = q * near(t, top) - p * own(t, top)
                else:
                    div = p * near(t, top) - q * own(t, top)
                d_ns[int(top), pl.ds(t * 16 + 8 * half, 8), :] = div
                at = (t, pl.ds(256 * half + 31 * int(top), 8, stride=32), slice(None))
                acc[at] = acc[at] + split_dot(gain * div, pools[int(top)])

    def keep(n, values):
        high, low = halves(values)
        chunks[0:128, pl.ds(n * 128, 128)] = high
        chunks[128:256, pl.ds(n * 128, 128)] = low

    def every_fourth(ref, *lead, j):
        return jnp.concatenate(
            [ref[(*lead, pl.ds(32 * m + j, 8, stride=4), slice(None))] for m in range(16)], axis=0
        )

    gains = []
    den4 = jnp.zeros((128, 128), F32)
    for j in range(4):
        den = every_fourth(den2, j=j)
        gains.append(1.0 / jnp.maximum(den, weight_floor))
        den4 = den4 + split_dot(den, quarter[j])
    gain4 = 1.0 / jnp.maximum(den4, weight_floor)
    for t in range(TR):
        num4 = jnp.zeros((128, 128), F32)
        for j in range(4):
            num = every_fourth(acc, t, j=j)
            keep(t * 4 + j, num * gains[j])
            num4 = num4 + split_dot(num, quarter[j])
        keep(16 + t, num4 * gain4)

    each = CAP * DEV // PARTS
    copies = []
    for part in range(PARTS):
        left = placing[pl.ds(part * each, each), :]
        for n in range(CHUNKS // 2):
            placed = jnp.dot(left, chunks[:, pl.ds(n * 256, 256)], preferred_element_type=F32)
            for c in range(2):
                for m in range(each // 8):
                    start = (part * each + m * 8) * CHUNKS + 2 * n + c
                    send_s[pl.ds(start, 8, stride=CHUNKS), :] = placed[
                        m * 8 : m * 8 + 8, c * 128 : c * 128 + 128
                    ]
        rows = pl.ds(part * each * CHUNKS, each * CHUNKS)
        copies.append(pltpu.make_async_copy(send_s.at[rows], send.at[rows], sems.at[part]))
        copies[-1].start()
    for copy in copies:
        copy.wait()


def kernel_second_call(*args):
    vmem = pl.BlockSpec(memory_space=pltpu.VMEM)
    return pl.pallas_call(
        kernel_second,
        name="second",
        out_shape=(
            pltpu.HBM((DEV * CAP * CHUNKS, 128), F32),
            jax.ShapeDtypeStruct((16, 8, 128), F32),
            jax.ShapeDtypeStruct((2, 64, 128), F32),
        ),
        in_specs=[vmem] * 9 + [pl.BlockSpec(memory_space=pltpu.SMEM), vmem],
        out_specs=(pl.BlockSpec(memory_space=pltpu.HBM), vmem, vmem),
        scratch_shapes=[
            pltpu.VMEM((2, 4, 8, 128), F32),
            pltpu.VMEM((TR, 512, 128), F32),
            pltpu.VMEM((256, 2560), BF16),
            pltpu.VMEM((DEV * CAP * CHUNKS, 128), F32),
            pltpu.SemaphoreType.DMA((PARTS,)),
        ],
        compiler_params=pltpu.CompilerParams(vmem_limit_bytes=16 * MIB),
        cost_estimate=pl.CostEstimate(flops=60_000_000, bytes_accessed=6 * MIB, transcendentals=0),
    )(*args)


def kernel_third(
    tr, fill, mask, east, north, diff, area, d_ew, d_ns,
    out,
    tr_s, fill_s, mask_s, east_s, north_s, area_s, out_s, moved_s, sems, area_sem, out_sems,
):
    hbm, vmem = (tr, fill, mask, east, north), (tr_s, fill_s, mask_s, east_s, north_s)
    copies = input_copies(hbm, vmem, sems)
    area_copy = pltpu.make_async_copy(area, area_s, area_sem)
    for group in range(GROUPS):
        for copy in copies(group):
            copy.start()
        if group == 0:
            area_copy.start()
    area_copy.wait()
    lane, sub = lane_iota(), sub_iota()
    ends = (lane == 0) | (lane == 127)
    not_last, not_top = lane < 127, sub < 7
    per = LV // GROUPS

    def out_copy(group):
        levels = pl.ds(group * per, per)
        return pltpu.make_async_copy(out_s.at[:, levels], out.at[:, levels], out_sems.at[group])

    def level(k):
        mixing = diff[k]

        def load(ref, start):
            return ref[(k, *row_set(start))]

        def depth(start):
            return load(fill_s, start) * load(mask_s, start).astype(F32)

        for v in range(16):
            edge = d_ew[v]
            for t in range(TR):
                moved = pltpu.roll(edge, 127 - 2 * k + (128 - 32 * t), 1)
                moved_s[v, t] = jnp.where(ends, moved, 0.0)

        before = [jnp.zeros((8, 128), F32)] * TR
        for q in range(4):
            hs = [depth(32 * q + j) for j in range(4)]
            vs = [load(north_s, 32 * q + j) for j in range(4)]
            if q < 3:
                hs.append(depth(32 * q + 4))
                vs.append(load(north_s, 32 * q + 4))
            else:
                hs.append(pltpu.roll(hs[0], 7, 0))
                vs.append(pltpu.roll(vs[0], 7, 0))
            coefs = []
            for j in range(4):
                top = q == 3 and j == 3
                h, u = hs[j], load(east_s, 32 * q + j)
                rate = time_step / (area_s[row_set(32 * q + j)] * jnp.maximum(h, depth_floor))
                coefs.append(
                    face(h, pltpu.roll(h, 127, 1), u, pltpu.roll(u, 127, 1), mixing, keep=not_last)
                    + face(h, hs[j + 1], vs[j], vs[j + 1], mixing, keep=not_top if top else None)
                    + (rate,)
                )
            for t in range(TR):
                cells = [tr_s[(t, k, *row_set(32 * q + j))] for j in range(4)]
                if q < 3:
                    cells.append(tr_s[(t, k, *row_set(32 * q + 4))])
                else:
                    cells.append(pltpu.roll(cells[0], 7, 0))
                norths = [coefs[j][2] * cells[j] - coefs[j][3] * cells[j + 1] for j in range(4)]
                turned = pltpu.roll(norths[3], 1, 0)
                souths = [jnp.where(sub > 0, turned, before[t])] + norths[:3]
                before[t] = turned
                for j in range(4):
                    p_e, q_e, _, _, rate = coefs[j]
                    cell = cells[j]
                    flux = p_e * cell - q_e * pltpu.roll(cell, 127, 1)
                    div = (pltpu.roll(flux, 1, 1) - flux) + (souths[j] - norths[j])
                    div = div + moved_s[4 * q + j, t]
                    if q == 0 and j == 0:
                        div = div + jnp.where(sub == 0, d_ns[0, pl.ds(t * 16 + k, 1), :], 0.0)
                    if q == 3 and j == 3:
                        div = div + jnp.where(sub == 7, d_ns[1, pl.ds(t * 16 + k, 1), :], 0.0)
                    out_s[(t, k, *row_set(32 * q + j))] = cell + rate * div

    def group_body(group, carry):
        for copy in copies(group):
            copy.wait()
        for n in range(per):
            level(group * per + n)
        out_copy(group).start()
        return carry

    lax.fori_loop(0, GROUPS, group_body, 0)
    for group in range(GROUPS):
        out_copy(group).wait()


def kernel_third_call(tracers, fill, mask, east, north, diff, area, d_ew, d_ns):
    hbm = pl.BlockSpec(memory_space=pltpu.HBM)
    vmem = pl.BlockSpec(memory_space=pltpu.VMEM)
    return pl.pallas_call(
        kernel_third,
        name="third",
        out_shape=jax.ShapeDtypeStruct((TR, LV, ROWS, LANES), F32),
        in_specs=[hbm] * 5 + [pl.BlockSpec(memory_space=pltpu.SMEM), hbm, vmem, vmem],
        out_specs=hbm,
        scratch_shapes=[
            pltpu.VMEM((TR, LV, ROWS, LANES), F32),
            pltpu.VMEM((LV, ROWS, LANES), F32),
            pltpu.VMEM((LV, ROWS, LANES), jnp.int32),
            pltpu.VMEM((LV, ROWS, LANES), F32),
            pltpu.VMEM((LV, ROWS, LANES), F32),
            pltpu.VMEM((ROWS, LANES), F32),
            pltpu.VMEM((TR, LV, ROWS, LANES), F32),
            pltpu.VMEM((16, TR, 8, 128), F32),
            pltpu.SemaphoreType.DMA((5, GROUPS)),
            pltpu.SemaphoreType.DMA,
            pltpu.SemaphoreType.DMA((GROUPS,)),
        ],
        compiler_params=pltpu.CompilerParams(vmem_limit_bytes=24 * MIB),
        cost_estimate=pl.CostEstimate(flops=60_000_000, bytes_accessed=12 * MIB, transcendentals=0),
    )(tracers, fill, mask, east, north, diff, area, d_ew, d_ns)


SPLITS = 4


def kernel_last(got, two, four):
    for m in range(32 // SPLITS):
        for n in range(CHUNKS):
            value = got[pl.ds(m * 8 * CHUNKS + n, 8, stride=CHUNKS), :]
            if n < 16:
                two[pl.ds(m * 8, 8), pl.ds(n * 128, 128)] = value
            else:
                four[pl.ds(m * 8, 8), pl.ds((n - 16) * 128, 128)] = value


def kernel_last_call(got):
    return pl.pallas_call(
        kernel_last,
        name="last",
        grid=(SPLITS,),
        out_shape=(
            jax.ShapeDtypeStruct((DEV * CAP, 2048), F32),
            jax.ShapeDtypeStruct((DEV * CAP, 512), F32),
        ),
        in_specs=[pl.BlockSpec((DEV * 40 // SPLITS, 128), lambda s: (s, 0))],
        out_specs=(
            pl.BlockSpec((DEV * CAP // SPLITS, 2048), lambda s: (s, 0)),
            pl.BlockSpec((DEV * CAP // SPLITS, 512), lambda s: (s, 0)),
        ),
        compiler_params=pltpu.CompilerParams(vmem_limit_bytes=8 * MIB),
    )(got)


def local(
    tracers, fill_fraction, ocean_mask, east_speed, north_speed, diffusivity, cell_area, owner_map
):
    lon_count = lax.axis_size("lon")
    lat_count = lax.axis_size("lat")
    *in_hbm, diffusivity, area_hbm, owners = (
        pltpu.with_memory_space_constraint(x, pltpu.HBM)
        for x in (
            tracers, fill_fraction, ocean_mask, east_speed, north_speed, diffusivity, cell_area,
            owner_map.reshape(1, DEV),
        )
    )
    ns_one, ns_two, placing, pool = kernel_rows_call(
        in_hbm[0], in_hbm[1], in_hbm[2], in_hbm[4], owners
    )
    both = ("lon", "lat")

    def swapped(pairs):
        return [pair for a, b in pairs for pair in ((a, b), (b, a))]

    def at(lon, lat):
        return lon * lat_count + lat

    lons = range(lon_count)
    step_one = [(at(n, a), at(n, a + 1)) for n in lons for a in range(0, lat_count, 2)]
    step_two = [(at(n, a), at(n, a + 1)) for n in lons for a in range(1, lat_count - 1, 2)]
    fold = [
        (at(n, lat_count - 1), at(lon_count - 1 - n, lat_count - 1)) for n in range(lon_count // 2)
    ]
    got_one = lax.ppermute(ns_one, both, swapped(step_one))
    got_two = lax.ppermute(ns_two, both, swapped(step_two + fold))
    h_v, ew = kernel_edges_call(tracers, fill_fraction, ocean_mask, east_speed)
    ew_one = lax.ppermute(ew, "lon", swapped([(n, n + 1) for n in range(0, lon_count, 2)]))
    ew_two = lax.ppermute(
        ew, "lon", swapped([(n, (n + 1) % lon_count) for n in range(1, lon_count, 2)])
    )
    num2, den2 = kernel_first_call(
        tracers, h_v, east_speed, north_speed, cell_area, diffusivity, pool
    )
    send, d_ew, d_ns = kernel_second_call(
        num2, den2, ew, ew_one, ew_two, ns_one, ns_two, got_one, got_two, diffusivity, placing
    )
    got = lax.all_to_all(
        send.reshape(DEV, CAP * CHUNKS, 128), both, split_axis=0, concat_axis=0, tiled=True
    )
    updated = kernel_third_call(*in_hbm, diffusivity, area_hbm, d_ew, d_ns)
    two, four = kernel_last_call(got.reshape(DEV * CAP * CHUNKS, 128))
    return (updated, two[None], four[None])


def solution(mesh):
    in_specs = (
        P(None, None, "lat", "lon"),
        P(None, "lat", "lon"),
        P(None, "lat", "lon"),
        P(None, "lat", "lon"),
        P(None, "lat", "lon"),
        P(),
        P("lat", "lon"),
        P(("lon", "lat"), None),
    )
    out_specs = (
        P(None, None, "lat", "lon"),
        P(("lon", "lat"), None, None),
        P(("lon", "lat"), None, None),
    )
    return jax.shard_map(
        local,
        mesh=mesh, in_specs=in_specs, out_specs=out_specs, check_vma=False,
    )
```

```python
import jax
import jax.numpy as jnp
from jax import lax
from jax.experimental import pallas as pl
from jax.experimental.pallas import tpu as pltpu
from jax.sharding import PartitionSpec as P


time_step = 0.05
depth_floor = 0.25
weight_floor = 0.25

TR, LV = 4, 16
ROWS, LANES = 128, 128
GROUPS = 16
DEV, CAP = 128, 2
CHUNKS = 20
PARTS = 2
EACH = 16
PAIR = 2
STEP = 8
F32, BF16 = jnp.float32, jnp.bfloat16
MIB = 1 << 20


def lane_iota(shape=(8, 128)):
    return lax.broadcasted_iota(jnp.int32, shape, len(shape) - 1)


def sub_iota(shape=(8, 128)):
    return lax.broadcasted_iota(jnp.int32, shape, len(shape) - 2)


def face(lower_h, upper_h, lower_speed, upper_speed, mixing, keep=None):
    open_depth = jnp.minimum(lower_h, upper_h)
    if keep is not None:
        open_depth = jnp.where(keep, open_depth, 0.0)
    speed = 0.5 * (lower_speed + upper_speed)
    ahead = jnp.maximum(speed, 0.0)
    back = ahead - speed
    return open_depth * (ahead + mixing), open_depth * (back + mixing)


def half_face(lower_half, upper_half, lower_speed, upper_speed, twice_mixing, keep=None):
    open_half = jnp.minimum(lower_half, upper_half)
    if keep is not None:
        open_half = jnp.where(keep, open_half, 0.0)
    speeds = lower_speed + upper_speed
    ahead = jnp.maximum(speeds, 0.0)
    back = ahead - speeds
    return open_half * (ahead + twice_mixing), open_half * (back + twice_mixing)


def depth_gain(h):
    return time_step * jnp.minimum(h * (1.0 / depth_floor), 1.0)


def halves(values):
    high = values.astype(BF16)
    return high, (values - high.astype(F32)).astype(BF16)


def split_dot(left, right):
    high, low = halves(left)
    return jnp.dot(high, right, preferred_element_type=F32) + jnp.dot(
        low, right, preferred_element_type=F32
    )


def input_copies(hbm, vmem, sems):
    per = LV // GROUPS

    def copies(group):
        levels = pl.ds(group * per, per)
        out = [pltpu.make_async_copy(hbm[0].at[:, levels], vmem[0].at[:, levels], sems.at[0, group])]
        for n in range(1, 5):
            out.append(
                pltpu.make_async_copy(hbm[n].at[levels], vmem[n].at[levels], sems.at[n, group])
            )
        return out

    return copies


def row_set(start):
    return (pl.ds(start, 8, stride=4), slice(None))


def kernel_rows(
    tr, fill, mask, north, owner,
    ns_one, ns_two, placing, pool,
    tr_s, fill_s, mask_s, north_s, owner_s, sems, owner_sem,
):
    copies = []
    for n, (src, dst) in enumerate(((tr, tr_s), (fill, fill_s), (mask, mask_s), (north, north_s))):
        for side in range(2):
            rows = pl.ds(side * (ROWS - 8), 8)
            if n == 0:
                copies.append(
                    pltpu.make_async_copy(src.at[:, :, rows], dst.at[side], sems.at[n, side])
                )
            else:
                copies.append(
                    pltpu.make_async_copy(src.at[:, rows], dst.at[side], sems.at[n, side])
                )
            copies[-1].start()
    owner_copy = pltpu.make_async_copy(owner, owner_s, owner_sem)
    owner_copy.start()
    source = sub_iota((256, 128))
    match = lane_iota((256, 128)) == (source >> 7) * 64 + ((source & 127) >> 1)
    for term in range(2):
        pool[pl.ds(256 * term, 256), :] = jnp.where(match, 1.0, 0.0).astype(BF16)
    across = lane_iota((DEV, DEV))
    down = sub_iota((DEV, DEV))
    owner_copy.wait()
    who_row = owner_s[...]
    who = jnp.sum(jnp.where(down == across, who_row, 0), axis=1, keepdims=True)
    same = jnp.where((who == who_row) & (down < across), 1, 0)
    rank = jnp.sum(same, axis=0, keepdims=True)
    row_of = who_row * CAP + rank
    for part in range(CAP):
        here = jnp.where(down + part * DEV == row_of, 1.0, 0.0).astype(BF16)
        placing[pl.ds(part * DEV, DEV), 0:DEV] = here
        placing[pl.ds(part * DEV, DEV), DEV : 2 * DEV] = here
    for copy in copies:
        copy.wait()
    odd = lax.axis_index("lat") % 2 == 1
    for n in range(6):
        for half in range(2):
            levels = range(8 * half, 8 * half + 8)
            lines = []
            for side in range(2):
                row = 7 * side
                pick = lambda ref, k: ref[side, k, pl.ds(row, 1), :]
                if n < TR:
                    parts = [tr_s[side, n, k, pl.ds(row, 1), :] for k in levels]
                elif n == TR:
                    parts = [pick(fill_s, k) * pick(mask_s, k).astype(F32) for k in levels]
                else:
                    parts = [pick(north_s, k) for k in levels]
                lines.append(jnp.concatenate(parts, axis=0))
            at = pl.ds(n * 16 + 8 * half, 8)
            ns_one[at, :] = jnp.where(odd, lines[0], lines[1])
            ns_two[at, :] = jnp.where(odd, lines[1], lines[0])


def kernel_rows_call(tracers, fill, mask, north, owner):
    hbm = pl.BlockSpec(memory_space=pltpu.HBM)
    vmem = pl.BlockSpec(memory_space=pltpu.VMEM)
    return pl.pallas_call(
        kernel_rows,
        name="rows",
        out_shape=(
            jax.ShapeDtypeStruct((96, 128), F32),
            jax.ShapeDtypeStruct((96, 128), F32),
            jax.ShapeDtypeStruct((CAP * DEV, 2 * DEV), BF16),
            jax.ShapeDtypeStruct((512, 128), BF16),
        ),
        in_specs=[hbm] * 5,
        out_specs=(vmem,) * 4,
        scratch_shapes=[
            pltpu.VMEM((2, TR, LV, 8, LANES), F32),
            pltpu.VMEM((2, LV, 8, LANES), F32),
            pltpu.VMEM((2, LV, 8, LANES), jnp.int32),
            pltpu.VMEM((2, LV, 8, LANES), F32),
            pltpu.VMEM((1, DEV), jnp.int32),
            pltpu.SemaphoreType.DMA((4, 2)),
            pltpu.SemaphoreType.DMA,
        ],
        compiler_params=pltpu.CompilerParams(vmem_limit_bytes=4 * MIB),
        cost_estimate=pl.CostEstimate(flops=1_000_000, bytes_accessed=MIB, transcendentals=0),
    )(tracers, fill, mask, north, owner)


def kernel_edges(tr_v, fill_v, mask_v, east_v, h_v, ew):
    lane = lane_iota()

    def level(k, carry):
        where_t = [(lane >> 1) == t * 16 + k for t in range(TR)]

        for v in range(16):
            at = row_set(32 * (v // 4) + v % 4)
            h = 0.5 * (fill_v[(k, *at)] * mask_v[(k, *at)].astype(F32))
            h_v[k, v] = h
            base = 64 * (v % 2)
            packed = ew[16 + v // 2]
            packed = jnp.where(
                (lane >> 1) == k + base // 2, pltpu.roll(h, 2 * k + 1 + base, 1), packed
            )
            ew[16 + v // 2] = jnp.where(
                (lane >> 1) == k + 16 + base // 2,
                pltpu.roll(east_v[(k, *at)], 2 * k + 33 + base, 1),
                packed,
            )
            packed = ew[v]
            for t in range(TR):
                moved = pltpu.roll(tr_v[(t, k, *at)], 2 * k + 32 * t + 1, 1)
                packed = jnp.where(where_t[t], moved, packed)
            ew[v] = packed
        return carry

    def step(n, carry):
        for m in range(STEP):
            level(n * STEP + m, carry)
        return carry

    lax.fori_loop(0, LV // STEP, step, 0)


def kernel_edges_call(tracers, fill, mask, east):
    vmem = pl.BlockSpec(memory_space=pltpu.VMEM)
    return pl.pallas_call(
        kernel_edges,
        name="edges",
        out_shape=(
            jax.ShapeDtypeStruct((LV, 16, 8, LANES), F32),
            jax.ShapeDtypeStruct((24, 8, 128), F32),
        ),
        in_specs=[vmem] * 4,
        out_specs=(vmem,) * 2,
        compiler_params=pltpu.CompilerParams(vmem_limit_bytes=16 * MIB),
        cost_estimate=pl.CostEstimate(flops=60_000_000, bytes_accessed=11 * MIB, transcendentals=0),
    )(tracers, fill, mask, east)


def kernel_first(
    tr_s, h_v, east_s, north_s, area_v, diff, pool,
    num2, den2,
    area_s, gains, all_faces, coefs, stores,
):
    lane, sub = lane_iota(), sub_iota()
    is_even = (lane & 1) == 0
    not_last, not_top = lane < 127, sub < 7
    swap = jnp.where(is_even, lane + 127, lane + 1) & 127
    for v in range(16):
        area_s[v] = 2.0 * area_v[row_set(32 * (v // 4) + v % 4)]

    def level(k, n):
        twice_mixing = 2.0 * diff[k]
        g_s, face_s, coef, store = gains.at[n], all_faces.at[n], coefs.at[n], stores.at[n]

        for v in range(16):
            h, u = h_v[k, v], east_s[(k, *row_set(32 * (v // 4) + v % 4))]
            p_e, q_e = half_face(
                h, pltpu.roll(h, 127, 1), u, pltpu.roll(u, 127, 1), twice_mixing, keep=not_last
            )
            g_s[v] = depth_gain(2.0 * h)
            face_s[0, v] = p_e
            face_s[1, v] = q_e

        for v in range(16):
            start = 32 * (v // 4) + v % 4
            h, speed = h_v[k, v], north_s[(k, *row_set(start))]
            keep = None
            if v == 15:
                h_up, keep = pltpu.roll(h_v[k, 12], 7, 0), not_top
                speed_up = pltpu.roll(north_s[(k, *row_set(96))], 7, 0)
            else:
                speed_up = north_s[(k, *row_set(start + 1))]
                if v % 4 < 3:
                    h_up = h_v[k, v + 1]
                else:
                    h_up = jnp.where(
                        not_top, pltpu.roll(h_v[k, v - 3], 7, 0), pltpu.roll(h_v[k, v + 1], 7, 0)
                    )
            p_n, q_n = half_face(h, h_up, speed, speed_up, twice_mixing, keep)
            face_s[2, v] = p_n
            face_s[3, v] = q_n

        for q in range(4):
            south = []
            for n in (2, 3):
                low = pltpu.roll(face_s[n, 4 * q + 3], 1, 0)
                under = pltpu.roll(face_s[n, 4 * q - 1], 1, 0) if q else 0.0
                south.append(jnp.where(sub > 0, low, under))
            for par in range(2):
                centre, weight = [], 0.0
                for n in range(2):
                    v = 4 * q + 2 * par + n
                    h, g = h_v[k, v], g_s[v]
                    w = area_s[v] * h
                    p_e, q_w = face_s[0, v], pltpu.roll(face_s[1, v], 1, 1)
                    p_n, q_n = face_s[2, v], face_s[3, v]
                    p_s, q_s = south if v % 4 == 0 else (
                        face_s[2, v - 1], face_s[3, v - 1]
                    )
                    to_west = pltpu.roll(g, 1, 1) * q_w
                    to_east = pltpu.roll(g, 127, 1) * p_e
                    own = w - g * ((p_e + q_w) + (p_n + q_s))
                    centre.append(own + jnp.where(is_even, to_east, to_west))
                    coef[4 + n, 2 * q + par] = jnp.where(is_even, to_west, to_east)
                    if n == 0:
                        low, up = g * p_s, g * q_n
                    else:
                        down, high = g * p_s, g * q_n
                    weight = weight + w
                coef[0, 2 * q + par] = low
                coef[1, 2 * q + par] = centre[0] + down
                coef[2, 2 * q + par] = centre[1] + up
                coef[3, 2 * q + par] = high
                store[pl.ds(128 + q * 8, 8), pl.ds(par * 128, 128)] = weight

        for q in range(4):
            for par in range(2):
                low_c, a_c, b_c, high_c, a_x, b_x = [coef[n, 2 * q + par] for n in range(6)]
                for t in range(TR):
                    cell = lambda start: tr_s[(t, k, *row_set(start))]
                    start = 32 * q + 2 * par
                    a, b = cell(start), cell(start + 1)
                    low = cell(start - 1) if start else pltpu.roll(cell(3), 1, 0)
                    high = cell(start + 2) if start < 98 else pltpu.roll(cell(96), 7, 0)
                    side = a_x * a + b_x * b
                    value = (a_c * a + b_c * b) + (low_c * low + high_c * high)
                    value = value + jnp.take_along_axis(side, swap, axis=1)
                    store[pl.ds(t * 32 + q * 8, 8), pl.ds(par * 128, 128)] = value

    def pooled(k, n):
        both = jnp.concatenate(halves(stores[n]), axis=1)
        values = jnp.dot(both, pool[...], preferred_element_type=F32)
        rows = pl.ds(pl.multiple_of(k * 32, 32), 32)
        for t in range(TR):
            num2[t, rows, :] = values[t * 32 : t * 32 + 32]
        den2[rows, :] = values[128:160]

    def group_body(k, carry):
        for n in range(PAIR):
            pooled((k * PAIR + n + LV - PAIR) % LV, n)
        for n in range(PAIR):
            level(k * PAIR + n, n)
        return carry

    stores[...] = jnp.zeros_like(stores)
    lax.fori_loop(0, LV // PAIR, group_body, 0)
    for n in range(PAIR):
        pooled(LV - PAIR + n, n)


def kernel_first_call(tr_v, h_v, east_v, north_v, area_v, diff, pool):
    vmem = pl.BlockSpec(memory_space=pltpu.VMEM)
    return pl.pallas_call(
        kernel_first,
        name="first",
        out_shape=(
            jax.ShapeDtypeStruct((TR, 512, 128), F32),
            jax.ShapeDtypeStruct((512, 128), F32),
        ),
        in_specs=[vmem] * 5 + [pl.BlockSpec(memory_space=pltpu.SMEM), vmem],
        out_specs=(vmem,) * 2,
        scratch_shapes=[
            pltpu.VMEM((16, 8, 128), F32),
            pltpu.VMEM((PAIR, 16, 8, 128), F32),
            pltpu.VMEM((PAIR, 4, 16, 8, 128), F32),
            pltpu.VMEM((PAIR, 6, 8, 8, 128), F32),
            pltpu.VMEM((PAIR, 160, 256), F32),
        ],
        compiler_params=pltpu.CompilerParams(vmem_limit_bytes=16 * MIB),
        cost_estimate=pl.CostEstimate(flops=60_000_000, bytes_accessed=11 * MIB, transcendentals=0),
    )(tr_v, h_v, east_v, north_v, area_v, diff, pool)


def spread(values, offset):
    index = (lane_iota() & 31) + offset
    return jnp.take_along_axis(values, index, axis=1)


def kernel_second(
    num2, den2, ew, ew_one, ew_two, ns_one, ns_two, got_one, got_two, diff, placing,
    send, d_ew, d_ns,
    work, acc, chunks, send_s, sems,
):
    lane, sub = lane_iota(), sub_iota()
    odd = lax.axis_index("lat") % 2 == 1
    odd_lon = lax.axis_index("lon") % 2 == 1
    at_fold = lax.axis_index("lat") == lax.axis_size("lat") - 1
    is_east = (lane & 1) == 0
    level_of = (lane >> 1) & 15
    mixing = jnp.zeros((8, 128), F32)
    for k in range(LV):
        mixing = jnp.where(level_of == k, 2.0 * diff[k], mixing)

    def neighbour(n):
        one, two = ew_one[n], ew_two[n]
        from_east, from_west = jnp.where(odd_lon, two, one), jnp.where(odd_lon, one, two)
        return jnp.where(is_east, pltpu.roll(from_east, 127, 1), pltpu.roll(from_west, 1, 1))

    pending = None
    for v in range(16):
        own_hu, near_hu = ew[16 + v // 2], neighbour(16 + v // 2)
        base = 64 * (v % 2)
        h = spread(own_hu, base)
        p, q = half_face(
            h, spread(near_hu, base), spread(own_hu, base + 32), spread(near_hu, base + 32), mixing
        )
        div = jnp.where(is_east, q, p) * neighbour(v) - jnp.where(is_east, p, q) * ew[v]
        d_ew[v] = div
        value = depth_gain(2.0 * h) * div
        if v % 2 == 0:
            pending = value
        else:
            value = pending + value
            far_value = pltpu.roll(value, 64, 1)
            q, par = v // 4, (v // 2) % 2
            plain = jnp.where(is_east, value, far_value)
            moved = jnp.where(is_east, far_value, value)
            if par == 0:
                lower = plain, moved
            else:
                for half in range(2):
                    first_lanes = (lane < 64) == is_east
                    mine = first_lanes if half == 0 else ~first_lanes
                    work[half, q] = jnp.where(mine, lower[0], moved)

    ends = ((lane & 63) == 0) | ((lane & 63) == 63)

    def add_ends(step, carry):
        for n in range(EACH):
            k = step * EACH + n
            for t in range(TR):
                for q in range(4):
                    rows = pl.ds(pl.multiple_of(k * 32 + q * 8, 8), 8)
                    moved = pltpu.roll(work[t // 2, q], 63 - 2 * k + (128 - 32 * t), 1)
                    acc[t, rows, :] = num2[t, rows, :] + jnp.where(ends, moved, 0.0)
        return carry

    lax.fori_loop(0, LV // EACH, add_ends, 0)

    source = sub_iota((128, 128))
    target = lane_iota((128, 128))
    pools = [
        jnp.where(target == par * 64 + (source >> 1), 1.0, 0.0).astype(BF16) for par in range(2)
    ]
    quarter = [
        jnp.where(target == j * 32 + ((source & 63) >> 1), 1.0, 0.0).astype(BF16) for j in range(4)
    ]

    back = 127 - lane
    for half in range(2):
        mix = jnp.zeros((8, 128), F32)
        for k in range(8):
            mix = jnp.where(sub == k, diff[8 * half + k], mix)

        def rows_of(ref, n):
            return ref[pl.ds(n * 16 + 8 * half, 8), :]

        def own(n, top):
            pair = (ns_two, ns_one) if top else (ns_one, ns_two)
            return jnp.where(odd, rows_of(pair[0], n), rows_of(pair[1], n))

        def near(n, top, sign=1.0):
            if not top:
                return jnp.where(odd, rows_of(got_one, n), rows_of(got_two, n))
            value = jnp.where(odd, rows_of(got_two, n), rows_of(got_one, n))
            turned = sign * jnp.take_along_axis(value, back, axis=1)
            return jnp.where(at_fold, turned, value)

        for top in (False, True):
            h = own(4, top)
            p, q = face(h, near(4, top), own(5, top), near(5, top, -1.0), mix)
            gain = depth_gain(h)
            for t in range(TR):
                if top:
                    div = q * near(t, top) - p * own(t, top)
                else:
                    div = p * near(t, top) - q * own(t, top)
                d_ns[int(top), pl.ds(t * 16 + 8 * half, 8), :] = div
                at = (t, pl.ds(256 * half + 31 * int(top), 8, stride=32), slice(None))
                acc[at] = acc[at] + split_dot(gain * div, pools[int(top)])

    def keep(n, values):
        high, low = halves(values)
        chunks[0:128, pl.ds(n * 128, 128)] = high
        chunks[128:256, pl.ds(n * 128, 128)] = low

    def every_fourth(ref, *lead, j):
        return jnp.concatenate(
            [ref[(*lead, pl.ds(32 * m + j, 8, stride=4), slice(None))] for m in range(16)], axis=0
        )

    gains = []
    den4 = jnp.zeros((128, 128), F32)
    for j in range(4):
        den = every_fourth(den2, j=j)
        gains.append(1.0 / jnp.maximum(den, weight_floor))
        den4 = den4 + split_dot(den, quarter[j])
    gain4 = 1.0 / jnp.maximum(den4, weight_floor)
    for t in range(TR):
        num4 = jnp.zeros((128, 128), F32)
        for j in range(4):
            num = every_fourth(acc, t, j=j)
            keep(t * 4 + j, num * gains[j])
            num4 = num4 + split_dot(num, quarter[j])
        keep(16 + t, num4 * gain4)

    each = CAP * DEV // PARTS
    copies = []
    for part in range(PARTS):
        left = placing[pl.ds(part * each, each), :]
        for n in range(CHUNKS // 2):
            placed = jnp.dot(left, chunks[:, pl.ds(n * 256, 256)], preferred_element_type=F32)
            for c in range(2):
                for m in range(each // 8):
                    start = (part * each + m * 8) * CHUNKS + 2 * n + c
                    send_s[pl.ds(start, 8, stride=CHUNKS), :] = placed[
                        m * 8 : m * 8 + 8, c * 128 : c * 128 + 128
                    ]
        rows = pl.ds(part * each * CHUNKS, each * CHUNKS)
        copies.append(pltpu.make_async_copy(send_s.at[rows], send.at[rows], sems.at[part]))
        copies[-1].start()
    for copy in copies:
        copy.wait()


def kernel_second_call(*args):
    vmem = pl.BlockSpec(memory_space=pltpu.VMEM)
    return pl.pallas_call(
        kernel_second,
        name="second",
        out_shape=(
            pltpu.HBM((DEV * CAP * CHUNKS, 128), F32),
            jax.ShapeDtypeStruct((16, 8, 128), F32),
            jax.ShapeDtypeStruct((2, 64, 128), F32),
        ),
        in_specs=[vmem] * 9 + [pl.BlockSpec(memory_space=pltpu.SMEM), vmem],
        out_specs=(pl.BlockSpec(memory_space=pltpu.HBM), vmem, vmem),
        scratch_shapes=[
            pltpu.VMEM((2, 4, 8, 128), F32),
            pltpu.VMEM((TR, 512, 128), F32),
            pltpu.VMEM((256, 2560), BF16),
            pltpu.VMEM((DEV * CAP * CHUNKS, 128), F32),
            pltpu.SemaphoreType.DMA((PARTS,)),
        ],
        compiler_params=pltpu.CompilerParams(vmem_limit_bytes=16 * MIB),
        cost_estimate=pl.CostEstimate(flops=60_000_000, bytes_accessed=6 * MIB, transcendentals=0),
    )(*args)


def kernel_third(
    tr, fill, mask, east, north, diff, area, d_ew, d_ns,
    out,
    tr_s, fill_s, mask_s, east_s, north_s, area_s, out_s, moved_s, sems, area_sem, out_sems,
):
    hbm, vmem = (tr, fill, mask, east, north), (tr_s, fill_s, mask_s, east_s, north_s)
    copies = input_copies(hbm, vmem, sems)
    area_copy = pltpu.make_async_copy(area, area_s, area_sem)
    for group in range(GROUPS):
        for copy in copies(group):
            copy.start()
        if group == 0:
            area_copy.start()
    area_copy.wait()
    lane, sub = lane_iota(), sub_iota()
    ends = (lane == 0) | (lane == 127)
    not_last, not_top = lane < 127, sub < 7
    per = LV // GROUPS

    def out_copy(group):
        levels = pl.ds(group * per, per)
        return pltpu.make_async_copy(out_s.at[:, levels], out.at[:, levels], out_sems.at[group])

    def level(k):
        mixing = diff[k]

        def load(ref, start):
            return ref[(k, *row_set(start))]

        def depth(start):
            return load(fill_s, start) * load(mask_s, start).astype(F32)

        for v in range(16):
            edge = d_ew[v]
            for t in range(TR):
                moved = pltpu.roll(edge, 127 - 2 * k + (128 - 32 * t), 1)
                moved_s[v, t] = jnp.where(ends, moved, 0.0)

        before = [jnp.zeros((8, 128), F32)] * TR
        for q in range(4):
            hs = [depth(32 * q + j) for j in range(4)]
            vs = [load(north_s, 32 * q + j) for j in range(4)]
            if q < 3:
                hs.append(depth(32 * q + 4))
                vs.append(load(north_s, 32 * q + 4))
            else:
                hs.append(pltpu.roll(hs[0], 7, 0))
                vs.append(pltpu.roll(vs[0], 7, 0))
            coefs = []
            for j in range(4):
                top = q == 3 and j == 3
                h, u = hs[j], load(east_s, 32 * q + j)
                rate = time_step / (area_s[row_set(32 * q + j)] * jnp.maximum(h, depth_floor))
                coefs.append(
                    face(h, pltpu.roll(h, 127, 1), u, pltpu.roll(u, 127, 1), mixing, keep=not_last)
                    + face(h, hs[j + 1], vs[j], vs[j + 1], mixing, keep=not_top if top else None)
                    + (rate,)
                )
            for t in range(TR):
                cells = [tr_s[(t, k, *row_set(32 * q + j))] for j in range(4)]
                if q < 3:
                    cells.append(tr_s[(t, k, *row_set(32 * q + 4))])
                else:
                    cells.append(pltpu.roll(cells[0], 7, 0))
                norths = [coefs[j][2] * cells[j] - coefs[j][3] * cells[j + 1] for j in range(4)]
                turned = pltpu.roll(norths[3], 1, 0)
                souths = [jnp.where(sub > 0, turned, before[t])] + norths[:3]
                before[t] = turned
                for j in range(4):
                    p_e, q_e, _, _, rate = coefs[j]
                    cell = cells[j]
                    flux = p_e * cell - q_e * pltpu.roll(cell, 127, 1)
                    div = (pltpu.roll(flux, 1, 1) - flux) + (souths[j] - norths[j])
                    div = div + moved_s[4 * q + j, t]
                    if q == 0 and j == 0:
                        div = div + jnp.where(sub == 0, d_ns[0, pl.ds(t * 16 + k, 1), :], 0.0)
                    if q == 3 and j == 3:
                        div = div + jnp.where(sub == 7, d_ns[1, pl.ds(t * 16 + k, 1), :], 0.0)
                    out_s[(t, k, *row_set(32 * q + j))] = cell + rate * div

    def group_body(group, carry):
        for copy in copies(group):
            copy.wait()
        for n in range(per):
            level(group * per + n)
        out_copy(group).start()
        return carry

    lax.fori_loop(0, GROUPS, group_body, 0)
    for group in range(GROUPS):
        out_copy(group).wait()


def kernel_third_call(tracers, fill, mask, east, north, diff, area, d_ew, d_ns):
    hbm = pl.BlockSpec(memory_space=pltpu.HBM)
    vmem = pl.BlockSpec(memory_space=pltpu.VMEM)
    return pl.pallas_call(
        kernel_third,
        name="third",
        out_shape=jax.ShapeDtypeStruct((TR, LV, ROWS, LANES), F32),
        in_specs=[hbm] * 5 + [pl.BlockSpec(memory_space=pltpu.SMEM), hbm, vmem, vmem],
        out_specs=hbm,
        scratch_shapes=[
            pltpu.VMEM((TR, LV, ROWS, LANES), F32),
            pltpu.VMEM((LV, ROWS, LANES), F32),
            pltpu.VMEM((LV, ROWS, LANES), jnp.int32),
            pltpu.VMEM((LV, ROWS, LANES), F32),
            pltpu.VMEM((LV, ROWS, LANES), F32),
            pltpu.VMEM((ROWS, LANES), F32),
            pltpu.VMEM((TR, LV, ROWS, LANES), F32),
            pltpu.VMEM((16, TR, 8, 128), F32),
            pltpu.SemaphoreType.DMA((5, GROUPS)),
            pltpu.SemaphoreType.DMA,
            pltpu.SemaphoreType.DMA((GROUPS,)),
        ],
        compiler_params=pltpu.CompilerParams(vmem_limit_bytes=24 * MIB),
        cost_estimate=pl.CostEstimate(flops=60_000_000, bytes_accessed=12 * MIB, transcendentals=0),
    )(tracers, fill, mask, east, north, diff, area, d_ew, d_ns)


SPLITS = 4


def kernel_last(got, two, four):
    for m in range(32 // SPLITS):
        for n in range(CHUNKS):
            value = got[pl.ds(m * 8 * CHUNKS + n, 8, stride=CHUNKS), :]
            if n < 16:
                two[pl.ds(m * 8, 8), pl.ds(n * 128, 128)] = value
            else:
                four[pl.ds(m * 8, 8), pl.ds((n - 16) * 128, 128)] = value


def kernel_last_call(got):
    return pl.pallas_call(
        kernel_last,
        name="last",
        grid=(SPLITS,),
        out_shape=(
            jax.ShapeDtypeStruct((DEV * CAP, 2048), F32),
            jax.ShapeDtypeStruct((DEV * CAP, 512), F32),
        ),
        in_specs=[pl.BlockSpec((DEV * 40 // SPLITS, 128), lambda s: (s, 0))],
        out_specs=(
            pl.BlockSpec((DEV * CAP // SPLITS, 2048), lambda s: (s, 0)),
            pl.BlockSpec((DEV * CAP // SPLITS, 512), lambda s: (s, 0)),
        ),
        compiler_params=pltpu.CompilerParams(vmem_limit_bytes=8 * MIB),
    )(got)


def local(
    tracers, fill_fraction, ocean_mask, east_speed, north_speed, diffusivity, cell_area, owner_map
):
    lon_count = lax.axis_size("lon")
    lat_count = lax.axis_size("lat")
    *in_hbm, diffusivity, area_hbm, owners = (
        pltpu.with_memory_space_constraint(x, pltpu.HBM)
        for x in (
            tracers, fill_fraction, ocean_mask, east_speed, north_speed, diffusivity, cell_area,
            owner_map.reshape(1, DEV),
        )
    )
    ns_one, ns_two, placing, pool = kernel_rows_call(
        in_hbm[0], in_hbm[1], in_hbm[2], in_hbm[4], owners
    )
    both = ("lon", "lat")

    def swapped(pairs):
        return [pair for a, b in pairs for pair in ((a, b), (b, a))]

    def at(lon, lat):
        return lon * lat_count + lat

    lons = range(lon_count)
    step_one = [(at(n, a), at(n, a + 1)) for n in lons for a in range(0, lat_count, 2)]
    step_two = [(at(n, a), at(n, a + 1)) for n in lons for a in range(1, lat_count - 1, 2)]
    fold = [
        (at(n, lat_count - 1), at(lon_count - 1 - n, lat_count - 1)) for n in range(lon_count // 2)
    ]
    got_one = lax.ppermute(ns_one, both, swapped(step_one))
    got_two = lax.ppermute(ns_two, both, swapped(step_two + fold))
    h_v, ew = kernel_edges_call(tracers, fill_fraction, ocean_mask, east_speed)
    ew_one = lax.ppermute(ew, "lon", swapped([(n, n + 1) for n in range(0, lon_count, 2)]))
    ew_two = lax.ppermute(
        ew, "lon", swapped([(n, (n + 1) % lon_count) for n in range(1, lon_count, 2)])
    )
    num2, den2 = kernel_first_call(
        tracers, h_v, east_speed, north_speed, cell_area, diffusivity, pool
    )
    send, d_ew, d_ns = kernel_second_call(
        num2, den2, ew, ew_one, ew_two, ns_one, ns_two, got_one, got_two, diffusivity, placing
    )
    got = lax.all_to_all(
        send.reshape(DEV, CAP * CHUNKS, 128), both, split_axis=0, concat_axis=0, tiled=True
    )
    updated = kernel_third_call(*in_hbm, diffusivity, area_hbm, d_ew, d_ns)
    two, four = kernel_last_call(got.reshape(DEV * CAP * CHUNKS, 128))
    return (updated, two[None], four[None])


def solution(mesh):
    in_specs = (
        P(None, None, "lat", "lon"),
        P(None, "lat", "lon"),
        P(None, "lat", "lon"),
        P(None, "lat", "lon"),
        P(None, "lat", "lon"),
        P(),
        P("lat", "lon"),
        P(("lon", "lat"), None),
    )
    out_specs = (
        P(None, None, "lat", "lon"),
        P(("lon", "lat"), None, None),
        P(("lon", "lat"), None, None),
    )
    return jax.shard_map(
        local,
        mesh=mesh, in_specs=in_specs, out_specs=out_specs, check_vma=False,
    )
```

```python
import jax
import jax.numpy as jnp
from jax import lax
from jax.experimental import pallas as pl
from jax.experimental.pallas import tpu as pltpu
from jax.sharding import PartitionSpec as P


time_step = 0.05
depth_floor = 0.25
weight_floor = 0.25

TR, LV = 4, 16
ROWS, LANES = 128, 128
GROUPS = 16
DEV, CAP = 128, 2
CHUNKS = 20
PARTS = 2
EACH = 16
PAIR = 2
STEP = 8
F32, BF16 = jnp.float32, jnp.bfloat16
MIB = 1 << 20


def lane_iota(shape=(8, 128)):
    return lax.broadcasted_iota(jnp.int32, shape, len(shape) - 1)


def sub_iota(shape=(8, 128)):
    return lax.broadcasted_iota(jnp.int32, shape, len(shape) - 2)


def face(lower_h, upper_h, lower_speed, upper_speed, mixing, keep=None):
    open_depth = jnp.minimum(lower_h, upper_h)
    if keep is not None:
        open_depth = jnp.where(keep, open_depth, 0.0)
    speed = 0.5 * (lower_speed + upper_speed)
    ahead = jnp.maximum(speed, 0.0)
    back = ahead - speed
    return open_depth * (ahead + mixing), open_depth * (back + mixing)


def half_face(lower_half, upper_half, lower_speed, upper_speed, twice_mixing, keep=None):
    open_half = jnp.minimum(lower_half, upper_half)
    if keep is not None:
        open_half = jnp.where(keep, open_half, 0.0)
    speeds = lower_speed + upper_speed
    ahead = jnp.maximum(speeds, 0.0)
    back = ahead - speeds
    return open_half * (ahead + twice_mixing), open_half * (back + twice_mixing)


def depth_gain(h):
    return time_step * jnp.minimum(h * (1.0 / depth_floor), 1.0)


def halves(values):
    high = values.astype(BF16)
    return high, (values - high.astype(F32)).astype(BF16)


def split_dot(left, right):
    high, low = halves(left)
    return jnp.dot(high, right, preferred_element_type=F32) + jnp.dot(
        low, right, preferred_element_type=F32
    )


def input_copies(hbm, vmem, sems):
    per = LV // GROUPS

    def copies(group):
        levels = pl.ds(group * per, per)
        out = [pltpu.make_async_copy(hbm[0].at[:, levels], vmem[0].at[:, levels], sems.at[0, group])]
        for n in range(1, 5):
            out.append(
                pltpu.make_async_copy(hbm[n].at[levels], vmem[n].at[levels], sems.at[n, group])
            )
        return out

    return copies


def row_set(start):
    return (pl.ds(start, 8, stride=4), slice(None))


def kernel_rows(
    tr, fill, mask, north, owner,
    ns_one, ns_two, placing, pool, shares,
    tr_s, fill_s, mask_s, north_s, owner_s, sems, owner_sem,
):
    copies = []
    for n, (src, dst) in enumerate(((tr, tr_s), (fill, fill_s), (mask, mask_s), (north, north_s))):
        for side in range(2):
            rows = pl.ds(side * (ROWS - 8), 8)
            if n == 0:
                copies.append(
                    pltpu.make_async_copy(src.at[:, :, rows], dst.at[side], sems.at[n, side])
                )
            else:
                copies.append(
                    pltpu.make_async_copy(src.at[:, rows], dst.at[side], sems.at[n, side])
                )
            copies[-1].start()
    owner_copy = pltpu.make_async_copy(owner, owner_s, owner_sem)
    owner_copy.start()
    source = sub_iota((256, 128))
    match = lane_iota((256, 128)) == (source >> 7) * 64 + ((source & 127) >> 1)
    for term in range(2):
        pool[pl.ds(256 * term, 256), :] = jnp.where(match, 1.0, 0.0).astype(BF16)
    source, target = sub_iota((128, 128)), lane_iota((128, 128))
    for n in range(6):
        place = n * 64 + (source >> 1) if n < 2 else (n - 2) * 32 + ((source & 63) >> 1)
        shares[n] = jnp.where(target == place, 1.0, 0.0).astype(BF16)
    across = lane_iota((DEV, DEV))
    down = sub_iota((DEV, DEV))
    owner_copy.wait()
    who_row = owner_s[...]
    who = jnp.sum(jnp.where(down == across, who_row, 0), axis=1, keepdims=True)
    same = jnp.where((who == who_row) & (down < across), 1, 0)
    rank = jnp.sum(same, axis=0, keepdims=True)
    row_of = who_row * CAP + rank
    for part in range(CAP):
        here = jnp.where(down + part * DEV == row_of, 1.0, 0.0).astype(BF16)
        placing[pl.ds(part * DEV, DEV), 0:DEV] = here
        placing[pl.ds(part * DEV, DEV), DEV : 2 * DEV] = here
    for copy in copies:
        copy.wait()
    odd = lax.axis_index("lat") % 2 == 1
    for n in range(6):
        for half in range(2):
            levels = range(8 * half, 8 * half + 8)
            lines = []
            for side in range(2):
                row = 7 * side
                pick = lambda ref, k: ref[side, k, pl.ds(row, 1), :]
                if n < TR:
                    parts = [tr_s[side, n, k, pl.ds(row, 1), :] for k in levels]
                elif n == TR:
                    parts = [pick(fill_s, k) * pick(mask_s, k).astype(F32) for k in levels]
                else:
                    parts = [pick(north_s, k) for k in levels]
                lines.append(jnp.concatenate(parts, axis=0))
            at = pl.ds(n * 16 + 8 * half, 8)
            ns_one[at, :] = jnp.where(odd, lines[0], lines[1])
            ns_two[at, :] = jnp.where(odd, lines[1], lines[0])


def kernel_rows_call(tracers, fill, mask, north, owner):
    hbm = pl.BlockSpec(memory_space=pltpu.HBM)
    vmem = pl.BlockSpec(memory_space=pltpu.VMEM)
    return pl.pallas_call(
        kernel_rows,
        name="rows",
        out_shape=(
            jax.ShapeDtypeStruct((96, 128), F32),
            jax.ShapeDtypeStruct((96, 128), F32),
            jax.ShapeDtypeStruct((CAP * DEV, 2 * DEV), BF16),
            jax.ShapeDtypeStruct((512, 128), BF16),
            jax.ShapeDtypeStruct((6, 128, 128), BF16),
        ),
        in_specs=[hbm] * 5,
        out_specs=(vmem,) * 5,
        scratch_shapes=[
            pltpu.VMEM((2, TR, LV, 8, LANES), F32),
            pltpu.VMEM((2, LV, 8, LANES), F32),
            pltpu.VMEM((2, LV, 8, LANES), jnp.int32),
            pltpu.VMEM((2, LV, 8, LANES), F32),
            pltpu.VMEM((1, DEV), jnp.int32),
            pltpu.SemaphoreType.DMA((4, 2)),
            pltpu.SemaphoreType.DMA,
        ],
        compiler_params=pltpu.CompilerParams(vmem_limit_bytes=4 * MIB),
        cost_estimate=pl.CostEstimate(flops=1_000_000, bytes_accessed=MIB, transcendentals=0),
    )(tracers, fill, mask, north, owner)


def kernel_edges(tr_v, fill_v, mask_v, east_v, h_v, ew):
    lane = lane_iota()

    def level(k, carry):
        where_t = [(lane >> 1) == t * 16 + k for t in range(TR)]

        for v in range(16):
            at = row_set(32 * (v // 4) + v % 4)
            h = 0.5 * (fill_v[(k, *at)] * mask_v[(k, *at)].astype(F32))
            h_v[k, v] = h
            base = 64 * (v % 2)
            packed = ew[16 + v // 2]
            packed = jnp.where(
                (lane >> 1) == k + base // 2, pltpu.roll(h, 2 * k + 1 + base, 1), packed
            )
            ew[16 + v // 2] = jnp.where(
                (lane >> 1) == k + 16 + base // 2,
                pltpu.roll(east_v[(k, *at)], 2 * k + 33 + base, 1),
                packed,
            )
            packed = ew[v]
            for t in range(TR):
                moved = pltpu.roll(tr_v[(t, k, *at)], 2 * k + 32 * t + 1, 1)
                packed = jnp.where(where_t[t], moved, packed)
            ew[v] = packed
        return carry

    def step(n, carry):
        for m in range(STEP):
            level(n * STEP + m, carry)
        return carry

    lax.fori_loop(0, LV // STEP, step, 0)


def kernel_edges_call(tracers, fill, mask, east):
    vmem = pl.BlockSpec(memory_space=pltpu.VMEM)
    return pl.pallas_call(
        kernel_edges,
        name="edges",
        out_shape=(
            jax.ShapeDtypeStruct((LV, 16, 8, LANES), F32),
            jax.ShapeDtypeStruct((24, 8, 128), F32),
        ),
        in_specs=[vmem] * 4,
        out_specs=(vmem,) * 2,
        compiler_params=pltpu.CompilerParams(vmem_limit_bytes=16 * MIB),
        cost_estimate=pl.CostEstimate(flops=60_000_000, bytes_accessed=11 * MIB, transcendentals=0),
    )(tracers, fill, mask, east)


def kernel_first(
    tr_s, h_v, east_s, north_s, area_v, diff, pool,
    num2, den2,
    area_s, gains, all_faces, coefs, stores,
):
    lane, sub = lane_iota(), sub_iota()
    is_even = (lane & 1) == 0
    not_last, not_top = lane < 127, sub < 7
    swap = jnp.where(is_even, lane + 127, lane + 1) & 127
    for v in range(16):
        area_s[v] = 2.0 * area_v[row_set(32 * (v // 4) + v % 4)]

    def level(k, n):
        twice_mixing = 2.0 * diff[k]
        g_s, face_s, coef, store = gains.at[n], all_faces.at[n], coefs.at[n], stores.at[n]

        for v in range(16):
            h, u = h_v[k, v], east_s[(k, *row_set(32 * (v // 4) + v % 4))]
            p_e, q_e = half_face(
                h, pltpu.roll(h, 127, 1), u, pltpu.roll(u, 127, 1), twice_mixing, keep=not_last
            )
            g_s[v] = depth_gain(2.0 * h)
            face_s[0, v] = p_e
            face_s[1, v] = q_e

        for v in range(16):
            start = 32 * (v // 4) + v % 4
            h, speed = h_v[k, v], north_s[(k, *row_set(start))]
            keep = None
            if v == 15:
                h_up, keep = pltpu.roll(h_v[k, 12], 7, 0), not_top
                speed_up = pltpu.roll(north_s[(k, *row_set(96))], 7, 0)
            else:
                speed_up = north_s[(k, *row_set(start + 1))]
                if v % 4 < 3:
                    h_up = h_v[k, v + 1]
                else:
                    h_up = jnp.where(
                        not_top, pltpu.roll(h_v[k, v - 3], 7, 0), pltpu.roll(h_v[k, v + 1], 7, 0)
                    )
            p_n, q_n = half_face(h, h_up, speed, speed_up, twice_mixing, keep)
            face_s[2, v] = p_n
            face_s[3, v] = q_n

        for q in range(4):
            south = []
            for n in (2, 3):
                low = pltpu.roll(face_s[n, 4 * q + 3], 1, 0)
                under = pltpu.roll(face_s[n, 4 * q - 1], 1, 0) if q else 0.0
                south.append(jnp.where(sub > 0, low, under))
            for par in range(2):
                centre, weight = [], 0.0
                for n in range(2):
                    v = 4 * q + 2 * par + n
                    h, g = h_v[k, v], g_s[v]
                    w = area_s[v] * h
                    p_e, q_w = face_s[0, v], pltpu.roll(face_s[1, v], 1, 1)
                    p_n, q_n = face_s[2, v], face_s[3, v]
                    p_s, q_s = south if v % 4 == 0 else (
                        face_s[2, v - 1], face_s[3, v - 1]
                    )
                    to_west = pltpu.roll(g, 1, 1) * q_w
                    to_east = pltpu.roll(g, 127, 1) * p_e
                    own = w - g * ((p_e + q_w) + (p_n + q_s))
                    centre.append(own + jnp.where(is_even, to_east, to_west))
                    coef[4 + n, 2 * q + par] = jnp.where(is_even, to_west, to_east)
                    if n == 0:
                        low, up = g * p_s, g * q_n
                    else:
                        down, high = g * p_s, g * q_n
                    weight = weight + w
                coef[0, 2 * q + par] = low
                coef[1, 2 * q + par] = centre[0] + down
                coef[2, 2 * q + par] = centre[1] + up
                coef[3, 2 * q + par] = high
                store[pl.ds(128 + q * 8, 8), pl.ds(par * 128, 128)] = weight

        for q in range(4):
            for par in range(2):
                low_c, a_c, b_c, high_c, a_x, b_x = [coef[n, 2 * q + par] for n in range(6)]
                for t in range(TR):
                    cell = lambda start: tr_s[(t, k, *row_set(start))]
                    start = 32 * q + 2 * par
                    a, b = cell(start), cell(start + 1)
                    low = cell(start - 1) if start else pltpu.roll(cell(3), 1, 0)
                    high = cell(start + 2) if start < 98 else pltpu.roll(cell(96), 7, 0)
                    side = a_x * a + b_x * b
                    value = (a_c * a + b_c * b) + (low_c * low + high_c * high)
                    value = value + jnp.take_along_axis(side, swap, axis=1)
                    store[pl.ds(t * 32 + q * 8, 8), pl.ds(par * 128, 128)] = value

    def pooled(k, n):
        both = jnp.concatenate(halves(stores[n]), axis=1)
        values = jnp.dot(both, pool[...], preferred_element_type=F32)
        rows = pl.ds(pl.multiple_of(k * 32, 32), 32)
        for t in range(TR):
            num2[t, rows, :] = values[t * 32 : t * 32 + 32]
        den2[rows, :] = values[128:160]

    def group_body(k, carry):
        for n in range(PAIR):
            pooled((k * PAIR + n + LV - PAIR) % LV, n)
        for n in range(PAIR):
            level(k * PAIR + n, n)
        return carry

    stores[...] = jnp.zeros_like(stores)
    lax.fori_loop(0, LV // PAIR, group_body, 0)
    for n in range(PAIR):
        pooled(LV - PAIR + n, n)


def kernel_first_call(tr_v, h_v, east_v, north_v, area_v, diff, pool):
    vmem = pl.BlockSpec(memory_space=pltpu.VMEM)
    return pl.pallas_call(
        kernel_first,
        name="first",
        out_shape=(
            jax.ShapeDtypeStruct((TR, 512, 128), F32),
            jax.ShapeDtypeStruct((512, 128), F32),
        ),
        in_specs=[vmem] * 5 + [pl.BlockSpec(memory_space=pltpu.SMEM), vmem],
        out_specs=(vmem,) * 2,
        scratch_shapes=[
            pltpu.VMEM((16, 8, 128), F32),
            pltpu.VMEM((PAIR, 16, 8, 128), F32),
            pltpu.VMEM((PAIR, 4, 16, 8, 128), F32),
            pltpu.VMEM((PAIR, 6, 8, 8, 128), F32),
            pltpu.VMEM((PAIR, 160, 256), F32),
        ],
        compiler_params=pltpu.CompilerParams(vmem_limit_bytes=16 * MIB),
        cost_estimate=pl.CostEstimate(flops=60_000_000, bytes_accessed=11 * MIB, transcendentals=0),
    )(tr_v, h_v, east_v, north_v, area_v, diff, pool)


def spread(values, offset):
    index = (lane_iota() & 31) + offset
    return jnp.take_along_axis(values, index, axis=1)


def kernel_second(
    num2, den2, ew, ew_one, ew_two, ns_one, ns_two, got_one, got_two, diff, placing, shares,
    send, d_ew, d_ns,
    work, acc, chunks, send_s, sems,
):
    lane, sub = lane_iota(), sub_iota()
    odd = lax.axis_index("lat") % 2 == 1
    odd_lon = lax.axis_index("lon") % 2 == 1
    at_fold = lax.axis_index("lat") == lax.axis_size("lat") - 1
    is_east = (lane & 1) == 0
    level_of = (lane >> 1) & 15
    mixing = jnp.zeros((8, 128), F32)
    for k in range(LV):
        mixing = jnp.where(level_of == k, 2.0 * diff[k], mixing)

    def neighbour(n):
        one, two = ew_one[n], ew_two[n]
        from_east, from_west = jnp.where(odd_lon, two, one), jnp.where(odd_lon, one, two)
        return jnp.where(is_east, pltpu.roll(from_east, 127, 1), pltpu.roll(from_west, 1, 1))

    pending = None
    for v in range(16):
        own_hu, near_hu = ew[16 + v // 2], neighbour(16 + v // 2)
        base = 64 * (v % 2)
        h = spread(own_hu, base)
        p, q = half_face(
            h, spread(near_hu, base), spread(own_hu, base + 32), spread(near_hu, base + 32), mixing
        )
        div = jnp.where(is_east, q, p) * neighbour(v) - jnp.where(is_east, p, q) * ew[v]
        d_ew[v] = div
        value = depth_gain(2.0 * h) * div
        if v % 2 == 0:
            pending = value
        else:
            value = pending + value
            far_value = pltpu.roll(value, 64, 1)
            q, par = v // 4, (v // 2) % 2
            plain = jnp.where(is_east, value, far_value)
            moved = jnp.where(is_east, far_value, value)
            if par == 0:
                lower = plain, moved
            else:
                for half in range(2):
                    first_lanes = (lane < 64) == is_east
                    mine = first_lanes if half == 0 else ~first_lanes
                    work[half, q] = jnp.where(mine, lower[0], moved)

    ends = ((lane & 63) == 0) | ((lane & 63) == 63)

    def add_ends(step, carry):
        for n in range(EACH):
            k = step * EACH + n
            for t in range(TR):
                for q in range(4):
                    rows = pl.ds(pl.multiple_of(k * 32 + q * 8, 8), 8)
                    moved = pltpu.roll(work[t // 2, q], 63 - 2 * k + (128 - 32 * t), 1)
                    acc[t, rows, :] = num2[t, rows, :] + jnp.where(ends, moved, 0.0)
        return carry

    lax.fori_loop(0, LV // EACH, add_ends, 0)

    pools = [shares[par] for par in range(2)]
    quarter = [shares[2 + j] for j in range(4)]

    back = 127 - lane
    for half in range(2):
        mix = jnp.zeros((8, 128), F32)
        for k in range(8):
            mix = jnp.where(sub == k, diff[8 * half + k], mix)

        def rows_of(ref, n):
            return ref[pl.ds(n * 16 + 8 * half, 8), :]

        def own(n, top):
            pair = (ns_two, ns_one) if top else (ns_one, ns_two)
            return jnp.where(odd, rows_of(pair[0], n), rows_of(pair[1], n))

        def near(n, top, sign=1.0):
            if not top:
                return jnp.where(odd, rows_of(got_one, n), rows_of(got_two, n))
            value = jnp.where(odd, rows_of(got_two, n), rows_of(got_one, n))
            turned = sign * jnp.take_along_axis(value, back, axis=1)
            return jnp.where(at_fold, turned, value)

        for top in (False, True):
            h = own(4, top)
            p, q = face(h, near(4, top), own(5, top), near(5, top, -1.0), mix)
            gain = depth_gain(h)
            for t in range(TR):
                if top:
                    div = q * near(t, top) - p * own(t, top)
                else:
                    div = p * near(t, top) - q * own(t, top)
                d_ns[int(top), pl.ds(t * 16 + 8 * half, 8), :] = div
                at = (t, pl.ds(256 * half + 31 * int(top), 8, stride=32), slice(None))
                acc[at] = acc[at] + split_dot(gain * div, pools[int(top)])

    def keep(n, values):
        high, low = halves(values)
        chunks[0:128, pl.ds(n * 128, 128)] = high
        chunks[128:256, pl.ds(n * 128, 128)] = low

    def every_fourth(ref, *lead, j):
        return jnp.concatenate(
            [ref[(*lead, pl.ds(32 * m + j, 8, stride=4), slice(None))] for m in range(16)], axis=0
        )

    gains = []
    den4 = jnp.zeros((128, 128), F32)
    for j in range(4):
        den = every_fourth(den2, j=j)
        gains.append(1.0 / jnp.maximum(den, weight_floor))
        den4 = den4 + split_dot(den, quarter[j])
    gain4 = 1.0 / jnp.maximum(den4, weight_floor)
    for t in range(TR):
        num4 = jnp.zeros((128, 128), F32)
        for j in range(4):
            num = every_fourth(acc, t, j=j)
            keep(t * 4 + j, num * gains[j])
            num4 = num4 + split_dot(num, quarter[j])
        keep(16 + t, num4 * gain4)

    each = CAP * DEV // PARTS
    copies = []
    for part in range(PARTS):
        left = placing[pl.ds(part * each, each), :]
        for n in range(CHUNKS // 2):
            placed = jnp.dot(left, chunks[:, pl.ds(n * 256, 256)], preferred_element_type=F32)
            for c in range(2):
                for m in range(each // 8):
                    start = (part * each + m * 8) * CHUNKS + 2 * n + c
                    send_s[pl.ds(start, 8, stride=CHUNKS), :] = placed[
                        m * 8 : m * 8 + 8, c * 128 : c * 128 + 128
                    ]
        rows = pl.ds(part * each * CHUNKS, each * CHUNKS)
        copies.append(pltpu.make_async_copy(send_s.at[rows], send.at[rows], sems.at[part]))
        copies[-1].start()
    for copy in copies:
        copy.wait()


def kernel_second_call(*args):
    vmem = pl.BlockSpec(memory_space=pltpu.VMEM)
    return pl.pallas_call(
        kernel_second,
        name="second",
        out_shape=(
            pltpu.HBM((DEV * CAP * CHUNKS, 128), F32),
            jax.ShapeDtypeStruct((16, 8, 128), F32),
            jax.ShapeDtypeStruct((2, 64, 128), F32),
        ),
        in_specs=[vmem] * 9 + [pl.BlockSpec(memory_space=pltpu.SMEM), vmem, vmem],
        out_specs=(pl.BlockSpec(memory_space=pltpu.HBM), vmem, vmem),
        scratch_shapes=[
            pltpu.VMEM((2, 4, 8, 128), F32),
            pltpu.VMEM((TR, 512, 128), F32),
            pltpu.VMEM((256, 2560), BF16),
            pltpu.VMEM((DEV * CAP * CHUNKS, 128), F32),
            pltpu.SemaphoreType.DMA((PARTS,)),
        ],
        compiler_params=pltpu.CompilerParams(vmem_limit_bytes=16 * MIB),
        cost_estimate=pl.CostEstimate(flops=60_000_000, bytes_accessed=6 * MIB, transcendentals=0),
    )(*args)


def kernel_third(
    tr, fill, mask, east, north, diff, area, d_ew, d_ns,
    out,
    tr_s, fill_s, mask_s, east_s, north_s, area_s, out_s, moved_s, sems, area_sem, out_sems,
):
    hbm, vmem = (tr, fill, mask, east, north), (tr_s, fill_s, mask_s, east_s, north_s)
    copies = input_copies(hbm, vmem, sems)
    area_copy = pltpu.make_async_copy(area, area_s, area_sem)
    for group in range(GROUPS):
        for copy in copies(group):
            copy.start()
        if group == 0:
            area_copy.start()
    area_copy.wait()
    lane, sub = lane_iota(), sub_iota()
    ends = (lane == 0) | (lane == 127)
    not_last, not_top = lane < 127, sub < 7
    per = LV // GROUPS

    def out_copy(group):
        levels = pl.ds(group * per, per)
        return pltpu.make_async_copy(out_s.at[:, levels], out.at[:, levels], out_sems.at[group])

    def level(k):
        mixing = diff[k]

        def load(ref, start):
            return ref[(k, *row_set(start))]

        def depth(start):
            return load(fill_s, start) * load(mask_s, start).astype(F32)

        for v in range(16):
            edge = d_ew[v]
            for t in range(TR):
                moved = pltpu.roll(edge, 127 - 2 * k + (128 - 32 * t), 1)
                moved_s[v, t] = jnp.where(ends, moved, 0.0)

        before = [jnp.zeros((8, 128), F32)] * TR
        for q in range(4):
            hs = [depth(32 * q + j) for j in range(4)]
            vs = [load(north_s, 32 * q + j) for j in range(4)]
            if q < 3:
                hs.append(depth(32 * q + 4))
                vs.append(load(north_s, 32 * q + 4))
            else:
                hs.append(pltpu.roll(hs[0], 7, 0))
                vs.append(pltpu.roll(vs[0], 7, 0))
            coefs = []
            for j in range(4):
                top = q == 3 and j == 3
                h, u = hs[j], load(east_s, 32 * q + j)
                rate = time_step / (area_s[row_set(32 * q + j)] * jnp.maximum(h, depth_floor))
                coefs.append(
                    face(h, pltpu.roll(h, 127, 1), u, pltpu.roll(u, 127, 1), mixing, keep=not_last)
                    + face(h, hs[j + 1], vs[j], vs[j + 1], mixing, keep=not_top if top else None)
                    + (rate,)
                )
            for t in range(TR):
                cells = [tr_s[(t, k, *row_set(32 * q + j))] for j in range(4)]
                if q < 3:
                    cells.append(tr_s[(t, k, *row_set(32 * q + 4))])
                else:
                    cells.append(pltpu.roll(cells[0], 7, 0))
                norths = [coefs[j][2] * cells[j] - coefs[j][3] * cells[j + 1] for j in range(4)]
                turned = pltpu.roll(norths[3], 1, 0)
                souths = [jnp.where(sub > 0, turned, before[t])] + norths[:3]
                before[t] = turned
                for j in range(4):
                    p_e, q_e, _, _, rate = coefs[j]
                    cell = cells[j]
                    flux = p_e * cell - q_e * pltpu.roll(cell, 127, 1)
                    div = (pltpu.roll(flux, 1, 1) - flux) + (souths[j] - norths[j])
                    div = div + moved_s[4 * q + j, t]
                    if q == 0 and j == 0:
                        div = div + jnp.where(sub == 0, d_ns[0, pl.ds(t * 16 + k, 1), :], 0.0)
                    if q == 3 and j == 3:
                        div = div + jnp.where(sub == 7, d_ns[1, pl.ds(t * 16 + k, 1), :], 0.0)
                    out_s[(t, k, *row_set(32 * q + j))] = cell + rate * div

    def group_body(group, carry):
        for copy in copies(group):
            copy.wait()
        for n in range(per):
            level(group * per + n)
        out_copy(group).start()
        return carry

    lax.fori_loop(0, GROUPS, group_body, 0)
    for group in range(GROUPS):
        out_copy(group).wait()


def kernel_third_call(tracers, fill, mask, east, north, diff, area, d_ew, d_ns):
    hbm = pl.BlockSpec(memory_space=pltpu.HBM)
    vmem = pl.BlockSpec(memory_space=pltpu.VMEM)
    return pl.pallas_call(
        kernel_third,
        name="third",
        out_shape=jax.ShapeDtypeStruct((TR, LV, ROWS, LANES), F32),
        in_specs=[hbm] * 5 + [pl.BlockSpec(memory_space=pltpu.SMEM), hbm, vmem, vmem],
        out_specs=hbm,
        scratch_shapes=[
            pltpu.VMEM((TR, LV, ROWS, LANES), F32),
            pltpu.VMEM((LV, ROWS, LANES), F32),
            pltpu.VMEM((LV, ROWS, LANES), jnp.int32),
            pltpu.VMEM((LV, ROWS, LANES), F32),
            pltpu.VMEM((LV, ROWS, LANES), F32),
            pltpu.VMEM((ROWS, LANES), F32),
            pltpu.VMEM((TR, LV, ROWS, LANES), F32),
            pltpu.VMEM((16, TR, 8, 128), F32),
            pltpu.SemaphoreType.DMA((5, GROUPS)),
            pltpu.SemaphoreType.DMA,
            pltpu.SemaphoreType.DMA((GROUPS,)),
        ],
        compiler_params=pltpu.CompilerParams(vmem_limit_bytes=24 * MIB),
        cost_estimate=pl.CostEstimate(flops=60_000_000, bytes_accessed=12 * MIB, transcendentals=0),
    )(tracers, fill, mask, east, north, diff, area, d_ew, d_ns)


SPLITS = 4


def kernel_last(got, two, four, two_s, four_s, sems):
    each = DEV * CAP // SPLITS
    copies = []
    for part in range(SPLITS):
        for m in range(part * each // 8, (part + 1) * each // 8):
            for n in range(CHUNKS):
                value = got[pl.ds(m * 8 * CHUNKS + n, 8, stride=CHUNKS), :]
                if n < 16:
                    two_s[pl.ds(m * 8, 8), pl.ds(n * 128, 128)] = value
                else:
                    four_s[pl.ds(m * 8, 8), pl.ds((n - 16) * 128, 128)] = value
        rows = pl.ds(part * each, each)
        for n, (src, dst) in enumerate(((two_s, two), (four_s, four))):
            copies.append(pltpu.make_async_copy(src.at[rows], dst.at[rows], sems.at[n, part]))
            copies[-1].start()
    for copy in copies:
        copy.wait()


def kernel_last_call(got):
    hbm = pl.BlockSpec(memory_space=pltpu.HBM)
    return pl.pallas_call(
        kernel_last,
        name="last",
        out_shape=(pltpu.HBM((DEV * CAP, 2048), F32), pltpu.HBM((DEV * CAP, 512), F32)),
        in_specs=[pl.BlockSpec(memory_space=pltpu.VMEM)],
        out_specs=(hbm, hbm),
        scratch_shapes=[
            pltpu.VMEM((DEV * CAP, 2048), F32),
            pltpu.VMEM((DEV * CAP, 512), F32),
            pltpu.SemaphoreType.DMA((2, SPLITS)),
        ],
        compiler_params=pltpu.CompilerParams(vmem_limit_bytes=8 * MIB),
    )(got)


def local(
    tracers, fill_fraction, ocean_mask, east_speed, north_speed, diffusivity, cell_area, owner_map
):
    lon_count = lax.axis_size("lon")
    lat_count = lax.axis_size("lat")
    *in_hbm, diffusivity, area_hbm, owners = (
        pltpu.with_memory_space_constraint(x, pltpu.HBM)
        for x in (
            tracers, fill_fraction, ocean_mask, east_speed, north_speed, diffusivity, cell_area,
            owner_map.reshape(1, DEV),
        )
    )
    ns_one, ns_two, placing, pool, shares = kernel_rows_call(
        in_hbm[0], in_hbm[1], in_hbm[2], in_hbm[4], owners
    )
    both = ("lon", "lat")

    def swapped(pairs):
        return [pair for a, b in pairs for pair in ((a, b), (b, a))]

    def at(lon, lat):
        return lon * lat_count + lat

    lons = range(lon_count)
    step_one = [(at(n, a), at(n, a + 1)) for n in lons for a in range(0, lat_count, 2)]
    step_two = [(at(n, a), at(n, a + 1)) for n in lons for a in range(1, lat_count - 1, 2)]
    fold = [
        (at(n, lat_count - 1), at(lon_count - 1 - n, lat_count - 1)) for n in range(lon_count // 2)
    ]
    got_one = lax.ppermute(ns_one, both, swapped(step_one))
    got_two = lax.ppermute(ns_two, both, swapped(step_two + fold))
    h_v, ew = kernel_edges_call(tracers, fill_fraction, ocean_mask, east_speed)
    ew_one = lax.ppermute(ew, "lon", swapped([(n, n + 1) for n in range(0, lon_count, 2)]))
    ew_two = lax.ppermute(
        ew, "lon", swapped([(n, (n + 1) % lon_count) for n in range(1, lon_count, 2)])
    )
    num2, den2 = kernel_first_call(
        tracers, h_v, east_speed, north_speed, cell_area, diffusivity, pool
    )
    send, d_ew, d_ns = kernel_second_call(
        num2, den2, ew, ew_one, ew_two, ns_one, ns_two, got_one, got_two, diffusivity, placing,
        shares,
    )
    got = lax.all_to_all(
        send.reshape(DEV, CAP * CHUNKS, 128), both, split_axis=0, concat_axis=0, tiled=True
    )
    updated = kernel_third_call(*in_hbm, diffusivity, area_hbm, d_ew, d_ns)
    two, four = kernel_last_call(got.reshape(DEV * CAP * CHUNKS, 128))
    return (updated, two[None], four[None])


def solution(mesh):
    in_specs = (
        P(None, None, "lat", "lon"),
        P(None, "lat", "lon"),
        P(None, "lat", "lon"),
        P(None, "lat", "lon"),
        P(None, "lat", "lon"),
        P(),
        P("lat", "lon"),
        P(("lon", "lat"), None),
    )
    out_specs = (
        P(None, None, "lat", "lon"),
        P(("lon", "lat"), None, None),
        P(("lon", "lat"), None, None),
    )
    return jax.shard_map(
        local,
        mesh=mesh, in_specs=in_specs, out_specs=out_specs, check_vma=False,
    )
```

```python
import jax
import jax.numpy as jnp
from jax import lax
from jax.experimental import pallas as pl
from jax.experimental.pallas import tpu as pltpu
from jax.sharding import PartitionSpec as P


time_step = 0.05
depth_floor = 0.25
weight_floor = 0.25

TR, LV = 4, 16
ROWS, LANES = 128, 128
GROUPS = 16
DEV, CAP = 128, 2
CHUNKS = 20
PAIR = 2
STEP = 8
F32, BF16 = jnp.float32, jnp.bfloat16
MIB = 1 << 20


def lane_iota(shape=(8, 128)):
    return lax.broadcasted_iota(jnp.int32, shape, len(shape) - 1)


def sub_iota(shape=(8, 128)):
    return lax.broadcasted_iota(jnp.int32, shape, len(shape) - 2)


def face(lower_h, upper_h, lower_speed, upper_speed, mixing, keep=None):
    open_depth = jnp.minimum(lower_h, upper_h)
    if keep is not None:
        open_depth = jnp.where(keep, open_depth, 0.0)
    speed = 0.5 * (lower_speed + upper_speed)
    ahead = jnp.maximum(speed, 0.0)
    back = ahead - speed
    return open_depth * (ahead + mixing), open_depth * (back + mixing)


def half_face(lower_half, upper_half, lower_speed, upper_speed, twice_mixing, keep=None):
    open_half = jnp.minimum(lower_half, upper_half)
    if keep is not None:
        open_half = jnp.where(keep, open_half, 0.0)
    speeds = lower_speed + upper_speed
    ahead = jnp.maximum(speeds, 0.0)
    back = ahead - speeds
    return open_half * (ahead + twice_mixing), open_half * (back + twice_mixing)


def depth_gain(h):
    return time_step * jnp.minimum(h * (1.0 / depth_floor), 1.0)


def halves(values):
    high = values.astype(BF16)
    return high, (values - high.astype(F32)).astype(BF16)


def split_dot(left, right):
    high, low = halves(left)
    return jnp.dot(high, right, preferred_element_type=F32) + jnp.dot(
        low, right, preferred_element_type=F32
    )


def input_copies(hbm, vmem, sems):
    per = LV // GROUPS

    def copies(group):
        levels = pl.ds(group * per, per)
        out = [pltpu.make_async_copy(hbm[0].at[:, levels], vmem[0].at[:, levels], sems.at[0, group])]
        for n in range(1, 5):
            out.append(
                pltpu.make_async_copy(hbm[n].at[levels], vmem[n].at[levels], sems.at[n, group])
            )
        return out

    return copies


def row_set(start):
    return (pl.ds(start, 8, stride=4), slice(None))


def kernel_rows(
    tr, fill, mask, north, owner,
    ns_one, ns_two, placing, pool, shares,
    tr_s, fill_s, mask_s, north_s, owner_s, sems, owner_sem,
):
    copies = []
    for n, (src, dst) in enumerate(((tr, tr_s), (fill, fill_s), (mask, mask_s), (north, north_s))):
        for side in range(2):
            rows = pl.ds(side * (ROWS - 8), 8)
            if n == 0:
                copies.append(
                    pltpu.make_async_copy(src.at[:, :, rows], dst.at[side], sems.at[n, side])
                )
            else:
                copies.append(
                    pltpu.make_async_copy(src.at[:, rows], dst.at[side], sems.at[n, side])
                )
            copies[-1].start()
    owner_copy = pltpu.make_async_copy(owner, owner_s, owner_sem)
    owner_copy.start()
    source = sub_iota((256, 128))
    match = lane_iota((256, 128)) == (source >> 7) * 64 + ((source & 127) >> 1)
    for term in range(2):
        pool[pl.ds(256 * term, 256), :] = jnp.where(match, 1.0, 0.0).astype(BF16)
    source, target = sub_iota((128, 128)), lane_iota((128, 128))
    for n in range(6):
        place = n * 64 + (source >> 1) if n < 2 else (n - 2) * 32 + ((source & 63) >> 1)
        shares[n] = jnp.where(target == place, 1.0, 0.0).astype(BF16)
    across = lane_iota((DEV, DEV))
    down = sub_iota((DEV, DEV))
    owner_copy.wait()
    who_row = owner_s[...]
    who = jnp.sum(jnp.where(down == across, who_row, 0), axis=1, keepdims=True)
    same = jnp.where((who == who_row) & (down < across), 1, 0)
    rank = jnp.sum(same, axis=0, keepdims=True)
    row_of = rank * DEV + who_row
    for part in range(CAP):
        here = jnp.where(down + part * DEV == row_of, 1.0, 0.0).astype(BF16)
        placing[pl.ds(part * DEV, DEV), 0:DEV] = here
        placing[pl.ds(part * DEV, DEV), DEV : 2 * DEV] = here
    for copy in copies:
        copy.wait()
    odd = lax.axis_index("lat") % 2 == 1
    for n in range(6):
        for half in range(2):
            levels = range(8 * half, 8 * half + 8)
            lines = []
            for side in range(2):
                row = 7 * side
                pick = lambda ref, k: ref[side, k, pl.ds(row, 1), :]
                if n < TR:
                    parts = [tr_s[side, n, k, pl.ds(row, 1), :] for k in levels]
                elif n == TR:
                    parts = [pick(fill_s, k) * pick(mask_s, k).astype(F32) for k in levels]
                else:
                    parts = [pick(north_s, k) for k in levels]
                lines.append(jnp.concatenate(parts, axis=0))
            at = pl.ds(n * 16 + 8 * half, 8)
            ns_one[at, :] = jnp.where(odd, lines[0], lines[1])
            ns_two[at, :] = jnp.where(odd, lines[1], lines[0])


def kernel_rows_call(tracers, fill, mask, north, owner):
    hbm = pl.BlockSpec(memory_space=pltpu.HBM)
    vmem = pl.BlockSpec(memory_space=pltpu.VMEM)
    return pl.pallas_call(
        kernel_rows,
        name="rows",
        out_shape=(
            jax.ShapeDtypeStruct((96, 128), F32),
            jax.ShapeDtypeStruct((96, 128), F32),
            jax.ShapeDtypeStruct((CAP * DEV, 2 * DEV), BF16),
            jax.ShapeDtypeStruct((512, 128), BF16),
            jax.ShapeDtypeStruct((6, 128, 128), BF16),
        ),
        in_specs=[hbm] * 5,
        out_specs=(vmem,) * 5,
        scratch_shapes=[
            pltpu.VMEM((2, TR, LV, 8, LANES), F32),
            pltpu.VMEM((2, LV, 8, LANES), F32),
            pltpu.VMEM((2, LV, 8, LANES), jnp.int32),
            pltpu.VMEM((2, LV, 8, LANES), F32),
            pltpu.VMEM((1, DEV), jnp.int32),
            pltpu.SemaphoreType.DMA((4, 2)),
            pltpu.SemaphoreType.DMA,
        ],
        compiler_params=pltpu.CompilerParams(vmem_limit_bytes=4 * MIB),
        cost_estimate=pl.CostEstimate(flops=1_000_000, bytes_accessed=MIB, transcendentals=0),
    )(tracers, fill, mask, north, owner)


def kernel_edges(tr_v, fill_v, mask_v, east_v, h_v, ew):
    lane = lane_iota()

    def level(k, carry):
        where_t = [(lane >> 1) == t * 16 + k for t in range(TR)]

        for v in range(16):
            at = row_set(32 * (v // 4) + v % 4)
            h = 0.5 * (fill_v[(k, *at)] * mask_v[(k, *at)].astype(F32))
            h_v[k, v] = h
            base = 64 * (v % 2)
            packed = ew[16 + v // 2]
            packed = jnp.where(
                (lane >> 1) == k + base // 2, pltpu.roll(h, 2 * k + 1 + base, 1), packed
            )
            ew[16 + v // 2] = jnp.where(
                (lane >> 1) == k + 16 + base // 2,
                pltpu.roll(east_v[(k, *at)], 2 * k + 33 + base, 1),
                packed,
            )
            packed = ew[v]
            for t in range(TR):
                moved = pltpu.roll(tr_v[(t, k, *at)], 2 * k + 32 * t + 1, 1)
                packed = jnp.where(where_t[t], moved, packed)
            ew[v] = packed
        return carry

    def step(n, carry):
        for m in range(STEP):
            level(n * STEP + m, carry)
        return carry

    lax.fori_loop(0, LV // STEP, step, 0)


def kernel_edges_call(tracers, fill, mask, east):
    vmem = pl.BlockSpec(memory_space=pltpu.VMEM)
    return pl.pallas_call(
        kernel_edges,
        name="edges",
        out_shape=(
            jax.ShapeDtypeStruct((LV, 16, 8, LANES), F32),
            jax.ShapeDtypeStruct((24, 8, 128), F32),
        ),
        in_specs=[vmem] * 4,
        out_specs=(vmem,) * 2,
        compiler_params=pltpu.CompilerParams(vmem_limit_bytes=16 * MIB),
        cost_estimate=pl.CostEstimate(flops=60_000_000, bytes_accessed=11 * MIB, transcendentals=0),
    )(tracers, fill, mask, east)


def kernel_first(
    tr_s, h_v, east_s, north_s, area_v, diff, pool,
    num2, den2,
    area_s, gains, all_faces, coefs, stores,
):
    lane, sub = lane_iota(), sub_iota()
    is_even = (lane & 1) == 0
    not_last, not_top = lane < 127, sub < 7
    swap = jnp.where(is_even, lane + 127, lane + 1) & 127
    for v in range(16):
        area_s[v] = 2.0 * area_v[row_set(32 * (v // 4) + v % 4)]

    def level(k, n):
        twice_mixing = 2.0 * diff[k]
        g_s, face_s, coef, store = gains.at[n], all_faces.at[n], coefs.at[n], stores.at[n]

        for v in range(16):
            h, u = h_v[k, v], east_s[(k, *row_set(32 * (v // 4) + v % 4))]
            p_e, q_e = half_face(
                h, pltpu.roll(h, 127, 1), u, pltpu.roll(u, 127, 1), twice_mixing, keep=not_last
            )
            g_s[v] = depth_gain(2.0 * h)
            face_s[0, v] = p_e
            face_s[1, v] = q_e

        for v in range(16):
            start = 32 * (v // 4) + v % 4
            h, speed = h_v[k, v], north_s[(k, *row_set(start))]
            keep = None
            if v == 15:
                h_up, keep = pltpu.roll(h_v[k, 12], 7, 0), not_top
                speed_up = pltpu.roll(north_s[(k, *row_set(96))], 7, 0)
            else:
                speed_up = north_s[(k, *row_set(start + 1))]
                if v % 4 < 3:
                    h_up = h_v[k, v + 1]
                else:
                    h_up = jnp.where(
                        not_top, pltpu.roll(h_v[k, v - 3], 7, 0), pltpu.roll(h_v[k, v + 1], 7, 0)
                    )
            p_n, q_n = half_face(h, h_up, speed, speed_up, twice_mixing, keep)
            face_s[2, v] = p_n
            face_s[3, v] = q_n

        for q in range(4):
            south = []
            for n in (2, 3):
                low = pltpu.roll(face_s[n, 4 * q + 3], 1, 0)
                under = pltpu.roll(face_s[n, 4 * q - 1], 1, 0) if q else 0.0
                south.append(jnp.where(sub > 0, low, under))
            for par in range(2):
                centre, weight = [], 0.0
                for n in range(2):
                    v = 4 * q + 2 * par + n
                    h, g = h_v[k, v], g_s[v]
                    w = area_s[v] * h
                    p_e, q_w = face_s[0, v], pltpu.roll(face_s[1, v], 1, 1)
                    p_n, q_n = face_s[2, v], face_s[3, v]
                    p_s, q_s = south if v % 4 == 0 else (
                        face_s[2, v - 1], face_s[3, v - 1]
                    )
                    to_west = pltpu.roll(g, 1, 1) * q_w
                    to_east = pltpu.roll(g, 127, 1) * p_e
                    own = w - g * ((p_e + q_w) + (p_n + q_s))
                    centre.append(own + jnp.where(is_even, to_east, to_west))
                    coef[4 + n, 2 * q + par] = jnp.where(is_even, to_west, to_east)
                    if n == 0:
                        low, up = g * p_s, g * q_n
                    else:
                        down, high = g * p_s, g * q_n
                    weight = weight + w
                coef[0, 2 * q + par] = low
                coef[1, 2 * q + par] = centre[0] + down
                coef[2, 2 * q + par] = centre[1] + up
                coef[3, 2 * q + par] = high
                store[pl.ds(128 + q * 8, 8), pl.ds(par * 128, 128)] = weight

        for q in range(4):
            for par in range(2):
                low_c, a_c, b_c, high_c, a_x, b_x = [coef[n, 2 * q + par] for n in range(6)]
                for t in range(TR):
                    cell = lambda start: tr_s[(t, k, *row_set(start))]
                    start = 32 * q + 2 * par
                    a, b = cell(start), cell(start + 1)
                    low = cell(start - 1) if start else pltpu.roll(cell(3), 1, 0)
                    high = cell(start + 2) if start < 98 else pltpu.roll(cell(96), 7, 0)
                    side = a_x * a + b_x * b
                    value = (a_c * a + b_c * b) + (low_c * low + high_c * high)
                    value = value + jnp.take_along_axis(side, swap, axis=1)
                    store[pl.ds(t * 32 + q * 8, 8), pl.ds(par * 128, 128)] = value

    def pooled(k, n):
        both = jnp.concatenate(halves(stores[n]), axis=1)
        values = jnp.dot(both, pool[...], preferred_element_type=F32)
        rows = pl.ds(pl.multiple_of(k * 32, 32), 32)
        for t in range(TR):
            num2[t, rows, :] = values[t * 32 : t * 32 + 32]
        den2[rows, :] = values[128:160]

    def group_body(k, carry):
        for n in range(PAIR):
            pooled((k * PAIR + n + LV - PAIR) % LV, n)
        for n in range(PAIR):
            level(k * PAIR + n, n)
        return carry

    stores[...] = jnp.zeros_like(stores)
    lax.fori_loop(0, LV // PAIR, group_body, 0)
    for n in range(PAIR):
        pooled(LV - PAIR + n, n)


def kernel_first_call(tr_v, h_v, east_v, north_v, area_v, diff, pool):
    vmem = pl.BlockSpec(memory_space=pltpu.VMEM)
    return pl.pallas_call(
        kernel_first,
        name="first",
        out_shape=(
            jax.ShapeDtypeStruct((TR, 512, 128), F32),
            jax.ShapeDtypeStruct((512, 128), F32),
        ),
        in_specs=[vmem] * 5 + [pl.BlockSpec(memory_space=pltpu.SMEM), vmem],
        out_specs=(vmem,) * 2,
        scratch_shapes=[
            pltpu.VMEM((16, 8, 128), F32),
            pltpu.VMEM((PAIR, 16, 8, 128), F32),
            pltpu.VMEM((PAIR, 4, 16, 8, 128), F32),
            pltpu.VMEM((PAIR, 6, 8, 8, 128), F32),
            pltpu.VMEM((PAIR, 160, 256), F32),
        ],
        compiler_params=pltpu.CompilerParams(vmem_limit_bytes=16 * MIB),
        cost_estimate=pl.CostEstimate(flops=60_000_000, bytes_accessed=11 * MIB, transcendentals=0),
    )(tr_v, h_v, east_v, north_v, area_v, diff, pool)


def spread(values, offset):
    index = (lane_iota() & 31) + offset
    return jnp.take_along_axis(values, index, axis=1)


def kernel_second(
    num2, den2, ew, ew_one, ew_two, ns_one, ns_two, got_one, got_two, diff, placing, shares,
    send, d_ew, d_ns,
    work, pooled_rows, acc, chunks, send_s, sems,
):
    lane, sub = lane_iota(), sub_iota()
    odd = lax.axis_index("lat") % 2 == 1
    odd_lon = lax.axis_index("lon") % 2 == 1
    at_fold = lax.axis_index("lat") == lax.axis_size("lat") - 1
    is_east = (lane & 1) == 0
    level_of = (lane >> 1) & 15
    mixing = jnp.zeros((8, 128), F32)
    for k in range(LV):
        mixing = jnp.where(level_of == k, 2.0 * diff[k], mixing)

    def neighbour(n):
        one, two = ew_one[n], ew_two[n]
        from_east, from_west = jnp.where(odd_lon, two, one), jnp.where(odd_lon, one, two)
        return jnp.where(is_east, pltpu.roll(from_east, 127, 1), pltpu.roll(from_west, 1, 1))

    pending = None
    for v in range(16):
        own_hu, near_hu = ew[16 + v // 2], neighbour(16 + v // 2)
        base = 64 * (v % 2)
        h = spread(own_hu, base)
        p, q = half_face(
            h, spread(near_hu, base), spread(own_hu, base + 32), spread(near_hu, base + 32), mixing
        )
        div = jnp.where(is_east, q, p) * neighbour(v) - jnp.where(is_east, p, q) * ew[v]
        d_ew[v] = div
        value = depth_gain(2.0 * h) * div
        if v % 2 == 0:
            pending = value
        else:
            value = pending + value
            far_value = pltpu.roll(value, 64, 1)
            q, par = v // 4, (v // 2) % 2
            plain = jnp.where(is_east, value, far_value)
            moved = jnp.where(is_east, far_value, value)
            if par == 0:
                lower = plain, moved
            else:
                for half in range(2):
                    first_lanes = (lane < 64) == is_east
                    mine = first_lanes if half == 0 else ~first_lanes
                    work[half, q] = jnp.where(mine, lower[0], moved)

    ends = ((lane & 63) == 0) | ((lane & 63) == 63)

    def add_ends(t):
        for k in range(LV):
            for q in range(4):
                rows = pl.ds(k * 32 + q * 8, 8)
                moved = pltpu.roll(work[t // 2, q], (63 - 2 * k - 32 * t) % 128, 1)
                acc[t, rows, :] = num2[t, rows, :] + jnp.where(ends, moved, 0.0)
        for top in range(2):
            for half in range(2):
                at = (t, pl.ds(256 * half + 31 * top, 8, stride=32), slice(None))
                acc[at] = acc[at] + pooled_rows[top, t, pl.ds(8 * half, 8), :]

    pools = [shares[par] for par in range(2)]
    quarter = [shares[2 + j] for j in range(4)]

    back = 127 - lane
    for half in range(2):
        mix = jnp.zeros((8, 128), F32)
        for k in range(8):
            mix = jnp.where(sub == k, diff[8 * half + k], mix)

        def rows_of(ref, n):
            return ref[pl.ds(n * 16 + 8 * half, 8), :]

        def own(n, top):
            pair = (ns_two, ns_one) if top else (ns_one, ns_two)
            return jnp.where(odd, rows_of(pair[0], n), rows_of(pair[1], n))

        def near(n, top, sign=1.0):
            if not top:
                return jnp.where(odd, rows_of(got_one, n), rows_of(got_two, n))
            value = jnp.where(odd, rows_of(got_two, n), rows_of(got_one, n))
            turned = sign * jnp.take_along_axis(value, back, axis=1)
            return jnp.where(at_fold, turned, value)

        for top in (False, True):
            h = own(4, top)
            p, q = face(h, near(4, top), own(5, top), near(5, top, -1.0), mix)
            gain = depth_gain(h)
            for t in range(TR):
                if top:
                    div = q * near(t, top) - p * own(t, top)
                else:
                    div = p * near(t, top) - q * own(t, top)
                d_ns[int(top), pl.ds(t * 16 + 8 * half, 8), :] = div
                pooled_rows[int(top), t, pl.ds(8 * half, 8), :] = split_dot(
                    gain * div, pools[int(top)]
                )

    def keep(n, values):
        high, low = halves(values)
        chunks[0:128, pl.ds(n * 128, 128)] = high
        chunks[128:256, pl.ds(n * 128, 128)] = low

    def every_fourth(ref, *lead, j):
        return jnp.concatenate(
            [ref[(*lead, pl.ds(32 * m + j, 8, stride=4), slice(None))] for m in range(16)], axis=0
        )

    copies = []

    def place(group):
        placed = jnp.dot(
            placing[...], chunks[:, pl.ds(group * 512, 512)], preferred_element_type=F32
        )
        for c in range(4):
            for slot in range(CAP):
                for m in range(DEV // 8):
                    start = m * 8 * 40 + (4 * group + c) * CAP + slot
                    send_s[pl.ds(start, 8, stride=40), :] = placed[
                        slot * DEV + m * 8 : slot * DEV + m * 8 + 8, c * 128 : c * 128 + 128
                    ]
        part = send_s.reshape(DEV, 40, 128).at[:, pl.ds(8 * group, 8), :]
        copies.append(
            pltpu.make_async_copy(part, send.at[:, pl.ds(8 * group, 8), :], sems.at[group])
        )
        copies[-1].start()

    gains = []
    den4 = jnp.zeros((128, 128), F32)
    for j in range(4):
        den = every_fourth(den2, j=j)
        gains.append(1.0 / jnp.maximum(den, weight_floor))
        den4 = den4 + split_dot(den, quarter[j])
    gain4 = 1.0 / jnp.maximum(den4, weight_floor)
    for t in range(TR):
        add_ends(t)
        num4 = jnp.zeros((128, 128), F32)
        for j in range(4):
            num = every_fourth(acc, t, j=j)
            keep(t * 4 + j, num * gains[j])
            num4 = num4 + split_dot(num, quarter[j])
        keep(16 + t, num4 * gain4)
        place(t)
    place(TR)
    for copy in copies:
        copy.wait()


def kernel_second_call(*args):
    vmem = pl.BlockSpec(memory_space=pltpu.VMEM)
    return pl.pallas_call(
        kernel_second,
        name="second",
        out_shape=(
            pltpu.HBM((DEV, CAP * CHUNKS, 128), F32),
            jax.ShapeDtypeStruct((16, 8, 128), F32),
            jax.ShapeDtypeStruct((2, 64, 128), F32),
        ),
        in_specs=[vmem] * 9 + [pl.BlockSpec(memory_space=pltpu.SMEM), vmem, vmem],
        out_specs=(pl.BlockSpec(memory_space=pltpu.HBM), vmem, vmem),
        scratch_shapes=[
            pltpu.VMEM((2, 4, 8, 128), F32),
            pltpu.VMEM((2, TR, 16, 128), F32),
            pltpu.VMEM((TR, 512, 128), F32),
            pltpu.VMEM((256, 2560), BF16),
            pltpu.VMEM((DEV * CAP * CHUNKS, 128), F32),
            pltpu.SemaphoreType.DMA((TR + 1,)),
        ],
        compiler_params=pltpu.CompilerParams(vmem_limit_bytes=16 * MIB),
        cost_estimate=pl.CostEstimate(flops=60_000_000, bytes_accessed=6 * MIB, transcendentals=0),
    )(*args)


def kernel_third(
    tr, fill, mask, east, north, diff, area, d_ew, d_ns,
    out,
    tr_s, fill_s, mask_s, east_s, north_s, area_s, out_s, moved_s, sems, area_sem, out_sems,
):
    hbm, vmem = (tr, fill, mask, east, north), (tr_s, fill_s, mask_s, east_s, north_s)
    copies = input_copies(hbm, vmem, sems)
    area_copy = pltpu.make_async_copy(area, area_s, area_sem)
    for group in range(GROUPS):
        for copy in copies(group):
            copy.start()
        if group == 0:
            area_copy.start()
    area_copy.wait()
    lane, sub = lane_iota(), sub_iota()
    ends = (lane == 0) | (lane == 127)
    not_last, not_top = lane < 127, sub < 7
    per = LV // GROUPS

    def out_copy(group):
        levels = pl.ds(group * per, per)
        return pltpu.make_async_copy(out_s.at[:, levels], out.at[:, levels], out_sems.at[group])

    def level(k):
        mixing = diff[k]

        def load(ref, start):
            return ref[(k, *row_set(start))]

        def depth(start):
            return load(fill_s, start) * load(mask_s, start).astype(F32)

        for v in range(16):
            edge = d_ew[v]
            for t in range(TR):
                moved = pltpu.roll(edge, 127 - 2 * k + (128 - 32 * t), 1)
                moved_s[v, t] = jnp.where(ends, moved, 0.0)

        before = [jnp.zeros((8, 128), F32)] * TR
        for q in range(4):
            hs = [depth(32 * q + j) for j in range(4)]
            vs = [load(north_s, 32 * q + j) for j in range(4)]
            if q < 3:
                hs.append(depth(32 * q + 4))
                vs.append(load(north_s, 32 * q + 4))
            else:
                hs.append(pltpu.roll(hs[0], 7, 0))
                vs.append(pltpu.roll(vs[0], 7, 0))
            coefs = []
            for j in range(4):
                top = q == 3 and j == 3
                h, u = hs[j], load(east_s, 32 * q + j)
                rate = time_step / (area_s[row_set(32 * q + j)] * jnp.maximum(h, depth_floor))
                coefs.append(
                    face(h, pltpu.roll(h, 127, 1), u, pltpu.roll(u, 127, 1), mixing, keep=not_last)
                    + face(h, hs[j + 1], vs[j], vs[j + 1], mixing, keep=not_top if top else None)
                    + (rate,)
                )
            for t in range(TR):
                cells = [tr_s[(t, k, *row_set(32 * q + j))] for j in range(4)]
                if q < 3:
                    cells.append(tr_s[(t, k, *row_set(32 * q + 4))])
                else:
                    cells.append(pltpu.roll(cells[0], 7, 0))
                norths = [coefs[j][2] * cells[j] - coefs[j][3] * cells[j + 1] for j in range(4)]
                turned = pltpu.roll(norths[3], 1, 0)
                souths = [jnp.where(sub > 0, turned, before[t])] + norths[:3]
                before[t] = turned
                for j in range(4):
                    p_e, q_e, _, _, rate = coefs[j]
                    cell = cells[j]
                    flux = p_e * cell - q_e * pltpu.roll(cell, 127, 1)
                    div = (pltpu.roll(flux, 1, 1) - flux) + (souths[j] - norths[j])
                    div = div + moved_s[4 * q + j, t]
                    if q == 0 and j == 0:
                        div = div + jnp.where(sub == 0, d_ns[0, pl.ds(t * 16 + k, 1), :], 0.0)
                    if q == 3 and j == 3:
                        div = div + jnp.where(sub == 7, d_ns[1, pl.ds(t * 16 + k, 1), :], 0.0)
                    out_s[(t, k, *row_set(32 * q + j))] = cell + rate * div

    def group_body(group, carry):
        for copy in copies(group):
            copy.wait()
        for n in range(per):
            level(group * per + n)
        out_copy(group).start()
        return carry

    lax.fori_loop(0, GROUPS, group_body, 0)
    for group in range(GROUPS):
        out_copy(group).wait()


def kernel_third_call(tracers, fill, mask, east, north, diff, area, d_ew, d_ns):
    hbm = pl.BlockSpec(memory_space=pltpu.HBM)
    vmem = pl.BlockSpec(memory_space=pltpu.VMEM)
    return pl.pallas_call(
        kernel_third,
        name="third",
        out_shape=jax.ShapeDtypeStruct((TR, LV, ROWS, LANES), F32),
        in_specs=[hbm] * 5 + [pl.BlockSpec(memory_space=pltpu.SMEM), hbm, vmem, vmem],
        out_specs=hbm,
        scratch_shapes=[
            pltpu.VMEM((TR, LV, ROWS, LANES), F32),
            pltpu.VMEM((LV, ROWS, LANES), F32),
            pltpu.VMEM((LV, ROWS, LANES), jnp.int32),
            pltpu.VMEM((LV, ROWS, LANES), F32),
            pltpu.VMEM((LV, ROWS, LANES), F32),
            pltpu.VMEM((ROWS, LANES), F32),
            pltpu.VMEM((TR, LV, ROWS, LANES), F32),
            pltpu.VMEM((16, TR, 8, 128), F32),
            pltpu.SemaphoreType.DMA((5, GROUPS)),
            pltpu.SemaphoreType.DMA,
            pltpu.SemaphoreType.DMA((GROUPS,)),
        ],
        compiler_params=pltpu.CompilerParams(vmem_limit_bytes=24 * MIB),
        cost_estimate=pl.CostEstimate(flops=60_000_000, bytes_accessed=12 * MIB, transcendentals=0),
    )(tracers, fill, mask, east, north, diff, area, d_ew, d_ns)


def kernel_last(got, two, four, rows_s, sems):
    copies = []
    for n in range(CHUNKS):
        for slot in range(CAP):
            for m in range(DEV // 8):
                rows_s[n, pl.ds(m * 16 + slot, 8, stride=CAP), :] = got[
                    pl.ds(m * 8 * 40 + n * CAP + slot, 8, stride=40), :
                ]
        out = two.at[:, pl.ds(n * 128, 128)] if n < 16 else four.at[:, pl.ds((n - 16) * 128, 128)]
        copies.append(pltpu.make_async_copy(rows_s.at[n], out, sems.at[n]))
        copies[-1].start()
    for copy in copies:
        copy.wait()


def kernel_last_call(got):
    hbm = pl.BlockSpec(memory_space=pltpu.HBM)
    return pl.pallas_call(
        kernel_last,
        name="last",
        out_shape=(pltpu.HBM((DEV * CAP, 2048), F32), pltpu.HBM((DEV * CAP, 512), F32)),
        in_specs=[pl.BlockSpec(memory_space=pltpu.VMEM)],
        out_specs=(hbm, hbm),
        scratch_shapes=[
            pltpu.VMEM((CHUNKS, DEV * CAP, 128), F32),
            pltpu.SemaphoreType.DMA((CHUNKS,)),
        ],
        compiler_params=pltpu.CompilerParams(vmem_limit_bytes=8 * MIB),
    )(got)


def local(
    tracers, fill_fraction, ocean_mask, east_speed, north_speed, diffusivity, cell_area, owner_map
):
    lon_count = lax.axis_size("lon")
    lat_count = lax.axis_size("lat")
    *in_hbm, diffusivity, area_hbm, owners = (
        pltpu.with_memory_space_constraint(x, pltpu.HBM)
        for x in (
            tracers, fill_fraction, ocean_mask, east_speed, north_speed, diffusivity, cell_area,
            owner_map.reshape(1, DEV),
        )
    )
    ns_one, ns_two, placing, pool, shares = kernel_rows_call(
        in_hbm[0], in_hbm[1], in_hbm[2], in_hbm[4], owners
    )
    both = ("lon", "lat")

    def swapped(pairs):
        return [pair for a, b in pairs for pair in ((a, b), (b, a))]

    def at(lon, lat):
        return lon * lat_count + lat

    lons = range(lon_count)
    step_one = [(at(n, a), at(n, a + 1)) for n in lons for a in range(0, lat_count, 2)]
    step_two = [(at(n, a), at(n, a + 1)) for n in lons for a in range(1, lat_count - 1, 2)]
    fold = [
        (at(n, lat_count - 1), at(lon_count - 1 - n, lat_count - 1)) for n in range(lon_count // 2)
    ]
    got_one = lax.ppermute(ns_one, both, swapped(step_one))
    got_two = lax.ppermute(ns_two, both, swapped(step_two + fold))
    h_v, ew = kernel_edges_call(tracers, fill_fraction, ocean_mask, east_speed)
    ew_one = lax.ppermute(ew, "lon", swapped([(n, n + 1) for n in range(0, lon_count, 2)]))
    ew_two = lax.ppermute(
        ew, "lon", swapped([(n, (n + 1) % lon_count) for n in range(1, lon_count, 2)])
    )
    num2, den2 = kernel_first_call(
        tracers, h_v, east_speed, north_speed, cell_area, diffusivity, pool
    )
    send, d_ew, d_ns = kernel_second_call(
        num2, den2, ew, ew_one, ew_two, ns_one, ns_two, got_one, got_two, diffusivity, placing,
        shares,
    )
    got = lax.all_to_all(
        send, both, split_axis=0, concat_axis=0, tiled=True
    )
    updated = kernel_third_call(*in_hbm, diffusivity, area_hbm, d_ew, d_ns)
    two, four = kernel_last_call(got.reshape(DEV * CAP * CHUNKS, 128))
    return (updated, two[None], four[None])


def solution(mesh):
    in_specs = (
        P(None, None, "lat", "lon"),
        P(None, "lat", "lon"),
        P(None, "lat", "lon"),
        P(None, "lat", "lon"),
        P(None, "lat", "lon"),
        P(),
        P("lat", "lon"),
        P(("lon", "lat"), None),
    )
    out_specs = (
        P(None, None, "lat", "lon"),
        P(("lon", "lat"), None, None),
        P(("lon", "lat"), None, None),
    )
    return jax.shard_map(
        local,
        mesh=mesh, in_specs=in_specs, out_specs=out_specs, check_vma=False,
    )
```
